32 devices in a mesh: batch: 8 (over z, x), seq: 4 (over y, core).
Axes of the slice: x: 2, y: 2, z: 4, core: 2. Of those that a mesh axis runs over, the one named last changes fastest.
Arguments:
- acoustic_sequence: bfloat16 [16, 1024, 1024], P('batch', 'seq'), may hold values from -6 to 6
- utterance_durations: int32 [16], P('batch'), may hold values from 1 to 1024, 12288 in all
- chosen_entry_number: int32 [16, 1024], P('batch', 'seq'), may hold values from 0 to 1023
- discretizer_score_perturbation: bfloat16 [16, 1024, 1024], P('batch', 'seq'), may hold values from -6 to 6
- softmax_heat: float32 [], replicated, may hold values from 0.7 to 2
- normalizer_affine_rows: bfloat16 [14, 1024], P(None, 'batch'), may hold values from -0.5 to 1.3
- discretizer_score_projection: bfloat16 [1024, 1024], P('batch'), may hold values from -0.1875 to 0.1875
- lexicon_vectors: bfloat16 [1024, 1024], P('batch'), may hold values from -6 to 6
- opening_dense_entry_projection: bfloat16 [1024, 4096], P('batch'), may hold values from -0.1875 to 0.1875
- opening_dense_exit_projection: bfloat16 [4096, 1024], P('batch'), may hold values from -0.1875 to 0.1875
- request_projection: bfloat16 [1024, 1024], P('batch'), may hold values from -0.1875 to 0.1875
- lookup_projection: bfloat16 [1024, 1024], P('batch'), may hold values from -0.1875 to 0.1875
- content_projection_kernel: bfloat16 [1024, 1024], P('batch'), may hold values from -0.1875 to 0.1875
- relative_offset_projection: bfloat16 [1024, 1024], P('batch'), may hold values from -0.25 to 0.25
- mixing_exit_projection: bfloat16 [1024, 1024], P('batch'), may hold values from -1 to 1
- unit_kernel_before_gating: bfloat16 [1024, 2048], P('batch'), may hold values from -0.1875 to 0.1875
- channelwise_filter_coefficients: bfloat16 [5, 1024], P(None, 'batch'), may hold values from -2.5 to 2.5
- unit_kernel_after_normalizing: bfloat16 [1024, 1024], P('batch'), may hold values from -0.1875 to 0.1875
- closing_dense_entry_projection: bfloat16 [1024, 4096], P('batch'), may hold values from -0.1875 to 0.1875
- closing_dense_exit_projection: bfloat16 [4096, 1024], P('batch'), may hold values from -0.1875 to 0.1875
- result_adjoint: bfloat16 [16, 1024, 1024], P('batch', 'seq'), may hold values from -6 to 6
- discrete_label_adjoint: bfloat16 [16, 1024, 1024], P('batch', 'seq'), may hold values from -6 to 6
Outputs:
- output: bfloat16 [16, 1024, 1024], P('batch', 'seq')
- codes: bfloat16 [16, 1024, 1024], P('batch', 'seq')
- frames_grad: bfloat16 [16, 1024, 1024], P('batch', 'seq')
- vectors_grad: float32 [14, 1024], P(None, 'batch')
- quant_proj_grad: float32 [1024, 1024], P('batch', 'seq')
- codebook_grad: float32 [1024, 1024], P('batch', 'seq')
- macaron_in_grad: float32 [1024, 4096], P('batch', 'seq')
- macaron_out_grad: float32 [4096, 1024], P('batch', 'seq')
- query_grad: float32 [1024, 1024], P('batch', 'seq')
- key_grad: float32 [1024, 1024], P('batch', 'seq')
- value_grad: float32 [1024, 1024], P('batch', 'seq')
- pos_grad: float32 [1024, 1024], P('batch', 'seq')
- out_proj_grad: float32 [1024, 1024], P('batch', 'seq')
- conv_in_grad: float32 [1024, 2048], P('batch', 'seq')
- depth_grad: float32 [5, 1024], P(None, 'batch')
- conv_out_grad: float32 [1024, 1024], P('batch', 'seq')
- closing_in_grad: float32 [1024, 4096], P('batch', 'seq')
- closing_out_grad: float32 [4096, 1024], P('batch', 'seq')
The draws below stay inside these ranges and needn't reach their ends.
Inputs may be any that keep to these rules, and one draw needn't show every extreme that they name: `utterance_durations`: frames at or past an utterance's length are padding. Some utterance has exactly 1024 frames.
All inputs are finite; a program needn't handle non-finite values. No bound on the sum of `utterance_durations` on one device may be relied on, other than what follows from the above.
Results may differ from the reference program's by a relative error of at most 0.028.
Values may be sent and summed in bfloat16 or wider, within the bound.
No kernel may reach another device: no remote copies, remote signals or barrier semaphores. Data moves between devices by JAX's collectives and lax.ppermute only.
A program may use at most 320 MiB of HBM per device.

```python
import math
from functools import partial
import jax
import jax.numpy as jnp
import numpy as np
from jax import lax

D = 1024
FF = 4096
HEADS = 8
E = 1024
HEAD_DIM = 128
KERNEL = 5
NVEC = 14
LEN = 1024
UTT_GRP = 2
UTTS = 16
N_BATCH = 8


def draw_normalizer_affine_rows(key, part):
    base_draw = jnp.clip(jax.random.normal(key, (NVEC, D), jnp.float32) * 0.5, -1.0, 1.0)
    row_ids = jnp.arange(NVEC, dtype=jnp.int32)[:, None]
    is_scale = (row_ids < 5) | (row_ids == 10)
    is_bias = row_ids >= 12
    return jnp.where(is_scale, 1.0 + 0.3 * base_draw, jnp.where(is_bias, 0.5 * base_draw, 0.3 * base_draw)).astype(jnp.bfloat16)


def set_ends(values, own_key, smallest, top_value):
    shape = values.shape
    spot = [jax.random.randint(jax.random.fold_in(own_key, axis), (), 0, shape[axis]) for axis in range(len(shape))]
    values = values.at[tuple(spot)].set(smallest)
    longest = shape.index(max(shape))
    spot[longest] = (spot[longest] + 1) % shape[longest]
    return values.at[tuple(spot)].set(top_value)


def levels(own_key, extent, pieces, low, top_value):
    def one(axis_at, blocks):
        draws = jax.random.uniform(jax.random.fold_in(jax.random.fold_in(own_key, 6), axis_at), (blocks,), jnp.float32, low / len(pieces), top_value / len(pieces))
        return jnp.repeat(jnp.exp(draws), extent[axis_at] // blocks).reshape((-1,) + (1,) * (len(extent) - axis_at - 1))

    loudness = one(*pieces[0])
    for cut in pieces[1:]:
        loudness = loudness * one(*cut)
    return loudness


def split_up(amount, total, limit, lean):
    loads = [(1 << 20) // math.isqrt(grade ** lean) + 1 for grade in range(2, amount + 1)]
    surplus, given = total - limit - (amount - 1), [1] * (amount - 1)
    while surplus > 0:
        free = [i for i in range(amount - 1) if given[i] < limit]
        whole, remaining = sum([loads[i] for i in free]), surplus
        for i in free:
            more = min(limit - given[i], max(1, remaining * loads[i] // whole), surplus)
            given[i] = given[i] + more
            surplus = surplus - more
    return np.array([limit] + given)


def uneven_parts(stream_key, count, total, bound, skew):
    if count == 2:
        one = jax.random.randint(stream_key, (), max(1, total - bound), min(bound, total - 1) + 1)
        return jnp.stack([one, total - one])
    lengths = jnp.asarray(split_up(count, total, bound, skew), jnp.int32)
    couples = (count - 1) // 2
    donor, sink = lengths[1:1 + 2 * couples:2], lengths[2:2 + 2 * couples:2]
    margin = jnp.minimum(donor - 1, bound - sink)
    passed = jax.random.randint(jax.random.fold_in(stream_key, 1), (couples,), 0, 1 << 20) % (margin + 1)
    lengths = lengths.at[1:1 + 2 * couples:2].set(donor - passed).at[2:2 + 2 * couples:2].set(sink + passed)
    return lengths[jax.random.permutation(jax.random.fold_in(stream_key, 2), count)]


def gaussian(rng, extent, width, reach, cuts=(), kind=jnp.bfloat16):
    values = jax.random.normal(rng, extent, jnp.float32) * width
    if len(cuts) > 0:
        values = levels(rng, extent, cuts, -0.22, 0.18) * values
    return jnp.clip(values, min=-reach, max=reach).astype(kind)


def setup_inputs(seed: int = 0) -> dict:
    seeds = jax.random.split(jax.random.key(seed), 23)
    return {
        "acoustic_sequence": gaussian(seeds[0], (UTTS, LEN, D), 1.0, 6.0, ((0, 8), (1, 4))),
        "utterance_durations": uneven_parts(seeds[1], UTTS, 3 * UTTS * LEN // 4, LEN, 1).astype(jnp.int32),
        "chosen_entry_number": set_ends(jax.random.randint(seeds[2], (UTTS, LEN), 0, E), jax.random.fold_in(seeds[2], 1), 0, E - 1).astype(jnp.int32),
        "discretizer_score_perturbation": gaussian(seeds[3], (UTTS, LEN, E), 1.3, 6.0, ((0, 8), (1, 4))),
        "softmax_heat": jnp.clip(jax.random.uniform(seeds[4], (), jnp.float32, 0.7, 2.0), 0.7, 2.0),
        "normalizer_affine_rows": draw_normalizer_affine_rows(jax.random.fold_in(seeds[22], 71), 0),
        "discretizer_score_projection": gaussian(seeds[6], (D, E), D ** -0.5, 0.1875, ((0, 8),)),
        "lexicon_vectors": gaussian(seeds[7], (E, D), 1.0, 6.0, ((0, 8),)),
        "opening_dense_entry_projection": gaussian(seeds[8], (D, FF), D ** -0.5, 0.1875, ((0, 8),)),
        "opening_dense_exit_projection": gaussian(seeds[9], (FF, D), (FF // 4) ** -0.5, 0.1875, ((0, 8),)),
        "request_projection": gaussian(seeds[10], (D, D), D ** -0.5, 0.1875, ((0, 8),)),
        "lookup_projection": gaussian(seeds[11], (D, D), D ** -0.5, 0.1875, ((0, 8),)),
        "content_projection_kernel": gaussian(seeds[12], (D, D), D ** -0.5, 0.1875, ((0, 8),)),
        "relative_offset_projection": gaussian(seeds[13], (D, D), (D // 2) ** -0.5, 0.25, ((0, 8),)),
        "mixing_exit_projection": gaussian(seeds[14], (D, D), (D // 32) ** -0.5, 1.0, ((0, 8),)),
        "unit_kernel_before_gating": gaussian(seeds[15], (D, 2 * D), D ** -0.5, 0.1875, ((0, 8),)),
        "channelwise_filter_coefficients": gaussian(seeds[16], (KERNEL, D), KERNEL ** -0.5, 2.5, ((1, 8),)),
        "unit_kernel_after_normalizing": gaussian(seeds[17], (D, D), D ** -0.5, 0.1875, ((0, 8),)),
        "closing_dense_entry_projection": gaussian(seeds[18], (D, FF), D ** -0.5, 0.1875, ((0, 8),)),
        "closing_dense_exit_projection": gaussian(seeds[19], (FF, D), (FF // 4) ** -0.5, 0.1875, ((0, 8),)),
        "result_adjoint": gaussian(seeds[20], (UTTS, LEN, D), 1.0, 6.0, ((0, 8), (1, 4))),
        "discrete_label_adjoint": gaussian(seeds[21], (UTTS, LEN, D), 1.0, 6.0, ((0, 8), (1, 4))),
    }


epsilon = 1e-05
precise = lax.Precision.HIGHEST

@jax.custom_vjp
def low(v):
    return lax.optimization_barrier(v.astype(jnp.bfloat16)).astype(jnp.float32)

@jax.custom_vjp
def low_back(v):
    return v

def low_keep(v):
    return (low(v), None)

def low_pass(kept, grad):
    return (grad,)

def back_keep(v):
    return (v, None)

def back_low(kept, grad):
    return (low(grad),)
low.defvjp(low_keep, low_pass)
low_back.defvjp(back_keep, back_low)

def product(left_side, right_side):
    return jnp.matmul(left_side, right_side, precision=precise)

def linear(block_arguments, weight):
    return low_back(product(low(block_arguments), weight))

def layer_norm(values, scale_row, shift_row):
    center = values - lax.optimization_barrier(jnp.mean(values, axis=-1, keepdims=True))
    spread = lax.optimization_barrier(jnp.mean(center * center, axis=-1, keepdims=True))
    return center * lax.rsqrt(spread + epsilon) * scale_row + shift_row

def glu_gate(gated_rows):
    half_width = gated_rows.shape[-1] // 2
    return gated_rows[..., :half_width] * jax.nn.sigmoid(gated_rows[..., half_width:])

def batch_norm(conv_value, sum_first, sum_second, scale_row, shift_row, count_all):
    center = sum_first / count_all
    spread = sum_second / count_all - center * center
    return (conv_value - center) * lax.rsqrt(spread + epsilon) * scale_row + shift_row

def feed_forward(values, scale_row, shift_row, weight_in, weight_out):
    hidden = jax.nn.silu(linear(layer_norm(values, scale_row, shift_row), weight_in))
    return linear(hidden, weight_out)

def position_table(length, model_width):
    offsets = (jnp.arange(2 * length - 1, dtype=jnp.int32) - (length - 1)).astype(jnp.float32)
    pairs = jnp.arange(model_width // 2, dtype=jnp.int32).astype(jnp.float32)
    rates = jnp.exp(pairs * (-2.0 * math.log(10000.0) / model_width))
    angles = offsets[:, None] * rates[None, :]
    return jnp.stack([jnp.sin(angles), jnp.cos(angles)], axis=-1).reshape(2 * length - 1, model_width)

def relative_shift(relative):
    head_count, row_count, span_len = relative.shape
    flat_rows = relative.reshape(head_count, row_count * span_len)
    moved_rows = lax.slice_in_dim(flat_rows, row_count - 1, row_count - 1 + row_count * (span_len - 1), axis=1)
    return moved_rows.reshape(head_count, row_count, span_len - 1)[:, :, :row_count]

def depth_conv(padded, kernel_rows, length):
    result = kernel_rows[0] * padded[:, 0:length]
    for offset in range(1, kernel_rows.shape[0]):
        result = result + kernel_rows[offset] * padded[:, offset:offset + length]
    return result

def attend_one(items, position_rows, content_bias, position_bias):
    query_rows, key_rows, value_rows, length_one = items
    content = jnp.einsum('ihd,jhd->hij', low(query_rows + content_bias), key_rows, precision=precise)
    relative = jnp.einsum('ihd,nhd->hin', low(query_rows + position_bias), position_rows, precision=precise)
    raw_scores = low_back(content + relative_shift(relative))
    key_valid = jnp.arange(LEN, dtype=jnp.int32)[None, None, :] < length_one
    discretizer_scores = jnp.where(key_valid, raw_scores * (1.0 / math.sqrt(HEAD_DIM)), -1e+30)
    weights_soft = jax.nn.softmax(discretizer_scores, axis=-1)
    return jnp.einsum('hij,jhd->ihd', low(weights_soft), value_rows, precision=precise)

def block_evaluation(block_arguments, block_coefficients, usable_mask_timesteps, utterance_durations, chosen_entry_number, perturbation_all_sets, softmax_heat):
    normalizer_affine_rows, discretizer_score_projection, lexicon_vectors, opening_dense_entry_projection, opening_dense_exit_projection, request_projection, lookup_projection, content_projection_kernel, relative_offset_projection, mixing_exit_projection, unit_kernel_before_gating, channelwise_filter_coefficients, unit_kernel_after_normalizing, closing_dense_entry_projection, closing_dense_exit_projection = block_coefficients
    table_low = low(position_table(LEN, D))
    split_heads = (UTT_GRP, LEN, HEADS, HEAD_DIM)
    content_bias = normalizer_affine_rows[12].reshape(HEADS, HEAD_DIM)
    position_bias = normalizer_affine_rows[13].reshape(HEADS, HEAD_DIM)
    rim = KERNEL // 2

    def first_section(carry, group):
        group_in, valid_mask, group_ids, perturbation_each_set, group_lengths = group
        discretizer_scores = low_back(product(low(group_in), discretizer_score_projection))
        relaxed_assignments = jax.nn.softmax((discretizer_scores + perturbation_each_set) / softmax_heat, axis=-1)
        one_hot = (group_ids[..., None] == jnp.arange(E, dtype=jnp.int32)).astype(jnp.float32)
        codes = valid_mask[..., None] * (product(one_hot, lexicon_vectors) + product(low(relaxed_assignments), lexicon_vectors))
        first_mid = group_in + 0.5 * feed_forward(group_in, normalizer_affine_rows[0], normalizer_affine_rows[5], opening_dense_entry_projection, opening_dense_exit_projection)
        normed = low(layer_norm(first_mid, normalizer_affine_rows[1], normalizer_affine_rows[6]))
        queries = low(linear(normed, request_projection)).reshape(split_heads)
        keys_part = low(linear(normed, lookup_projection)).reshape(split_heads)
        values_part = low(linear(normed, content_projection_kernel)).reshape(split_heads)
        position = low(low_back(product(table_low, relative_offset_projection))).reshape(2 * LEN - 1, HEADS, HEAD_DIM)
        attend = jax.checkpoint(partial(attend_one, position_rows=position, content_bias=content_bias, position_bias=position_bias))
        attended = lax.map(attend, (queries, keys_part, values_part, group_lengths))
        mixed = low(low_back(attended.reshape(UTT_GRP, LEN, D)))
        second_mid = first_mid + linear(mixed, mixing_exit_projection)
        gated_rows = linear(layer_norm(second_mid, normalizer_affine_rows[2], normalizer_affine_rows[7]), unit_kernel_before_gating)
        glu_low = low(valid_mask[..., None] * glu_gate(gated_rows))
        padded = jnp.pad(glu_low, ((0, 0), (rim, rim), (0, 0)))
        conv_value = low_back(depth_conv(padded, channelwise_filter_coefficients, LEN))
        masked = valid_mask[..., None] * conv_value
        carry_next = (carry[0] + lax.optimization_barrier(jnp.sum(masked, axis=(0, 1))), carry[1] + lax.optimization_barrier(jnp.sum(masked * conv_value, axis=(0, 1))))
        return (carry_next, (second_mid, conv_value, codes))
    valid_groups = usable_mask_timesteps.reshape(N_BATCH, UTT_GRP, LEN)
    groups_in = (block_arguments.reshape(N_BATCH, UTT_GRP, LEN, D), valid_groups, chosen_entry_number.reshape(N_BATCH, UTT_GRP, LEN), perturbation_all_sets.reshape(N_BATCH, UTT_GRP, LEN, E), utterance_durations.reshape(N_BATCH, UTT_GRP))
    start = (jnp.zeros((D,), jnp.float32), jnp.zeros((D,), jnp.float32))
    sums_pair, stacked = lax.scan(jax.checkpoint(first_section), start, groups_in)
    mids, convs, codes_all = stacked
    count_all = jnp.sum(usable_mask_timesteps)

    def second_section(group):
        second_mid, conv_value, valid_mask = group
        normalized = batch_norm(conv_value, sums_pair[0], sums_pair[1], normalizer_affine_rows[10], normalizer_affine_rows[11], count_all)
        third_mid = second_mid + linear(jax.nn.silu(normalized), unit_kernel_after_normalizing)
        fourth_mid = third_mid + 0.5 * feed_forward(third_mid, normalizer_affine_rows[3], normalizer_affine_rows[8], closing_dense_entry_projection, closing_dense_exit_projection)
        return valid_mask[..., None] * layer_norm(fourth_mid, normalizer_affine_rows[4], normalizer_affine_rows[9])
    outputs = lax.map(jax.checkpoint(second_section), (mids, convs, valid_groups))
    return (outputs.reshape(UTTS, LEN, D), codes_all.reshape(UTTS, LEN, D))

def reference(acoustic_sequence, utterance_durations, chosen_entry_number, discretizer_score_perturbation, softmax_heat, normalizer_affine_rows, discretizer_score_projection, lexicon_vectors, opening_dense_entry_projection, opening_dense_exit_projection, request_projection, lookup_projection, content_projection_kernel, relative_offset_projection, mixing_exit_projection, unit_kernel_before_gating, channelwise_filter_coefficients, unit_kernel_after_normalizing, closing_dense_entry_projection, closing_dense_exit_projection, result_adjoint, discrete_label_adjoint):
    block_coefficients = tuple((item.astype(jnp.float32) for item in (normalizer_affine_rows, discretizer_score_projection, lexicon_vectors, opening_dense_entry_projection, opening_dense_exit_projection, request_projection, lookup_projection, content_projection_kernel, relative_offset_projection, mixing_exit_projection, unit_kernel_before_gating, channelwise_filter_coefficients, unit_kernel_after_normalizing, closing_dense_entry_projection, closing_dense_exit_projection)))
    block_arguments = acoustic_sequence.astype(jnp.float32)
    usable_mask_timesteps = (jnp.arange(LEN, dtype=jnp.int32)[None, :] < utterance_durations[:, None]).astype(jnp.float32)
    perturbation_all_sets = discretizer_score_perturbation.astype(jnp.float32)
    limited_evaluation = partial(block_evaluation, usable_mask_timesteps=usable_mask_timesteps, utterance_durations=utterance_durations, chosen_entry_number=chosen_entry_number, perturbation_all_sets=perturbation_all_sets, softmax_heat=softmax_heat.astype(jnp.float32))
    out_pair, pullback = jax.vjp(limited_evaluation, block_arguments, block_coefficients)
    grad_inputs, grad_params = pullback((result_adjoint.astype(jnp.float32), discrete_label_adjoint.astype(jnp.float32)))
    g_vectors, g_quant, g_codebook, g_mac_in, g_mac_out, g_query, g_key, g_value, g_pos, g_out, g_conv_in, g_depth, g_conv_out, g_close_in, g_close_out = grad_params
    return (out_pair[0].astype(jnp.bfloat16), out_pair[1].astype(jnp.bfloat16), grad_inputs.astype(jnp.bfloat16), g_vectors, g_quant, g_codebook, g_mac_in, g_mac_out, g_query, g_key, g_value, g_pos, g_out, g_conv_in, g_depth, g_conv_out, g_close_in, g_close_out)
```

```python
from functools import partial
import math

import jax
import jax.numpy as jnp
from jax import lax
from jax.experimental import pallas as pl
from jax.experimental.pallas import tpu as pltpu
from jax.sharding import PartitionSpec as P

HEAD_WIDTH = 128


epsilon = 1e-05

F32, BF16 = jnp.float32, jnp.bfloat16

def dot(a, b, ca, cb):
    return lax.dot_general(a, b, (((ca,), (cb,)), ((), ())), preferred_element_type=F32)

def _fwd_body(len_ref, q_ref, k_ref, v_ref, pos_ref, bias_ref, o_ref, p_ref, *, rows, full, scale):
    block = pl.program_id(2)
    length = len_ref[pl.program_id(0)]
    query = q_ref[0, 0].astype(F32)
    content_query = (query + bias_ref[0:1, :]).astype(BF16)
    position_query = (query + bias_ref[1:2, :]).astype(BF16)
    content = dot(content_query, k_ref[0, 0], 1, 1)
    span = full + rows
    start = pl.multiple_of(full - rows - block * rows, rows)
    relative = dot(position_query, pos_ref[pl.ds(start, span), :], 1, 1)
    relative = pltpu.roll(relative, span - (rows - 1), 1, stride=1, stride_axis=0)
    raw = content + relative[:, :full]
    seen = lax.broadcasted_iota(jnp.int32, raw.shape, 1) < length
    scores = jnp.where(seen, raw * scale, -1e30)
    top = jnp.max(scores, axis=-1, keepdims=True)
    weights = jnp.exp(scores - top)
    total = jnp.sum(weights, axis=-1, keepdims=True)
    low = (weights * (1.0 / total)).astype(BF16)
    p_ref[0, 0] = low
    o_ref[0] = dot(low, v_ref[0, 0], 1, 0).astype(BF16)

def attend_forward(by_heads, position, bias, lengths, rows=256):
    _, groups, full, width = by_heads.shape
    depth = HEAD_WIDTH
    heads = width // depth
    body = partial(_fwd_body, rows=rows, full=full, scale=1.0 / math.sqrt(depth))
    flops = groups * heads * full * (2 * full * depth * 3 + 2 * rows * depth)
    return pl.pallas_call(
        body,
        grid_spec=pltpu.PrefetchScalarGridSpec(
            num_scalar_prefetch=1,
            grid=(groups, heads, full // rows),
            in_specs=[
                pl.BlockSpec((1, 1, rows, depth), lambda u, h, i, n: (0, u, i, h)),
                pl.BlockSpec((1, 1, full, depth), lambda u, h, i, n: (1, u, 0, h)),
                pl.BlockSpec((1, 1, full, depth), lambda u, h, i, n: (2, u, 0, h)),
                pl.BlockSpec((2 * full, depth), lambda u, h, i, n: (0, h)),
                pl.BlockSpec((2, depth), lambda u, h, i, n: (0, h)),
            ],
            out_specs=[
                pl.BlockSpec((1, rows, depth), lambda u, h, i, n: (u, i, h)),
                pl.BlockSpec((1, 1, rows, full), lambda u, h, i, n: (u, h, i, 0)),
            ],
        ),
        out_shape=[
            jax.ShapeDtypeStruct((groups, full, width), BF16),
            jax.ShapeDtypeStruct((groups, heads, full, full), BF16),
        ],
        compiler_params=pltpu.CompilerParams(vmem_limit_bytes=48 << 20),
        cost_estimate=pl.CostEstimate(flops=flops, transcendentals=groups * heads * full * full, bytes_accessed=groups * heads * full * full * 2 + 5 * groups * full * width * 2),
        name="attend_forward",
    )(lengths, by_heads, by_heads, by_heads, position, bias)

def _bwd_body(p_ref, q_ref, k_ref, v_ref, g_ref, pos_ref, bias_ref, d_ref, dpos_ref, dbias_ref,
              key_acc, value_acc, pos_acc, bias_acc, *, rows, full, scale):
    group, block = pl.program_id(1), pl.program_id(2)
    last_block = block == pl.num_programs(2) - 1

    @pl.when((group == 0) & (block == 0))
    def _():
        pos_acc[...] = jnp.zeros_like(pos_acc)
        bias_acc[...] = jnp.zeros_like(bias_acc)

    @pl.when(block == 0)
    def _():
        key_acc[...] = jnp.zeros_like(key_acc)
        value_acc[...] = jnp.zeros_like(value_acc)

    query = q_ref[0, 0].astype(F32)
    content_query = (query + bias_ref[0:1, :]).astype(BF16)
    position_query = (query + bias_ref[1:2, :]).astype(BF16)
    keys, grad = k_ref[0, 0], g_ref[0]
    low = p_ref[0, 0]
    weights = low.astype(F32)
    grad_weights = dot(grad, v_ref[0, 0], 1, 1)
    value_acc[...] += dot(grad, low, 0, 0)
    inner = jnp.sum(grad_weights * weights, axis=-1, keepdims=True)
    grad_raw = (weights * (grad_weights - inner) * scale).astype(BF16)
    key_acc[...] += dot(content_query, grad_raw, 0, 0)
    grad_content = dot(grad_raw, keys, 1, 0)
    row = lax.broadcasted_iota(jnp.int32, (rows, rows), 0)
    column = lax.broadcasted_iota(jnp.int32, (rows, rows), 1)
    flip = jnp.where(row + column == rows - 1, 1.0, 0.0).astype(BF16)
    span = full + rows
    start = pl.multiple_of(full - rows - block * rows, rows)
    turned = jnp.concatenate([dot(flip, grad_raw, 1, 0).astype(BF16), jnp.zeros((rows, rows), BF16)], axis=1)
    turned = pltpu.roll(turned, 0, 1, stride=1, stride_axis=0)
    turned_query = dot(flip, position_query, 1, 0).astype(BF16)
    pos_acc[:, pl.ds(start, span)] += dot(turned_query, turned, 0, 0)
    grad_turned = dot(turned, pos_ref[pl.ds(start, span), :], 1, 0)
    high = grad_turned.astype(BF16)
    rest = (grad_turned - high.astype(F32)).astype(BF16)
    grad_position = dot(flip, high, 1, 0) + dot(flip, rest, 1, 0)
    here = pl.ds(pl.multiple_of(block * rows, rows), rows)
    d_ref[0, 0, here, :] = (grad_content + grad_position).astype(BF16)
    bias_acc[0:1, :] += jnp.sum(grad_content, axis=0, keepdims=True)
    bias_acc[1:2, :] += jnp.sum(grad_position, axis=0, keepdims=True)

    @pl.when(last_block)
    def _():
        d_ref[1, 0] = key_acc[...].T.astype(BF16)
        d_ref[2, 0] = value_acc[...].T.astype(BF16)

    @pl.when(last_block & (group == pl.num_programs(1) - 1))
    def _():
        dpos_ref[...] = pos_acc[...].T.astype(BF16)
        dbias_ref[...] = bias_acc[...]

def attend_backward(probs, by_heads, grad_heads, position, bias, rows=256):
    _, groups, full, width = by_heads.shape
    depth = HEAD_WIDTH
    heads = width // depth
    body = partial(_bwd_body, rows=rows, full=full, scale=1.0 / math.sqrt(depth))
    flops = groups * heads * full * (2 * full * depth * 7 + 6 * rows * depth)
    return pl.pallas_call(
        body,
        grid_spec=pltpu.PrefetchScalarGridSpec(
            num_scalar_prefetch=0,
            grid=(heads, groups, full // rows),
            in_specs=[
                pl.BlockSpec((1, 1, rows, full), lambda h, u, i: (u, h, i, 0)),
                pl.BlockSpec((1, 1, rows, depth), lambda h, u, i: (0, u, i, h)),
                pl.BlockSpec((1, 1, full, depth), lambda h, u, i: (1, u, 0, h)),
                pl.BlockSpec((1, 1, full, depth), lambda h, u, i: (2, u, 0, h)),
                pl.BlockSpec((1, rows, depth), lambda h, u, i: (u, i, h)),
                pl.BlockSpec((2 * full, depth), lambda h, u, i: (0, h)),
                pl.BlockSpec((2, depth), lambda h, u, i: (0, h)),
            ],
            out_specs=[
                pl.BlockSpec((3, 1, full, depth), lambda h, u, i: (0, u, 0, h)),
                pl.BlockSpec((2 * full, depth), lambda h, u, i: (0, h)),
                pl.BlockSpec((2, depth), lambda h, u, i: (0, h)),
            ],
            scratch_shapes=[
                pltpu.VMEM((depth, full), F32),
                pltpu.VMEM((depth, full), F32),
                pltpu.VMEM((depth, 2 * full), F32),
                pltpu.VMEM((2, depth), F32),
            ],
        ),
        out_shape=[
            jax.ShapeDtypeStruct((3, groups, full, width), BF16),
            jax.ShapeDtypeStruct((2 * full, width), BF16),
            jax.ShapeDtypeStruct((2, width), F32),
        ],
        compiler_params=pltpu.CompilerParams(vmem_limit_bytes=48 << 20),
        cost_estimate=pl.CostEstimate(flops=flops, transcendentals=0, bytes_accessed=groups * heads * full * full * 2 + 8 * groups * full * width * 2),
        name="attend_backward",
    )(probs, by_heads, by_heads, by_heads, grad_heads, position, bias)


def extended(value, sides, width):
    for axis, dim in sides:
        size, length = (lax.axis_size(axis), value.shape[dim])
        up = [(i, (i + 1) % size) for i in range(size - 1)]
        down = [(j, i) for i, j in up]
        last = lax.slice_in_dim(value, length - width, length, axis=dim)
        initial = lax.slice_in_dim(value, 0, width, axis=dim)
        before = lax.ppermute(last, axis, up)
        after = lax.ppermute(initial, axis, down)
        value = jnp.concatenate([before, value, after], axis=dim)
    return value


def layer_norm(values, scale_row, shift_row):
    center = values - jnp.mean(values, axis=-1, keepdims=True)
    spread = jnp.mean(center * center, axis=-1, keepdims=True)
    return center * lax.rsqrt(spread + epsilon) * scale_row + shift_row


def glu_gate(gated_rows):
    half_width = gated_rows.shape[-1] // 2
    return gated_rows[..., :half_width] * jax.nn.sigmoid(gated_rows[..., half_width:])


def batch_norm(conv_value, sum_first, sum_second, scale_row, shift_row, count_all):
    center = sum_first / count_all
    spread = sum_second / count_all - center * center
    return (conv_value - center) * lax.rsqrt(spread + epsilon) * scale_row + shift_row


def position_table(length, model_width):
    fine = 64
    coarse = 2 * length // fine
    column = jnp.arange(model_width, dtype=jnp.int32)
    rates = jnp.exp((column // 2).astype(jnp.float32) * (-2.0 * math.log(10000.0) / model_width))
    odd = (column % 2 == 1)[None, :]
    start = (jnp.arange(coarse, dtype=jnp.int32) * fine - (length - 1)).astype(jnp.float32)
    large = start[:, None] * rates[None, :]
    small = jnp.arange(fine, dtype=jnp.int32).astype(jnp.float32)[:, None] * rates[None, :]
    sin_large, cos_large = jnp.sin(large), jnp.cos(large)
    first = jnp.where(odd, cos_large, sin_large)[:, None, :]
    second = jnp.where(odd, -sin_large, cos_large)[:, None, :]
    table = first * jnp.cos(small)[None] + second * jnp.sin(small)[None]
    return table.astype(jnp.bfloat16).reshape(2 * length, model_width)


def depth_conv(padded, kernel_rows, length):
    result = kernel_rows[0] * padded[:, 0:length]
    for offset in range(1, kernel_rows.shape[0]):
        result = result + kernel_rows[offset] * padded[:, offset : offset + length]
    return result


def depth_conv_back(padded_grad, kernel_rows, length):
    last_tap = kernel_rows.shape[0] - 1
    result = kernel_rows[0] * padded_grad[:, last_tap : last_tap + length]
    for offset in range(1, last_tap + 1):
        result = (
            result
            + kernel_rows[offset] * padded_grad[:, last_tap - offset : last_tap - offset + length]
        )
    return result


def matmul_rows(left_side, right_side):
    return jnp.dot(left_side, right_side, preferred_element_type=jnp.float32)


def times_transpose(left_side, right_side):
    return lax.dot_general(
        left_side, right_side, (((1,), (1,)), ((), ())), preferred_element_type=jnp.float32
    )


def transpose_times(left_side, right_side):
    return lax.dot_general(
        left_side, right_side, (((0,), (0,)), ((), ())), preferred_element_type=jnp.float32
    )


def linear_back(grad_rows, weight):
    grad_low = grad_rows.astype(jnp.bfloat16)
    return (times_transpose(grad_low, weight), grad_low)


def ffn_forward(values, scale_row, shift_row, weight_in, weight_out):
    normed_low = layer_norm(values, scale_row, shift_row).astype(jnp.bfloat16)
    hidden_pre = matmul_rows(normed_low, weight_in)
    hidden_low = jax.nn.silu(hidden_pre).astype(jnp.bfloat16)
    return (matmul_rows(hidden_low, weight_out), (normed_low, hidden_pre, hidden_low))


def ffn_backward(grad_rows, values, scale_row, shift_row, weight_in, weight_out, saved_parts):
    normed_low, hidden_pre, hidden_low = saved_parts
    grad_hidden, grad_out_low = linear_back(grad_rows, weight_out)
    silu_value, silu_back = jax.vjp(jax.nn.silu, hidden_pre)
    grad_pre = silu_back(grad_hidden)[0]
    grad_normed, grad_pre_low = linear_back(grad_pre, weight_in)
    norm_value, norm_back = jax.vjp(layer_norm, values, scale_row, shift_row)
    grad_values, grad_scale, grad_shift = norm_back(grad_normed)
    return (grad_values, grad_scale, grad_shift, grad_pre_low, grad_out_low)


def sum_everywhere(value):
    for axis in ("seq", "batch"):
        size, step = lax.axis_size(axis), 1
        while step < size:
            value = value + lax.ppermute(value, axis, [(i, i ^ step) for i in range(size)])
            step *= 2
    return value


def sum_small_seq(smalls):
    small_sums = (
        lax.psum(smalls[0].astype(jnp.bfloat16), "seq").astype(jnp.float32),
        lax.psum(smalls[1].astype(jnp.bfloat16), "seq").astype(jnp.float32),
    )
    return tuple(small_sums)


def sum_over_seq(matrices, smalls):
    (
        grad_one,
        grad_two,
        grad_three,
        grad_four,
        grad_five,
        grad_six,
        grad_seven,
        grad_eight,
        grad_nine,
        grad_ten,
        grad_eleven,
        grad_twelve,
        grad_thirteen,
    ) = matrices
    reduced = (
        lax.psum_scatter(
            grad_one.astype(jnp.bfloat16), "seq", scatter_dimension=1, tiled=True
        ).astype(jnp.float32),
        lax.psum_scatter(
            grad_two.astype(jnp.bfloat16), "seq", scatter_dimension=1, tiled=True
        ).astype(jnp.float32),
        lax.psum_scatter(
            grad_three.astype(jnp.bfloat16), "seq", scatter_dimension=1, tiled=True
        ).astype(jnp.float32),
        lax.psum_scatter(
            grad_four.astype(jnp.bfloat16), "seq", scatter_dimension=1, tiled=True
        ).astype(jnp.float32),
        lax.psum_scatter(
            grad_five.astype(jnp.bfloat16), "seq", scatter_dimension=1, tiled=True
        ).astype(jnp.float32),
        lax.psum_scatter(
            grad_six.astype(jnp.bfloat16), "seq", scatter_dimension=1, tiled=True
        ).astype(jnp.float32),
        lax.psum_scatter(
            grad_seven.astype(jnp.bfloat16), "seq", scatter_dimension=1, tiled=True
        ).astype(jnp.float32),
        lax.psum_scatter(
            grad_eight.astype(jnp.bfloat16), "seq", scatter_dimension=1, tiled=True
        ).astype(jnp.float32),
        lax.psum_scatter(
            grad_nine.astype(jnp.bfloat16), "seq", scatter_dimension=1, tiled=True
        ).astype(jnp.float32),
        lax.psum_scatter(
            grad_ten.astype(jnp.bfloat16), "seq", scatter_dimension=1, tiled=True
        ).astype(jnp.float32),
        lax.psum_scatter(
            grad_eleven.astype(jnp.bfloat16), "seq", scatter_dimension=1, tiled=True
        ).astype(jnp.float32),
        lax.psum_scatter(
            grad_twelve.astype(jnp.bfloat16), "seq", scatter_dimension=1, tiled=True
        ).astype(jnp.float32),
        lax.psum_scatter(
            grad_thirteen.astype(jnp.bfloat16), "seq", scatter_dimension=1, tiled=True
        ).astype(jnp.float32),
    )
    return (tuple(reduced), sum_small_seq(smalls))


def sum_over_batch(matrices, smalls):
    (
        grad_one,
        grad_two,
        grad_three,
        grad_four,
        grad_five,
        grad_six,
        grad_seven,
        grad_eight,
        grad_nine,
        grad_ten,
        grad_eleven,
        grad_twelve,
        grad_thirteen,
    ) = matrices
    small_one, small_two = smalls
    reduced = (
        lax.psum_scatter(
            grad_one.astype(jnp.bfloat16), "batch", scatter_dimension=0, tiled=True
        ).astype(jnp.float32),
        lax.psum_scatter(
            grad_two.astype(jnp.bfloat16), "batch", scatter_dimension=0, tiled=True
        ).astype(jnp.float32),
        lax.psum_scatter(
            grad_three.astype(jnp.bfloat16), "batch", scatter_dimension=0, tiled=True
        ).astype(jnp.float32),
        lax.psum_scatter(
            grad_four.astype(jnp.bfloat16), "batch", scatter_dimension=0, tiled=True
        ).astype(jnp.float32),
        lax.psum_scatter(
            grad_five.astype(jnp.bfloat16), "batch", scatter_dimension=0, tiled=True
        ).astype(jnp.float32),
        lax.psum_scatter(
            grad_six.astype(jnp.bfloat16), "batch", scatter_dimension=0, tiled=True
        ).astype(jnp.float32),
        lax.psum_scatter(
            grad_seven.astype(jnp.bfloat16), "batch", scatter_dimension=0, tiled=True
        ).astype(jnp.float32),
        lax.psum_scatter(
            grad_eight.astype(jnp.bfloat16), "batch", scatter_dimension=0, tiled=True
        ).astype(jnp.float32),
        lax.psum_scatter(
            grad_nine.astype(jnp.bfloat16), "batch", scatter_dimension=0, tiled=True
        ).astype(jnp.float32),
        lax.psum_scatter(
            grad_ten.astype(jnp.bfloat16), "batch", scatter_dimension=0, tiled=True
        ).astype(jnp.float32),
        lax.psum_scatter(
            grad_eleven.astype(jnp.bfloat16), "batch", scatter_dimension=0, tiled=True
        ).astype(jnp.float32),
        lax.psum_scatter(
            grad_twelve.astype(jnp.bfloat16), "batch", scatter_dimension=0, tiled=True
        ).astype(jnp.float32),
        lax.psum_scatter(
            grad_thirteen.astype(jnp.bfloat16), "batch", scatter_dimension=0, tiled=True
        ).astype(jnp.float32),
        lax.psum_scatter(
            small_one.astype(jnp.bfloat16), "batch", scatter_dimension=1, tiled=True
        ).astype(jnp.float32),
        lax.psum_scatter(
            small_two.astype(jnp.bfloat16), "batch", scatter_dimension=1, tiled=True
        ).astype(jnp.float32),
    )
    return (tuple(reduced[:13]), tuple(reduced[13:]))


def per_device(
    acoustic_sequence,
    utterance_durations,
    chosen_entry_number,
    discretizer_score_perturbation,
    softmax_heat,
    normalizer_affine_rows,
    discretizer_score_projection,
    lexicon_vectors,
    opening_dense_entry_projection,
    opening_dense_exit_projection,
    request_projection,
    lookup_projection,
    content_projection_kernel,
    relative_offset_projection,
    mixing_exit_projection,
    unit_kernel_before_gating,
    channelwise_filter_coefficients,
    unit_kernel_after_normalizing,
    closing_dense_entry_projection,
    closing_dense_exit_projection,
    result_adjoint,
    discrete_label_adjoint,
):
    (
        vectors_all,
        quant_all,
        codebook_all,
        macaron_in_all,
        macaron_out_all,
        query_all,
        key_all,
        value_all,
        pos_all,
        out_all,
        conv_in_all,
        depth_all,
        conv_out_all,
        closing_in_all,
        closing_out_all,
    ) = (
        lax.all_gather(normalizer_affine_rows, "batch", axis=1, tiled=True),
        lax.all_gather(discretizer_score_projection, "batch", axis=0, tiled=True),
        lax.all_gather(lexicon_vectors, "batch", axis=0, tiled=True),
        lax.all_gather(opening_dense_entry_projection, "batch", axis=0, tiled=True),
        lax.all_gather(opening_dense_exit_projection, "batch", axis=0, tiled=True),
        lax.all_gather(request_projection, "batch", axis=0, tiled=True),
        lax.all_gather(lookup_projection, "batch", axis=0, tiled=True),
        lax.all_gather(content_projection_kernel, "batch", axis=0, tiled=True),
        lax.all_gather(relative_offset_projection, "batch", axis=0, tiled=True),
        lax.all_gather(mixing_exit_projection, "batch", axis=0, tiled=True),
        lax.all_gather(unit_kernel_before_gating, "batch", axis=0, tiled=True),
        lax.all_gather(channelwise_filter_coefficients, "batch", axis=1, tiled=True),
        lax.all_gather(unit_kernel_after_normalizing, "batch", axis=0, tiled=True),
        lax.all_gather(closing_dense_entry_projection, "batch", axis=0, tiled=True),
        lax.all_gather(closing_dense_exit_projection, "batch", axis=0, tiled=True),
    )
    groups, local_len, model_width = acoustic_sequence.shape
    seq_count = lax.axis_size("seq")
    seq_place = lax.axis_index("seq")
    full_len = local_len * seq_count
    entries = codebook_all.shape[0]
    total_rows = groups * local_len
    local_width = model_width // seq_count
    kernel_size = depth_all.shape[0]
    rim_width = kernel_size // 2
    params_f = vectors_all.astype(jnp.float32)
    depth_f = depth_all.astype(jnp.float32)
    positions = seq_place * local_len + jnp.arange(local_len, dtype=jnp.int32)
    valid_mask = (positions[None, :] < utterance_durations[:, None]).astype(jnp.float32)
    valid_rows = valid_mask.reshape(total_rows, 1)
    inputs_low = acoustic_sequence.reshape(total_rows, model_width)
    inputs_f = inputs_low.astype(jnp.float32)
    quant_logits = matmul_rows(inputs_low, quant_all)
    scaled_logits = (
        quant_logits
        + discretizer_score_perturbation.reshape(total_rows, entries).astype(jnp.float32)
    ) / softmax_heat
    relaxed_assignments = jax.nn.softmax(scaled_logits, axis=-1)
    soft_low = relaxed_assignments.astype(jnp.bfloat16)
    one_hot = (
        chosen_entry_number.reshape(total_rows, 1) == jnp.arange(entries, dtype=jnp.int32)[None, :]
    ).astype(jnp.bfloat16)
    codes_value = valid_rows * (
        matmul_rows(one_hot, codebook_all) + matmul_rows(soft_low, codebook_all)
    )
    macaron_value, macaron_saved = ffn_forward(
        inputs_f, params_f[0], params_f[5], macaron_in_all, macaron_out_all
    )
    first_mid = inputs_f + 0.5 * macaron_value
    attn_normed = layer_norm(first_mid, params_f[1], params_f[6]).astype(jnp.bfloat16)
    stacked = (
        jnp.stack(
            [
                matmul_rows(attn_normed, query_all),
                matmul_rows(attn_normed, key_all),
                matmul_rows(attn_normed, value_all),
            ]
        )
        .astype(jnp.bfloat16)
        .reshape(3, groups, local_len, model_width)
    )
    by_heads = lax.all_to_all(stacked, "seq", split_axis=3, concat_axis=2, tiled=True)
    table_low = position_table(full_len, model_width)
    pos_columns = lax.dynamic_slice_in_dim(pos_all, seq_place * local_width, local_width, 1)
    position_low = matmul_rows(table_low, pos_columns).astype(jnp.bfloat16)
    biases = lax.dynamic_slice_in_dim(params_f[12:14], seq_place * local_width, local_width, 1)
    attended_low, probs = attend_forward(by_heads, position_low, biases, utterance_durations)
    back_time = lax.all_to_all(
        attended_low,
        "seq",
        split_axis=1,
        concat_axis=2,
        tiled=True,
    )
    attended_rows = back_time.reshape(total_rows, model_width)
    second_mid = first_mid + matmul_rows(attended_rows, out_all)
    conv_normed = layer_norm(second_mid, params_f[2], params_f[7]).astype(jnp.bfloat16)
    gated_rows = matmul_rows(conv_normed, conv_in_all)
    glu_low = (
        (valid_rows * glu_gate(gated_rows))
        .astype(jnp.bfloat16)
        .reshape(groups, local_len, model_width)
    )
    padded_glu = extended(glu_low, (("seq", 1),), rim_width)
    conv_value = depth_conv(padded_glu, depth_f, local_len).reshape(total_rows, model_width)
    masked_conv = valid_rows * conv_value
    sums = sum_everywhere(
        jnp.stack(
            [
                jnp.sum(masked_conv, axis=0),
                jnp.sum(masked_conv * conv_value, axis=0),
                jnp.broadcast_to(jnp.sum(valid_mask), (model_width,)),
            ]
        )
    )
    sum_first, sum_second, count_all = sums[0], sums[1], sums[2]
    bound_norm = partial(batch_norm, count_all=count_all)
    normalized = bound_norm(conv_value, sum_first, sum_second, params_f[10], params_f[11])
    act_low = jax.nn.silu(normalized).astype(jnp.bfloat16)
    third_mid = second_mid + matmul_rows(act_low, conv_out_all)
    closing_value, closing_saved = ffn_forward(
        third_mid, params_f[3], params_f[8], closing_in_all, closing_out_all
    )
    fourth_mid = third_mid + 0.5 * closing_value
    final_value, final_back = jax.vjp(layer_norm, fourth_mid, params_f[4], params_f[9])
    output = (valid_rows * final_value).astype(jnp.bfloat16).reshape(groups, local_len, model_width)
    codes = codes_value.astype(jnp.bfloat16).reshape(groups, local_len, model_width)
    grad_final = valid_rows * result_adjoint.reshape(total_rows, model_width).astype(jnp.float32)
    grad_fourth, scale_four, shift_four = final_back(grad_final)
    grad_closing, scale_three, shift_three, close_pre_low, close_out_low = ffn_backward(
        0.5 * grad_fourth,
        third_mid,
        params_f[3],
        params_f[8],
        closing_in_all,
        closing_out_all,
        closing_saved,
    )
    grad_third = grad_fourth + grad_closing
    grad_act, grad_third_low = linear_back(grad_third, conv_out_all)
    silu_value, silu_back = jax.vjp(jax.nn.silu, normalized)
    grad_normalized = silu_back(grad_act)[0]
    norm_value, norm_back = jax.vjp(
        bound_norm, conv_value, sum_first, sum_second, params_f[10], params_f[11]
    )
    grad_conv_direct, part_first, part_second, grad_bn_scale, grad_bn_shift = norm_back(
        grad_normalized
    )
    total_first, total_second = sum_everywhere(jnp.stack([part_first, part_second]))
    grad_conv = grad_conv_direct + valid_rows * (total_first + 2.0 * conv_value * total_second)
    grad_conv_low = grad_conv.astype(jnp.bfloat16).reshape(groups, local_len, model_width)
    padded_grad = extended(grad_conv_low, (("seq", 1),), rim_width)
    grad_glu = valid_rows * depth_conv_back(padded_grad, depth_f, local_len).reshape(
        total_rows, model_width
    )
    grad_conv_float = grad_conv_low.astype(jnp.float32)
    grad_depth = jnp.stack(
        [
            jnp.sum(
                padded_glu[:, offset : offset + local_len].astype(jnp.float32) * grad_conv_float,
                axis=(0, 1),
            )
            for offset in range(kernel_size)
        ]
    )
    glu_value, glu_back = jax.vjp(glu_gate, gated_rows)
    grad_gated = glu_back(grad_glu)[0]
    grad_conv_normed, grad_gated_low = linear_back(grad_gated, conv_in_all)
    conv_norm_value, conv_norm_back = jax.vjp(layer_norm, second_mid, params_f[2], params_f[7])
    grad_from_conv, scale_two, shift_two = conv_norm_back(grad_conv_normed)
    grad_second = grad_third + grad_from_conv
    grad_attended, grad_second_low = linear_back(grad_second, out_all)
    grad_heads = lax.all_to_all(
        grad_second_low_heads(grad_attended, groups, local_len, model_width),
        "seq",
        split_axis=2,
        concat_axis=1,
        tiled=True,
    )

    grad_stack, grad_position_low, grad_biases = attend_backward(
        probs, by_heads, grad_heads, position_low, biases
    )
    grad_time = lax.all_to_all(grad_stack, "seq", split_axis=2, concat_axis=3, tiled=True).reshape(
        3, total_rows, model_width
    )
    grad_attn_normed = (
        times_transpose(grad_time[0], query_all)
        + times_transpose(grad_time[1], key_all)
        + times_transpose(grad_time[2], value_all)
    )
    attn_norm_value, attn_norm_back = jax.vjp(layer_norm, first_mid, params_f[1], params_f[6])
    grad_from_attn, scale_one, shift_one = attn_norm_back(grad_attn_normed)
    grad_first = grad_second + grad_from_attn
    grad_pos_columns = transpose_times(table_low, grad_position_low)
    content_full, position_full = lax.dynamic_update_slice_in_dim(
        jnp.zeros((2, model_width), jnp.float32), grad_biases, seq_place * local_width, 1
    )
    grad_macaron, scale_zero, shift_zero, mac_pre_low, mac_out_low = ffn_backward(
        0.5 * grad_first,
        inputs_f,
        params_f[0],
        params_f[5],
        macaron_in_all,
        macaron_out_all,
        macaron_saved,
    )
    grad_layer_in = grad_first + grad_macaron
    grad_codes = (
        valid_rows * discrete_label_adjoint.reshape(total_rows, model_width).astype(jnp.float32)
    ).astype(jnp.bfloat16)
    grad_soft = times_transpose(grad_codes, codebook_all)
    rescaled_derivative = relaxed_assignments * (
        grad_soft - jnp.sum(grad_soft * relaxed_assignments, axis=-1, keepdims=True)
    )
    score_derivative_lowprecision = (rescaled_derivative / softmax_heat).astype(jnp.bfloat16)
    grad_quant_in = times_transpose(score_derivative_lowprecision, quant_all)
    frames_grad = (
        (grad_layer_in + grad_quant_in).astype(jnp.bfloat16).reshape(groups, local_len, model_width)
    )
    vectors_grad = jnp.stack(
        [
            scale_zero,
            scale_one,
            scale_two,
            scale_three,
            scale_four,
            shift_zero,
            shift_one,
            shift_two,
            shift_three,
            shift_four,
            grad_bn_scale,
            grad_bn_shift,
            content_full,
            position_full,
        ]
    )
    smalls = (vectors_grad, grad_depth)
    mac_normed, mac_pre, mac_hidden = macaron_saved
    close_normed, close_pre, close_hidden = closing_saved
    grad_pos_w = lax.dynamic_update_slice_in_dim(
        jnp.zeros((model_width, model_width), jnp.float32),
        grad_pos_columns,
        seq_place * local_width,
        1,
    )
    matrices = (
        transpose_times(inputs_low, score_derivative_lowprecision),
        transpose_times(one_hot, grad_codes) + transpose_times(soft_low, grad_codes),
        transpose_times(mac_normed, mac_pre_low),
        transpose_times(mac_hidden, mac_out_low),
        transpose_times(attn_normed, grad_time[0]),
        transpose_times(attn_normed, grad_time[1]),
        transpose_times(attn_normed, grad_time[2]),
        grad_pos_w,
        transpose_times(attended_rows, grad_second_low),
        transpose_times(conv_normed, grad_gated_low),
        transpose_times(act_low, grad_third_low),
        transpose_times(close_normed, close_pre_low),
        transpose_times(close_hidden, close_out_low),
    )
    matrices, smalls = sum_over_seq(matrices, smalls)
    matrices, smalls = sum_over_batch(matrices, smalls)
    (
        quant_sum,
        codebook_sum,
        macaron_in_sum,
        macaron_out_sum,
        query_sum,
        key_sum,
        value_sum,
        pos_sum,
        out_sum,
        conv_in_sum,
        conv_out_sum,
        closing_in_sum,
        closing_out_sum,
    ) = matrices
    vectors_sum, depth_sum = smalls
    return (
        output,
        codes,
        frames_grad,
        vectors_sum,
        quant_sum,
        codebook_sum,
        macaron_in_sum,
        macaron_out_sum,
        query_sum,
        key_sum,
        value_sum,
        pos_sum,
        out_sum,
        conv_in_sum,
        depth_sum,
        conv_out_sum,
        closing_in_sum,
        closing_out_sum,
    )


def grad_second_low_heads(grad_attended, groups, local_len, model_width):
    return grad_attended.astype(jnp.bfloat16).reshape(groups, local_len, model_width)


def flat_rows(blocks):
    return blocks.reshape(blocks.shape[0] * blocks.shape[1], blocks.shape[2])


def solution(mesh):
    placed = (
        P("batch", "seq", None),
        P("batch"),
        P("batch", "seq"),
        P("batch", "seq", None),
        P(),
        P(None, "batch"),
        P("batch", None),
        P("batch", None),
        P("batch", None),
        P("batch", None),
        P("batch", None),
        P("batch", None),
        P("batch", None),
        P("batch", None),
        P("batch", None),
        P("batch", None),
        P(None, "batch"),
        P("batch", None),
        P("batch", None),
        P("batch", None),
        P("batch", "seq", None),
        P("batch", "seq", None),
    )
    return jax.shard_map(
        per_device,
        mesh=mesh,
        in_specs=placed,
        out_specs=(
            P("batch", "seq", None),
            P("batch", "seq", None),
            P("batch", "seq", None),
            P(None, "batch"),
            P("batch", "seq"),
            P("batch", "seq"),
            P("batch", "seq"),
            P("batch", "seq"),
            P("batch", "seq"),
            P("batch", "seq"),
            P("batch", "seq"),
            P("batch", "seq"),
            P("batch", "seq"),
            P("batch", "seq"),
            P(None, "batch"),
            P("batch", "seq"),
            P("batch", "seq"),
            P("batch", "seq"),
        ),
        check_vma=False,
    )
```

```python
from functools import partial
import math

import jax
import jax.numpy as jnp
from jax import lax
from jax.experimental import pallas as pl
from jax.experimental.pallas import tpu as pltpu
from jax.sharding import PartitionSpec as P

HEAD_WIDTH = 128


epsilon = 1e-05

F32, BF16 = jnp.float32, jnp.bfloat16

def dot(a, b, ca, cb):
    return lax.dot_general(a, b, (((ca,), (cb,)), ((), ())), preferred_element_type=F32)

def _fwd_body(len_ref, q_ref, k_ref, v_ref, pos_ref, bias_ref, o_ref, p_ref, *, rows, full, scale):
    block = pl.program_id(2)
    length = len_ref[pl.program_id(0)]
    query = q_ref[0, 0].astype(F32)
    content_query = (query + bias_ref[0:1, :]).astype(BF16)
    position_query = (query + bias_ref[1:2, :]).astype(BF16)
    content = dot(content_query, k_ref[0, 0], 1, 1)
    span = full + rows
    start = pl.multiple_of(full - rows - block * rows, rows)
    relative = dot(position_query, pos_ref[pl.ds(start, span), :], 1, 1)
    relative = pltpu.roll(relative, span - (rows - 1), 1, stride=1, stride_axis=0)
    raw = content + relative[:, :full]
    seen = lax.broadcasted_iota(jnp.int32, raw.shape, 1) < length
    scores = jnp.where(seen, raw * scale, -1e30)
    top = jnp.max(scores, axis=-1, keepdims=True)
    weights = jnp.exp(scores - top)
    total = jnp.sum(weights, axis=-1, keepdims=True)
    low = (weights * (1.0 / total)).astype(BF16)
    p_ref[0, 0] = low
    o_ref[0] = dot(low, v_ref[0, 0], 1, 0).astype(BF16)

def attend_forward(by_heads, position, bias, lengths, rows=256):
    _, groups, full, width = by_heads.shape
    depth = HEAD_WIDTH
    heads = width // depth
    body = partial(_fwd_body, rows=rows, full=full, scale=1.0 / math.sqrt(depth))
    flops = groups * heads * full * (2 * full * depth * 3 + 2 * rows * depth)
    return pl.pallas_call(
        body,
        grid_spec=pltpu.PrefetchScalarGridSpec(
            num_scalar_prefetch=1,
            grid=(groups, heads, full // rows),
            in_specs=[
                pl.BlockSpec((1, 1, rows, depth), lambda u, h, i, n: (0, u, i, h)),
                pl.BlockSpec((1, 1, full, depth), lambda u, h, i, n: (1, u, 0, h)),
                pl.BlockSpec((1, 1, full, depth), lambda u, h, i, n: (2, u, 0, h)),
                pl.BlockSpec((2 * full, depth), lambda u, h, i, n: (0, h)),
                pl.BlockSpec((2, depth), lambda u, h, i, n: (0, h)),
            ],
            out_specs=[
                pl.BlockSpec((1, rows, depth), lambda u, h, i, n: (u, i, h)),
                pl.BlockSpec((1, 1, rows, full), lambda u, h, i, n: (u, h, i, 0)),
            ],
        ),
        out_shape=[
            jax.ShapeDtypeStruct((groups, full, width), BF16),
            jax.ShapeDtypeStruct((groups, heads, full, full), BF16),
        ],
        compiler_params=pltpu.CompilerParams(vmem_limit_bytes=48 << 20),
        cost_estimate=pl.CostEstimate(flops=flops, transcendentals=groups * heads * full * full, bytes_accessed=groups * heads * full * full * 2 + 5 * groups * full * width * 2),
        name="attend_forward",
    )(lengths, by_heads, by_heads, by_heads, position, bias)

def _bwd_body(p_ref, q_ref, k_ref, v_ref, g_ref, pos_ref, bias_ref, d_ref, dpos_ref, dbias_ref,
              key_acc, value_acc, pos_acc, bias_acc, *, rows, full, scale):
    group, block = pl.program_id(1), pl.program_id(2)
    last_block = block == pl.num_programs(2) - 1

    @pl.when((group == 0) & (block == 0))
    def _():
        pos_acc[...] = jnp.zeros_like(pos_acc)
        bias_acc[...] = jnp.zeros_like(bias_acc)

    @pl.when(block == 0)
    def _():
        key_acc[...] = jnp.zeros_like(key_acc)
        value_acc[...] = jnp.zeros_like(value_acc)

    query = q_ref[0, 0].astype(F32)
    content_query = (query + bias_ref[0:1, :]).astype(BF16)
    position_query = (query + bias_ref[1:2, :]).astype(BF16)
    keys, grad = k_ref[0, 0], g_ref[0]
    low = p_ref[0, 0]
    weights = low.astype(F32)
    grad_weights = dot(grad, v_ref[0, 0], 1, 1)
    value_acc[...] += dot(grad, low, 0, 0)
    inner = jnp.sum(grad_weights * weights, axis=-1, keepdims=True)
    grad_raw = (weights * (grad_weights - inner) * scale).astype(BF16)
    key_acc[...] += dot(content_query, grad_raw, 0, 0)
    grad_content = dot(grad_raw, keys, 1, 0)
    row = lax.broadcasted_iota(jnp.int32, (rows, rows), 0)
    column = lax.broadcasted_iota(jnp.int32, (rows, rows), 1)
    flip = jnp.where(row + column == rows - 1, 1.0, 0.0).astype(BF16)
    span = full + rows
    start = pl.multiple_of(full - rows - block * rows, rows)
    turned = jnp.concatenate([dot(flip, grad_raw, 1, 0).astype(BF16), jnp.zeros((rows, rows), BF16)], axis=1)
    turned = pltpu.roll(turned, 0, 1, stride=1, stride_axis=0)
    turned_query = dot(flip, position_query, 1, 0).astype(BF16)
    pos_acc[:, pl.ds(start, span)] += dot(turned_query, turned, 0, 0)
    grad_turned = dot(turned, pos_ref[pl.ds(start, span), :], 1, 0)
    high = grad_turned.astype(BF16)
    rest = (grad_turned - high.astype(F32)).astype(BF16)
    grad_position = dot(flip, high, 1, 0) + dot(flip, rest, 1, 0)
    here = pl.ds(pl.multiple_of(block * rows, rows), rows)
    d_ref[0, 0, here, :] = (grad_content + grad_position).astype(BF16)
    bias_acc[0:1, :] += jnp.sum(grad_content, axis=0, keepdims=True)
    bias_acc[1:2, :] += jnp.sum(grad_position, axis=0, keepdims=True)

    @pl.when(last_block)
    def _():
        d_ref[1, 0] = key_acc[...].T.astype(BF16)
        d_ref[2, 0] = value_acc[...].T.astype(BF16)

    @pl.when(last_block & (group == pl.num_programs(1) - 1))
    def _():
        dpos_ref[...] = pos_acc[...].T.astype(BF16)
        dbias_ref[...] = bias_acc[...]

def attend_backward(probs, by_heads, grad_heads, position, bias, rows=256):
    _, groups, full, width = by_heads.shape
    depth = HEAD_WIDTH
    heads = width // depth
    body = partial(_bwd_body, rows=rows, full=full, scale=1.0 / math.sqrt(depth))
    flops = groups * heads * full * (2 * full * depth * 7 + 6 * rows * depth)
    return pl.pallas_call(
        body,
        grid_spec=pltpu.PrefetchScalarGridSpec(
            num_scalar_prefetch=0,
            grid=(heads, groups, full // rows),
            in_specs=[
                pl.BlockSpec((1, 1, rows, full), lambda h, u, i: (u, h, i, 0)),
                pl.BlockSpec((1, 1, rows, depth), lambda h, u, i: (0, u, i, h)),
                pl.BlockSpec((1, 1, full, depth), lambda h, u, i: (1, u, 0, h)),
                pl.BlockSpec((1, 1, full, depth), lambda h, u, i: (2, u, 0, h)),
                pl.BlockSpec((1, rows, depth), lambda h, u, i: (u, i, h)),
                pl.BlockSpec((2 * full, depth), lambda h, u, i: (0, h)),
                pl.BlockSpec((2, depth), lambda h, u, i: (0, h)),
            ],
            out_specs=[
                pl.BlockSpec((3, 1, full, depth), lambda h, u, i: (0, u, 0, h)),
                pl.BlockSpec((2 * full, depth), lambda h, u, i: (0, h)),
                pl.BlockSpec((2, depth), lambda h, u, i: (0, h)),
            ],
            scratch_shapes=[
                pltpu.VMEM((depth, full), F32),
                pltpu.VMEM((depth, full), F32),
                pltpu.VMEM((depth, 2 * full), F32),
                pltpu.VMEM((2, depth), F32),
            ],
        ),
        out_shape=[
            jax.ShapeDtypeStruct((3, groups, full, width), BF16),
            jax.ShapeDtypeStruct((2 * full, width), BF16),
            jax.ShapeDtypeStruct((2, width), F32),
        ],
        compiler_params=pltpu.CompilerParams(vmem_limit_bytes=48 << 20),
        cost_estimate=pl.CostEstimate(flops=flops, transcendentals=0, bytes_accessed=groups * heads * full * full * 2 + 8 * groups * full * width * 2),
        name="attend_backward",
    )(probs, by_heads, by_heads, by_heads, grad_heads, position, bias)


def extended(value, sides, width):
    for axis, dim in sides:
        size, length = (lax.axis_size(axis), value.shape[dim])
        up = [(i, (i + 1) % size) for i in range(size - 1)]
        down = [(j, i) for i, j in up]
        last = lax.slice_in_dim(value, length - width, length, axis=dim)
        initial = lax.slice_in_dim(value, 0, width, axis=dim)
        before = lax.ppermute(last, axis, up)
        after = lax.ppermute(initial, axis, down)
        value = jnp.concatenate([before, value, after], axis=dim)
    return value


def line_factors(line):
    places = [(*device.coords, device.core_on_chip) for device in line]
    moving = [first != second for first, second in zip(places[0], places[1])].index(True)
    inner = len({place[moving] for place in places})
    return len(places) // inner, inner


class Grid:
    def __init__(self, mesh):
        devices = mesh.devices
        self.a, self.b = line_factors(list(devices[:, 0]))
        self.y, self.c = line_factors(list(devices[0, :]))
        self.size = {"a": self.a, "b": self.b, "y": self.y, "c": self.c}

    def places(self):
        batch, seq = lax.axis_index("batch"), lax.axis_index("seq")
        return jnp.stack([batch // self.b, batch % self.b, seq // self.c, seq % self.c]).astype(jnp.int32)

    def shift(self, value, axis, step):
        name = "batch" if axis in "ab" else "seq"
        outer, inner = (self.a, self.b) if axis in "ab" else (self.y, self.c)
        pairs = []
        for i in range(outer):
            for j in range(inner):
                if axis in "ay":
                    pairs.append((i * inner + j, (i + step) % outer * inner + j))
                else:
                    pairs.append((i * inner + j, i * inner + (j + step) % inner))
        return lax.ppermute(value, name, pairs)


def after(value, *tokens):
    return lax.optimization_barrier((value, *tokens))[0]


def spread(grid, value, axis):
    parts = [value] + [grid.shift(value, axis, k) for k in range(1, grid.size[axis])]
    return parts


def pieces(weights, place, count, width):
    rows = []
    for weight in weights:
        wide = weight.shape[1] // count
        piece = lax.dynamic_slice_in_dim(weight, place * wide, wide, 1)
        rows += [piece[:, i : i + width] for i in range(0, wide, width)]
    return jnp.concatenate(rows, axis=0)


def _assemble_body(place_ref, mine_ref, theirs_ref, *outs, grid, plan, split):
    y, c = place_ref[2], place_ref[3]
    for out, (row, height, blocks, width) in zip(outs, plan):
        for step in range(grid.y):
            side = lax.rem(y - step + grid.y, grid.y) if split else step
            for other, source in enumerate((mine_ref, theirs_ref)):
                column = side * grid.c + lax.rem(c + other, grid.c)
                for block in range(blocks):
                    place = pl.multiple_of((column * blocks + block) * width, width)
                    out[:, pl.ds(place, width)] = source[step, 0, pl.ds(row + block * height, height), :]


def assemble(grid, places, mine, theirs, shapes, width, split, name):
    plan, row = [], 0
    columns = grid.y * grid.c
    batches = grid.a * grid.b
    for height, wide in shapes:
        blocks = wide // (columns * width)
        rows = height // batches
        plan.append((row, rows, blocks, width))
        row += rows * blocks

    def slot(i, p):
        step_a = lax.rem(p[0] - lax.div(i, grid.b) + grid.a, grid.a)
        step_b = lax.rem(p[1] - lax.rem(i, grid.b) + grid.b, grid.b)
        return (0, step_b * grid.a + step_a, 0, 0)

    piece = pl.BlockSpec((grid.y, 1, row, width), slot)
    return pl.pallas_call(
        partial(_assemble_body, grid=grid, plan=plan, split=split),
        grid_spec=pltpu.PrefetchScalarGridSpec(
            num_scalar_prefetch=1,
            grid=(batches,),
            in_specs=[piece, piece],
            out_specs=[pl.BlockSpec((h // batches, w), lambda i, p: (i, 0)) for h, w in shapes],
        ),
        out_shape=[jax.ShapeDtypeStruct(shape, BF16) for shape in shapes],
        compiler_params=pltpu.CompilerParams(vmem_limit_bytes=48 << 20),
        cost_estimate=pl.CostEstimate(flops=0, transcendentals=0, bytes_accessed=4 * sum(h * w for h, w in shapes)),
        name=name,
    )(places, mine, theirs)


def gather_weights(grid, places, weights, width, split, name, token=None):
    seq = lax.axis_index("seq")
    columns = grid.y * grid.c
    if split:
        value = pieces(weights, seq, columns, width)[None]
    else:
        core = lax.rem(seq, grid.c)
        value = jnp.stack([pieces(weights, i * grid.c + core, columns, width) for i in range(grid.y)])
    if token is not None:
        value = after(value, token)
    first = spread(grid, value, "a")
    token = first[-1]
    rows = value.shape[1]
    value = jnp.stack(first, axis=1)
    value = jnp.concatenate([v[:, None] for v in spread(grid, value, "b")], axis=1)
    if split:
        value = jnp.concatenate(spread(grid, value, "y"), axis=0)
    mine = value.reshape(grid.y, grid.b * grid.a, rows, width)
    theirs = grid.shift(mine, "c", 1)
    shapes = [(w.shape[0] * grid.a * grid.b, w.shape[1]) for w in weights]
    return assemble(grid, places, mine, theirs, shapes, width, split, name), token


def _weight_grad_body(place_ref, *refs, grid, height, first, have_sum, aliased, split, blocks):
    left_ref, right_ref = refs[:2]
    refs = refs[2:]
    sum_ref = None
    if have_sum:
        sum_ref, refs = refs[0], refs[1:]
    refs = refs[aliased:]
    outs, turned, product = refs[:-2], refs[-2], refs[-1]
    a, b = place_ref[0], place_ref[1]
    side, block = pl.program_id(0), pl.program_id(1)

    @pl.when((side == 0) & (block == 0))
    def _():
        turned[...] = left_ref[...].T

    product[...] = jnp.dot(turned[...], right_ref[...], preferred_element_type=F32)
    for step_b in range(grid.b):
        for step_a in range(grid.a):
            owner = lax.rem(a + step_a, grid.a) * grid.b + lax.rem(b + step_b, grid.b)
            part = product[pl.ds(pl.multiple_of(owner * height, height), height), :]
            if have_sum:
                part = part + sum_ref[0, step_b, step_a].astype(F32)
            part = part.astype(BF16)
            if split == "b":
                outs[step_b][0, step_a] = part
            elif split == "y":
                for k, out in enumerate(outs):

                    @pl.when(side == k)
                    def _(out=out, part=part):
                        out[step_b, step_a] = part
            else:
                outs[0][0, step_b, step_a] = part


def weight_grad(grid, places, left, right, width, core_step, total_rows, row, buffers, split, received=None, name="weight_grad", local=False, sub=None):
    samples, depth = left.shape
    height = depth // (grid.a * grid.b)
    sides = 1 if local else grid.y
    columns = 1 if local else grid.y * grid.c
    blocks = right.shape[1] // (columns * width)
    lo, count = (0, blocks) if sub is None else sub
    first = row // height

    def right_index(k, i, p):
        if local:
            return (0, 0)
        side = lax.rem(p[2] + k, grid.y)
        core = lax.rem(p[3] + core_step, grid.c)
        return (0, (side * grid.c + core) * blocks + lo + i)

    if split == "b":
        shape = (sides, grid.a, total_rows, width)
        specs = [pl.BlockSpec((1, grid.a, height, width), lambda k, i, p: (k, 0, first + i, 0))] * grid.b
        number = grid.b
    elif split == "y":
        shape = (grid.b, grid.a, total_rows, width)

        def index_of(which):
            def index(k, i, p):
                return (0, 0, first + jnp.where(k < which, 0, jnp.where(k > which, count - 1, i)), 0)

            return index

        specs = [pl.BlockSpec((grid.b, grid.a, height, width), index_of(k)) for k in range(sides)]
        number = sides
    else:
        shape = (sides, grid.b, grid.a, total_rows, width)
        specs = [pl.BlockSpec((1, grid.b, grid.a, height, width), lambda k, i, p: (k, 0, 0, first + i, 0))]
        number = 1
    in_specs = [
        pl.BlockSpec((samples, depth), lambda k, i, p: (0, 0), pipeline_mode=pl.Buffered(1)),
        pl.BlockSpec((samples, width), right_index),
    ]
    operands = [left, right]
    if received is not None:
        in_specs.append(pl.BlockSpec((1, grid.b, grid.a, height, width), lambda k, i, p: (k, 0, 0, first + i, 0)))
        operands.append(received)
    aliases = {}
    if buffers is not None:
        for i, buffer in enumerate(buffers):
            aliases[1 + len(operands)] = i
            in_specs.append(pl.BlockSpec(memory_space=pl.ANY))
            operands.append(buffer)
    body = partial(
        _weight_grad_body, grid=grid, height=height, first=first, have_sum=received is not None,
        aliased=0 if buffers is None else len(buffers), split=split, blocks=count,
    )
    work = sides * count * width
    return pl.pallas_call(
        body,
        grid_spec=pltpu.PrefetchScalarGridSpec(
            num_scalar_prefetch=1,
            grid=(sides, count),
            in_specs=in_specs,
            out_specs=specs,
            scratch_shapes=[pltpu.VMEM((depth, samples), BF16), pltpu.VMEM((depth, width), F32)],
        ),
        out_shape=[jax.ShapeDtypeStruct(shape, BF16)] * number,
        input_output_aliases=aliases,
        compiler_params=pltpu.CompilerParams(vmem_limit_bytes=48 << 20),
        cost_estimate=pl.CostEstimate(flops=2 * samples * depth * work, transcendentals=0, bytes_accessed=2 * (samples * (depth + work) + depth * work)),
        name=name,
    )(places, *operands)


def added(parts):
    total = parts[0].astype(F32)
    for part in parts[1:]:
        total = total + part.astype(F32)
    return total


def reduce_group(grid, places, pairs, width, order, name, extra=None, sub=None):
    heights = [left.shape[1] // (grid.a * grid.b) for left, _ in pairs]
    columns = grid.y * grid.c
    counts = [right.shape[1] // (columns * width) if sub is None else sub[1] for _, right in pairs]
    total = sum(h * n for h, n in zip(heights, counts))

    def products(core_step, split, received):
        buffers, row = None, 0
        for i, ((left, right), h, n) in enumerate(zip(pairs, heights, counts)):
            buffers = weight_grad(
                grid, places, left, right, width, core_step, total, row, buffers, split, received,
                name=f"{name}_{i}_{core_step}", sub=sub,
            )
            row += h * n
        return buffers

    sent = products(1, None, None)[0]
    received = grid.shift(sent, "c", 1)
    near = products(0, order, received)
    for stage, axis in enumerate(("y", "b") if order == "y" else ("b", "y")):
        if extra is not None and axis == "b":
            near = [jnp.concatenate([p, q], axis=-2) for p, q in zip(near, extra)]
        parts = [near[0]] + [grid.shift(near[k], axis, k) for k in range(1, grid.size[axis])]
        following = grid.a if stage == 1 else grid.size["b" if axis == "y" else "y"]
        near = [added([p[k] for p in parts]).astype(BF16) for k in range(following)]
    parts = [near[0]] + [grid.shift(near[k], "a", k) for k in range(1, grid.a)]
    return added(parts)


def layer_norm(values, scale_row, shift_row):
    center = values - jnp.mean(values, axis=-1, keepdims=True)
    spread = jnp.mean(center * center, axis=-1, keepdims=True)
    return center * lax.rsqrt(spread + epsilon) * scale_row + shift_row


def glu_gate(gated_rows):
    half_width = gated_rows.shape[-1] // 2
    return gated_rows[..., :half_width] * jax.nn.sigmoid(gated_rows[..., half_width:])


def batch_norm(conv_value, sum_first, sum_second, scale_row, shift_row, count_all):
    center = sum_first / count_all
    spread = sum_second / count_all - center * center
    return (conv_value - center) * lax.rsqrt(spread + epsilon) * scale_row + shift_row


def position_table(length, model_width):
    fine = 64
    coarse = 2 * length // fine
    column = jnp.arange(model_width, dtype=jnp.int32)
    rates = jnp.exp((column // 2).astype(jnp.float32) * (-2.0 * math.log(10000.0) / model_width))
    odd = (column % 2 == 1)[None, :]
    start = (jnp.arange(coarse, dtype=jnp.int32) * fine - (length - 1)).astype(jnp.float32)
    large = start[:, None] * rates[None, :]
    small = jnp.arange(fine, dtype=jnp.int32).astype(jnp.float32)[:, None] * rates[None, :]
    sin_large, cos_large = jnp.sin(large), jnp.cos(large)
    first = jnp.where(odd, cos_large, sin_large)[:, None, :]
    second = jnp.where(odd, -sin_large, cos_large)[:, None, :]
    table = first * jnp.cos(small)[None] + second * jnp.sin(small)[None]
    return table.astype(jnp.bfloat16).reshape(2 * length, model_width)


def depth_conv(padded, kernel_rows, length):
    result = kernel_rows[0] * padded[:, 0:length]
    for offset in range(1, kernel_rows.shape[0]):
        result = result + kernel_rows[offset] * padded[:, offset : offset + length]
    return result


def depth_conv_back(padded_grad, kernel_rows, length):
    last_tap = kernel_rows.shape[0] - 1
    result = kernel_rows[0] * padded_grad[:, last_tap : last_tap + length]
    for offset in range(1, last_tap + 1):
        result = (
            result
            + kernel_rows[offset] * padded_grad[:, last_tap - offset : last_tap - offset + length]
        )
    return result


def matmul_rows(left_side, right_side):
    return jnp.dot(left_side, right_side, preferred_element_type=jnp.float32)


def times_transpose(left_side, right_side):
    return lax.dot_general(
        left_side, right_side, (((1,), (1,)), ((), ())), preferred_element_type=jnp.float32
    )


def transpose_times(left_side, right_side):
    return lax.dot_general(
        left_side, right_side, (((0,), (0,)), ((), ())), preferred_element_type=jnp.float32
    )


def linear_back(grad_rows, weight):
    grad_low = grad_rows.astype(jnp.bfloat16)
    return (times_transpose(grad_low, weight), grad_low)


def ffn_forward(values, scale_row, shift_row, weight_in, weight_out):
    normed_low = layer_norm(values, scale_row, shift_row).astype(jnp.bfloat16)
    hidden_pre = matmul_rows(normed_low, weight_in)
    hidden_low = jax.nn.silu(hidden_pre).astype(jnp.bfloat16)
    return (matmul_rows(hidden_low, weight_out), (normed_low, hidden_pre, hidden_low))


def ffn_backward(grad_rows, values, scale_row, shift_row, weight_in, weight_out, saved_parts):
    normed_low, hidden_pre, hidden_low = saved_parts
    grad_hidden, grad_out_low = linear_back(grad_rows, weight_out)
    silu_value, silu_back = jax.vjp(jax.nn.silu, hidden_pre)
    grad_pre = silu_back(grad_hidden)[0]
    grad_normed, grad_pre_low = linear_back(grad_pre, weight_in)
    norm_value, norm_back = jax.vjp(layer_norm, values, scale_row, shift_row)
    grad_values, grad_scale, grad_shift = norm_back(grad_normed)
    return (grad_values, grad_scale, grad_shift, grad_pre_low, grad_out_low)


def sum_everywhere(value):
    for axis in ("seq", "batch"):
        size, step = lax.axis_size(axis), 1
        while step < size:
            value = value + lax.ppermute(value, axis, [(i, i ^ step) for i in range(size)])
            step *= 2
    return value


def gather_small(grid, places, shard):
    value = jnp.stack(spread(grid, shard, "a"))
    value = jnp.concatenate(spread(grid, value[None], "b"))
    value = value.reshape(grid.b * grid.a, *shard.shape)
    owner = jnp.arange(grid.a * grid.b, dtype=jnp.int32)
    step_a = (places[0] - owner // grid.b) % grid.a
    step_b = (places[1] - owner % grid.b) % grid.b
    value = jnp.take(value, step_b * grid.a + step_a, axis=0)
    return value.transpose(1, 0, 2).reshape(shard.shape[0], -1)


def per_device(
    grid,
    acoustic_sequence,
    utterance_durations,
    chosen_entry_number,
    discretizer_score_perturbation,
    softmax_heat,
    normalizer_affine_rows,
    discretizer_score_projection,
    lexicon_vectors,
    opening_dense_entry_projection,
    opening_dense_exit_projection,
    request_projection,
    lookup_projection,
    content_projection_kernel,
    relative_offset_projection,
    mixing_exit_projection,
    unit_kernel_before_gating,
    channelwise_filter_coefficients,
    unit_kernel_after_normalizing,
    closing_dense_entry_projection,
    closing_dense_exit_projection,
    result_adjoint,
    discrete_label_adjoint,
):
    places = grid.places()
    small_all = gather_small(
        grid,
        places,
        jnp.concatenate([normalizer_affine_rows, channelwise_filter_coefficients], axis=0),
    )
    vector_rows = normalizer_affine_rows.shape[0]
    vectors_all, depth_all = small_all[:vector_rows], small_all[vector_rows:]
    piece_width = acoustic_sequence.shape[2] // (grid.y * grid.c)
    gather = partial(gather_weights, grid, places)
    (macaron_in_all,), token = gather(
        [opening_dense_entry_projection], piece_width, True, "gather_opening_entry"
    )
    (macaron_out_all,), token = gather(
        [opening_dense_exit_projection], piece_width, True, "gather_opening_exit", token
    )
    (query_all, key_all, value_all, pos_all), token = gather(
        [request_projection, lookup_projection, content_projection_kernel, relative_offset_projection],
        piece_width,
        True,
        "gather_attention",
        token,
    )
    (out_all, conv_in_all, conv_out_all, quant_all, codebook_all), token = gather(
        [
            mixing_exit_projection,
            unit_kernel_before_gating,
            unit_kernel_after_normalizing,
            discretizer_score_projection,
            lexicon_vectors,
        ],
        piece_width,
        True,
        "gather_convolution",
        token,
    )
    (closing_in_all, closing_out_all), token = gather(
        [closing_dense_entry_projection, closing_dense_exit_projection],
        piece_width,
        False,
        "gather_closing",
        token,
    )
    groups, local_len, model_width = acoustic_sequence.shape
    seq_count = lax.axis_size("seq")
    seq_place = lax.axis_index("seq")
    full_len = local_len * seq_count
    entries = codebook_all.shape[0]
    total_rows = groups * local_len
    local_width = model_width // seq_count
    kernel_size = depth_all.shape[0]
    rim_width = kernel_size // 2
    params_f = vectors_all.astype(jnp.float32)
    depth_f = depth_all.astype(jnp.float32)
    positions = seq_place * local_len + jnp.arange(local_len, dtype=jnp.int32)
    valid_mask = (positions[None, :] < utterance_durations[:, None]).astype(jnp.float32)
    valid_rows = valid_mask.reshape(total_rows, 1)
    inputs_low = acoustic_sequence.reshape(total_rows, model_width)
    inputs_f = inputs_low.astype(jnp.float32)
    quant_logits = matmul_rows(inputs_low, quant_all)
    scaled_logits = (
        quant_logits
        + discretizer_score_perturbation.reshape(total_rows, entries).astype(jnp.float32)
    ) / softmax_heat
    relaxed_assignments = jax.nn.softmax(scaled_logits, axis=-1)
    soft_low = relaxed_assignments.astype(jnp.bfloat16)
    one_hot = (
        chosen_entry_number.reshape(total_rows, 1) == jnp.arange(entries, dtype=jnp.int32)[None, :]
    ).astype(jnp.bfloat16)
    codes_value = valid_rows * (
        matmul_rows(one_hot, codebook_all) + matmul_rows(soft_low, codebook_all)
    )
    macaron_value, macaron_saved = ffn_forward(
        inputs_f, params_f[0], params_f[5], macaron_in_all, macaron_out_all
    )
    first_mid = inputs_f + 0.5 * macaron_value
    attn_normed = layer_norm(first_mid, params_f[1], params_f[6]).astype(jnp.bfloat16)
    stacked = (
        jnp.stack(
            [
                matmul_rows(attn_normed, query_all),
                matmul_rows(attn_normed, key_all),
                matmul_rows(attn_normed, value_all),
            ]
        )
        .astype(jnp.bfloat16)
        .reshape(3, groups, local_len, model_width)
    )
    by_heads = lax.all_to_all(stacked, "seq", split_axis=3, concat_axis=2, tiled=True)
    table_low = position_table(full_len, model_width)
    pos_columns = lax.dynamic_slice_in_dim(pos_all, seq_place * local_width, local_width, 1)
    position_low = matmul_rows(table_low, pos_columns).astype(jnp.bfloat16)
    biases = lax.dynamic_slice_in_dim(params_f[12:14], seq_place * local_width, local_width, 1)
    attended_low, probs = attend_forward(by_heads, position_low, biases, utterance_durations)
    back_time = lax.all_to_all(
        attended_low,
        "seq",
        split_axis=1,
        concat_axis=2,
        tiled=True,
    )
    attended_rows = back_time.reshape(total_rows, model_width)
    second_mid = first_mid + matmul_rows(attended_rows, out_all)
    conv_normed = layer_norm(second_mid, params_f[2], params_f[7]).astype(jnp.bfloat16)
    gated_rows = matmul_rows(conv_normed, conv_in_all)
    glu_low = (
        (valid_rows * glu_gate(gated_rows))
        .astype(jnp.bfloat16)
        .reshape(groups, local_len, model_width)
    )
    padded_glu = extended(glu_low, (("seq", 1),), rim_width)
    conv_value = depth_conv(padded_glu, depth_f, local_len).reshape(total_rows, model_width)
    masked_conv = valid_rows * conv_value
    sums = sum_everywhere(
        jnp.stack(
            [
                jnp.sum(masked_conv, axis=0),
                jnp.sum(masked_conv * conv_value, axis=0),
                jnp.broadcast_to(jnp.sum(valid_mask), (model_width,)),
            ]
        )
    )
    sum_first, sum_second, count_all = sums[0], sums[1], sums[2]
    bound_norm = partial(batch_norm, count_all=count_all)
    normalized = bound_norm(conv_value, sum_first, sum_second, params_f[10], params_f[11])
    act_low = jax.nn.silu(normalized).astype(jnp.bfloat16)
    third_mid = second_mid + matmul_rows(act_low, conv_out_all)
    closing_value, closing_saved = ffn_forward(
        third_mid, params_f[3], params_f[8], closing_in_all, closing_out_all
    )
    fourth_mid = third_mid + 0.5 * closing_value
    final_value, final_back = jax.vjp(layer_norm, fourth_mid, params_f[4], params_f[9])
    output = (valid_rows * final_value).astype(jnp.bfloat16).reshape(groups, local_len, model_width)
    codes = codes_value.astype(jnp.bfloat16).reshape(groups, local_len, model_width)
    grad_final = valid_rows * result_adjoint.reshape(total_rows, model_width).astype(jnp.float32)
    grad_fourth, scale_four, shift_four = final_back(grad_final)
    grad_closing, scale_three, shift_three, close_pre_low, close_out_low = ffn_backward(
        0.5 * grad_fourth,
        third_mid,
        params_f[3],
        params_f[8],
        closing_in_all,
        closing_out_all,
        closing_saved,
    )
    grad_third = grad_fourth + grad_closing
    grad_act, grad_third_low = linear_back(grad_third, conv_out_all)
    silu_value, silu_back = jax.vjp(jax.nn.silu, normalized)
    grad_normalized = silu_back(grad_act)[0]
    norm_value, norm_back = jax.vjp(
        bound_norm, conv_value, sum_first, sum_second, params_f[10], params_f[11]
    )
    grad_conv_direct, part_first, part_second, grad_bn_scale, grad_bn_shift = norm_back(
        grad_normalized
    )
    total_first, total_second = sum_everywhere(jnp.stack([part_first, part_second]))
    grad_conv = grad_conv_direct + valid_rows * (total_first + 2.0 * conv_value * total_second)
    grad_conv_low = grad_conv.astype(jnp.bfloat16).reshape(groups, local_len, model_width)
    padded_grad = extended(grad_conv_low, (("seq", 1),), rim_width)
    grad_glu = valid_rows * depth_conv_back(padded_grad, depth_f, local_len).reshape(
        total_rows, model_width
    )
    grad_conv_float = grad_conv_low.astype(jnp.float32)
    grad_depth = jnp.stack(
        [
            jnp.sum(
                padded_glu[:, offset : offset + local_len].astype(jnp.float32) * grad_conv_float,
                axis=(0, 1),
            )
            for offset in range(kernel_size)
        ]
    )
    glu_value, glu_back = jax.vjp(glu_gate, gated_rows)
    grad_gated = glu_back(grad_glu)[0]
    grad_conv_normed, grad_gated_low = linear_back(grad_gated, conv_in_all)
    conv_norm_value, conv_norm_back = jax.vjp(layer_norm, second_mid, params_f[2], params_f[7])
    grad_from_conv, scale_two, shift_two = conv_norm_back(grad_conv_normed)
    grad_second = grad_third + grad_from_conv
    grad_attended, grad_second_low = linear_back(grad_second, out_all)
    grad_heads = lax.all_to_all(
        grad_second_low_heads(grad_attended, groups, local_len, model_width),
        "seq",
        split_axis=2,
        concat_axis=1,
        tiled=True,
    )

    grad_stack, grad_position_low, grad_biases = attend_backward(
        probs, by_heads, grad_heads, position_low, biases
    )
    grad_time = lax.all_to_all(grad_stack, "seq", split_axis=2, concat_axis=3, tiled=True).reshape(
        3, total_rows, model_width
    )
    grad_attn_normed = (
        times_transpose(grad_time[0], query_all)
        + times_transpose(grad_time[1], key_all)
        + times_transpose(grad_time[2], value_all)
    )
    attn_norm_value, attn_norm_back = jax.vjp(layer_norm, first_mid, params_f[1], params_f[6])
    grad_from_attn, scale_one, shift_one = attn_norm_back(grad_attn_normed)
    grad_first = grad_second + grad_from_attn
    content_full, position_full = lax.dynamic_update_slice_in_dim(
        jnp.zeros((2, model_width), jnp.float32), grad_biases, seq_place * local_width, 1
    )
    grad_macaron, scale_zero, shift_zero, mac_pre_low, mac_out_low = ffn_backward(
        0.5 * grad_first,
        inputs_f,
        params_f[0],
        params_f[5],
        macaron_in_all,
        macaron_out_all,
        macaron_saved,
    )
    grad_layer_in = grad_first + grad_macaron
    grad_codes = (
        valid_rows * discrete_label_adjoint.reshape(total_rows, model_width).astype(jnp.float32)
    ).astype(jnp.bfloat16)
    grad_soft = times_transpose(grad_codes, codebook_all)
    rescaled_derivative = relaxed_assignments * (
        grad_soft - jnp.sum(grad_soft * relaxed_assignments, axis=-1, keepdims=True)
    )
    score_derivative_lowprecision = (rescaled_derivative / softmax_heat).astype(jnp.bfloat16)
    grad_quant_in = times_transpose(score_derivative_lowprecision, quant_all)
    frames_grad = (
        (grad_layer_in + grad_quant_in).astype(jnp.bfloat16).reshape(groups, local_len, model_width)
    )
    vectors_grad = jnp.stack(
        [
            scale_zero,
            scale_one,
            scale_two,
            scale_three,
            scale_four,
            shift_zero,
            shift_one,
            shift_two,
            shift_three,
            shift_four,
            grad_bn_scale,
            grad_bn_shift,
            content_full,
            position_full,
        ]
    )
    small_sums = sum_everywhere(jnp.concatenate([vectors_grad, grad_depth], axis=0))
    small_width = model_width // (grid.a * grid.b)
    small_sums = lax.dynamic_slice_in_dim(
        small_sums, lax.axis_index("batch") * small_width, small_width, 1
    )
    vectors_sum, depth_sum = small_sums[:vector_rows], small_sums[vector_rows:]
    mac_normed, mac_pre, mac_hidden = macaron_saved
    close_normed, close_pre, close_hidden = closing_saved
    reduce = partial(reduce_group, grid, places)
    height = model_width // (grid.a * grid.b)
    closing_out_sum = reduce([(close_hidden, close_out_low)], piece_width, "y", "closing_exit")
    closing_in_sum = reduce([(close_normed, close_pre_low)], piece_width, "b", "closing_entry")
    chosen_soft = one_hot + soft_low
    first_sums = reduce(
        [
            (inputs_low, score_derivative_lowprecision),
            (chosen_soft, grad_codes),
            (act_low, grad_third_low),
        ],
        piece_width,
        "y",
        "quantizer",
    )
    quant_sum, codebook_sum, conv_out_sum = (first_sums[i * height : (i + 1) * height] for i in range(3))
    second_sums = reduce(
        [(conv_normed, grad_gated_low), (attended_rows, grad_second_low)], piece_width, "b", "convolution"
    )
    conv_in_sum, out_sum = second_sums[: 2 * height], second_sums[2 * height :]
    position_parts = weight_grad(
        grid, places, table_low, grad_position_low, piece_width, 0, height, 0, None, "b",
        name="position_grad", local=True,
    )
    third_sums = reduce(
        [(attn_normed, grad_time[i]) for i in range(3)],
        piece_width,
        "y",
        "attention",
        extra=[part[0] for part in position_parts],
    )
    query_sum, key_sum, value_sum, pos_sum = (third_sums[i * height : (i + 1) * height] for i in range(4))
    macaron_out_sum = reduce([(mac_hidden, mac_out_low)], piece_width, "b", "opening_exit")
    macaron_in_sum = reduce([(mac_normed, mac_pre_low)], piece_width, "y", "opening_entry")

    def side_by_side(blocks):
        return jnp.concatenate(
            [blocks[i : i + height] for i in range(0, blocks.shape[0], height)], axis=1
        )

    closing_in_sum, conv_in_sum, macaron_in_sum = (
        side_by_side(closing_in_sum),
        side_by_side(conv_in_sum),
        side_by_side(macaron_in_sum),
    )
    return (
        output,
        codes,
        frames_grad,
        vectors_sum,
        quant_sum,
        codebook_sum,
        macaron_in_sum,
        macaron_out_sum,
        query_sum,
        key_sum,
        value_sum,
        pos_sum,
        out_sum,
        conv_in_sum,
        depth_sum,
        conv_out_sum,
        closing_in_sum,
        closing_out_sum,
    )


def grad_second_low_heads(grad_attended, groups, local_len, model_width):
    return grad_attended.astype(jnp.bfloat16).reshape(groups, local_len, model_width)


def solution(mesh):
    placed = (
        P("batch", "seq", None),
        P("batch"),
        P("batch", "seq"),
        P("batch", "seq", None),
        P(),
        P(None, "batch"),
        P("batch", None),
        P("batch", None),
        P("batch", None),
        P("batch", None),
        P("batch", None),
        P("batch", None),
        P("batch", None),
        P("batch", None),
        P("batch", None),
        P("batch", None),
        P(None, "batch"),
        P("batch", None),
        P("batch", None),
        P("batch", None),
        P("batch", "seq", None),
        P("batch", "seq", None),
    )
    return jax.shard_map(
        partial(per_device, Grid(mesh)),
        mesh=mesh,
        in_specs=placed,
        out_specs=(
            P("batch", "seq", None),
            P("batch", "seq", None),
            P("batch", "seq", None),
            P(None, "batch"),
            P("batch", "seq"),
            P("batch", "seq"),
            P("batch", "seq"),
            P("batch", "seq"),
            P("batch", "seq"),
            P("batch", "seq"),
            P("batch", "seq"),
            P("batch", "seq"),
            P("batch", "seq"),
            P("batch", "seq"),
            P(None, "batch"),
            P("batch", "seq"),
            P("batch", "seq"),
            P("batch", "seq"),
        ),
        check_vma=False,
    )
```

```python
from functools import partial
import math

import jax
import jax.numpy as jnp
from jax import lax
from jax.experimental import pallas as pl
from jax.experimental.pallas import tpu as pltpu
from jax.sharding import PartitionSpec as P

HEAD_WIDTH = 128


epsilon = 1e-05

F32, BF16 = jnp.float32, jnp.bfloat16

def dot(a, b, ca, cb):
    return lax.dot_general(a, b, (((ca,), (cb,)), ((), ())), preferred_element_type=F32)

def _fwd_body(len_ref, q_ref, k_ref, v_ref, pos_ref, bias_ref, o_ref, p_ref, *, rows, full, scale):
    block = pl.program_id(2)
    length = len_ref[pl.program_id(0)]
    query = q_ref[0, 0, 0].astype(F32)
    content_query = (query + bias_ref[0:1, :]).astype(BF16)
    position_query = (query + bias_ref[1:2, :]).astype(BF16)
    content = dot(content_query, k_ref[:, 0, 0].reshape(full, -1), 1, 1)
    span = full + rows
    start = pl.multiple_of(full - rows - block * rows, rows)
    relative = dot(position_query, pos_ref[pl.ds(start, span), :], 1, 1)
    relative = pltpu.roll(relative, span - (rows - 1), 1, stride=1, stride_axis=0)
    raw = content + relative[:, :full]
    seen = lax.broadcasted_iota(jnp.int32, raw.shape, 1) < length
    scores = jnp.where(seen, raw * scale, -1e30)
    top = jnp.max(scores, axis=-1, keepdims=True)
    weights = jnp.exp(scores - top)
    total = jnp.sum(weights, axis=-1, keepdims=True)
    low = (weights * (1.0 / total)).astype(BF16)
    p_ref[0, 0] = low
    o_ref[0, 0] = dot(low, v_ref[:, 0, 0].reshape(full, -1), 1, 0).astype(BF16)

def attend_forward(by_heads, position, bias, lengths):
    parts, _, groups, rows, width = by_heads.shape
    depth, full = HEAD_WIDTH, parts * rows
    heads = width // depth
    body = partial(_fwd_body, rows=rows, full=full, scale=1.0 / math.sqrt(depth))
    flops = groups * heads * full * (2 * full * depth * 3 + 2 * rows * depth)
    return pl.pallas_call(
        body,
        grid_spec=pltpu.PrefetchScalarGridSpec(
            num_scalar_prefetch=1,
            grid=(groups, heads, parts),
            in_specs=[
                pl.BlockSpec((1, 1, 1, rows, depth), lambda u, h, i, n: (i, 0, u, 0, h)),
                pl.BlockSpec((parts, 1, 1, rows, depth), lambda u, h, i, n: (0, 1, u, 0, h)),
                pl.BlockSpec((parts, 1, 1, rows, depth), lambda u, h, i, n: (0, 2, u, 0, h)),
                pl.BlockSpec((2 * full, depth), lambda u, h, i, n: (0, h)),
                pl.BlockSpec((2, depth), lambda u, h, i, n: (0, h)),
            ],
            out_specs=[
                pl.BlockSpec((1, 1, rows, depth), lambda u, h, i, n: (i, u, 0, h)),
                pl.BlockSpec((1, 1, rows, full), lambda u, h, i, n: (u, h, i, 0)),
            ],
        ),
        out_shape=[
            jax.ShapeDtypeStruct((parts, groups, rows, width), BF16),
            jax.ShapeDtypeStruct((groups, heads, full, full), BF16),
        ],
        compiler_params=pltpu.CompilerParams(vmem_limit_bytes=48 << 20),
        cost_estimate=pl.CostEstimate(flops=flops, transcendentals=groups * heads * full * full, bytes_accessed=groups * heads * full * full * 2 + 5 * groups * full * width * 2),
        name="attend_forward",
    )(lengths, by_heads, by_heads, by_heads, position, bias)

def _bwd_body(p_ref, q_ref, k_ref, v_ref, g_ref, pos_ref, bias_ref, d_ref, dpos_ref, dbias_ref,
              key_acc, value_acc, pos_acc, bias_acc, *, rows, full, scale):
    group, block = pl.program_id(1), pl.program_id(2)
    last_block = block == pl.num_programs(2) - 1

    @pl.when((group == 0) & (block == 0))
    def _():
        pos_acc[...] = jnp.zeros_like(pos_acc)
        bias_acc[...] = jnp.zeros_like(bias_acc)

    @pl.when(block == 0)
    def _():
        key_acc[...] = jnp.zeros_like(key_acc)
        value_acc[...] = jnp.zeros_like(value_acc)

    query = q_ref[0, 0, 0].astype(F32)
    content_query = (query + bias_ref[0:1, :]).astype(BF16)
    position_query = (query + bias_ref[1:2, :]).astype(BF16)
    keys, values, grad = k_ref[:, 0, 0].reshape(full, -1), v_ref[:, 0, 0].reshape(full, -1), g_ref[0, 0]
    low = p_ref[0, 0]
    weights = low.astype(F32)
    grad_weights = dot(grad, values, 1, 1)
    value_acc[...] += dot(grad, low, 0, 0)
    inner = jnp.sum(grad_weights * weights, axis=-1, keepdims=True)
    grad_raw = (weights * (grad_weights - inner) * scale).astype(BF16)
    key_acc[...] += dot(content_query, grad_raw, 0, 0)
    grad_content = dot(grad_raw, keys, 1, 0)
    row = lax.broadcasted_iota(jnp.int32, (rows, rows), 0)
    column = lax.broadcasted_iota(jnp.int32, (rows, rows), 1)
    flip = jnp.where(row + column == rows - 1, 1.0, 0.0).astype(BF16)
    span = full + rows
    start = pl.multiple_of(full - rows - block * rows, rows)
    turned = jnp.concatenate([dot(flip, grad_raw, 1, 0).astype(BF16), jnp.zeros((rows, rows), BF16)], axis=1)
    turned = pltpu.roll(turned, 0, 1, stride=1, stride_axis=0)
    turned_query = dot(flip, position_query, 1, 0).astype(BF16)
    pos_acc[:, pl.ds(start, span)] += dot(turned_query, turned, 0, 0)
    grad_turned = dot(turned, pos_ref[pl.ds(start, span), :], 1, 0)
    high = grad_turned.astype(BF16)
    rest = (grad_turned - high.astype(F32)).astype(BF16)
    grad_position = dot(flip, high, 1, 0) + dot(flip, rest, 1, 0)
    d_ref[block, 0, 0] = (grad_content + grad_position).astype(BF16)
    bias_acc[0:1, :] += jnp.sum(grad_content, axis=0, keepdims=True)
    bias_acc[1:2, :] += jnp.sum(grad_position, axis=0, keepdims=True)

    @pl.when(last_block)
    def _():
        d_ref[:, 1, 0] = key_acc[...].T.astype(BF16).reshape(full // rows, rows, -1)
        d_ref[:, 2, 0] = value_acc[...].T.astype(BF16).reshape(full // rows, rows, -1)

    @pl.when(last_block & (group == pl.num_programs(1) - 1))
    def _():
        dpos_ref[...] = pos_acc[...].T.astype(BF16)
        dbias_ref[...] = bias_acc[...]

def attend_backward(probs, by_heads, grad_heads, position, bias):
    parts, _, groups, rows, width = by_heads.shape
    depth, full = HEAD_WIDTH, parts * rows
    heads = width // depth
    body = partial(_bwd_body, rows=rows, full=full, scale=1.0 / math.sqrt(depth))
    flops = groups * heads * full * (2 * full * depth * 7 + 6 * rows * depth)
    return pl.pallas_call(
        body,
        grid_spec=pltpu.PrefetchScalarGridSpec(
            num_scalar_prefetch=0,
            grid=(heads, groups, parts),
            in_specs=[
                pl.BlockSpec((1, 1, rows, full), lambda h, u, i: (u, h, i, 0)),
                pl.BlockSpec((1, 1, 1, rows, depth), lambda h, u, i: (i, 0, u, 0, h)),
                pl.BlockSpec((parts, 1, 1, rows, depth), lambda h, u, i: (0, 1, u, 0, h)),
                pl.BlockSpec((parts, 1, 1, rows, depth), lambda h, u, i: (0, 2, u, 0, h)),
                pl.BlockSpec((1, 1, rows, depth), lambda h, u, i: (i, u, 0, h)),
                pl.BlockSpec((2 * full, depth), lambda h, u, i: (0, h)),
                pl.BlockSpec((2, depth), lambda h, u, i: (0, h)),
            ],
            out_specs=[
                pl.BlockSpec((parts, 3, 1, rows, depth), lambda h, u, i: (0, 0, u, 0, h)),
                pl.BlockSpec((2 * full, depth), lambda h, u, i: (0, h)),
                pl.BlockSpec((2, depth), lambda h, u, i: (0, h)),
            ],
            scratch_shapes=[
                pltpu.VMEM((depth, full), F32),
                pltpu.VMEM((depth, full), F32),
                pltpu.VMEM((depth, 2 * full), F32),
                pltpu.VMEM((2, depth), F32),
            ],
        ),
        out_shape=[
            jax.ShapeDtypeStruct((parts, 3, groups, rows, width), BF16),
            jax.ShapeDtypeStruct((2 * full, width), BF16),
            jax.ShapeDtypeStruct((2, width), F32),
        ],
        compiler_params=pltpu.CompilerParams(vmem_limit_bytes=48 << 20),
        cost_estimate=pl.CostEstimate(flops=flops, transcendentals=0, bytes_accessed=groups * heads * full * full * 2 + 8 * groups * full * width * 2),
        name="attend_backward",
    )(probs, by_heads, by_heads, by_heads, grad_heads, position, bias)


def extended(value, sides, width):
    for axis, dim in sides:
        size, length = (lax.axis_size(axis), value.shape[dim])
        up = [(i, (i + 1) % size) for i in range(size - 1)]
        down = [(j, i) for i, j in up]
        last = lax.slice_in_dim(value, length - width, length, axis=dim)
        initial = lax.slice_in_dim(value, 0, width, axis=dim)
        before = lax.ppermute(last, axis, up)
        after = lax.ppermute(initial, axis, down)
        value = jnp.concatenate([before, value, after], axis=dim)
    return value


def _project_body(left_ref, *refs):
    out = refs[-1]
    for i, weight in enumerate(refs[:-1]):
        out[0, i] = dot(left_ref[...], weight[...], 1, 0).astype(BF16).reshape(out.shape[2:])


def project_heads(left, weights, groups, parts):
    rows, depth = left.shape
    width = weights[0].shape[1] // parts
    shape = (parts, len(weights), groups, rows // groups, width)
    return pl.pallas_call(
        _project_body,
        grid=(parts,),
        in_specs=[pl.BlockSpec((rows, depth), lambda s: (0, 0))]
        + [pl.BlockSpec((depth, width), lambda s: (0, s))] * len(weights),
        out_specs=pl.BlockSpec((1, *shape[1:]), lambda s: (s, 0, 0, 0, 0)),
        out_shape=jax.ShapeDtypeStruct(shape, BF16),
        compiler_params=pltpu.CompilerParams(vmem_limit_bytes=48 << 20),
        cost_estimate=pl.CostEstimate(flops=2 * rows * depth * width * parts * len(weights), transcendentals=0, bytes_accessed=2 * len(weights) * (rows + depth) * width * parts + 2 * rows * depth),
        name="project_heads",
    )(left, *weights)


def _unproject_body(left_ref, weight_ref, out_ref):
    out_ref[0] = dot(left_ref[...], weight_ref[...], 1, 1).astype(BF16).reshape(out_ref.shape[1:])


def unproject_heads(left, weight, groups, parts):
    rows, depth = left.shape
    width = weight.shape[0] // parts
    shape = (parts, groups, rows // groups, width)
    return pl.pallas_call(
        _unproject_body,
        grid=(parts,),
        in_specs=[
            pl.BlockSpec((rows, depth), lambda s: (0, 0)),
            pl.BlockSpec((width, depth), lambda s: (s, 0)),
        ],
        out_specs=pl.BlockSpec((1, *shape[1:]), lambda s: (s, 0, 0, 0)),
        out_shape=jax.ShapeDtypeStruct(shape, BF16),
        compiler_params=pltpu.CompilerParams(vmem_limit_bytes=48 << 20),
        cost_estimate=pl.CostEstimate(flops=2 * rows * depth * width * parts, transcendentals=0, bytes_accessed=2 * (rows + depth) * width * parts + 2 * rows * depth),
        name="unproject_heads",
    )(left, weight)


def _join_body(grad_ref, *refs):
    out = refs[-1]

    @pl.when(pl.program_id(0) == 0)
    def _():
        out[...] = jnp.zeros_like(out)

    total = out[...]
    for i, weight in enumerate(refs[:-1]):
        total = total + dot(grad_ref[0, i].reshape(out.shape[0], -1), weight[...], 1, 1)
    out[...] = total


def join_heads(grads, weights):
    parts, count, groups, frames, width = grads.shape
    rows, depth = groups * frames, weights[0].shape[0]
    return pl.pallas_call(
        _join_body,
        grid=(parts,),
        in_specs=[pl.BlockSpec((1, count, groups, frames, width), lambda s: (s, 0, 0, 0, 0))]
        + [pl.BlockSpec((depth, width), lambda s: (0, s))] * count,
        out_specs=pl.BlockSpec((rows, depth), lambda s: (0, 0)),
        out_shape=jax.ShapeDtypeStruct((rows, depth), F32),
        compiler_params=pltpu.CompilerParams(vmem_limit_bytes=48 << 20),
        cost_estimate=pl.CostEstimate(flops=2 * rows * depth * width * parts * count, transcendentals=0, bytes_accessed=2 * count * (rows + depth) * width * parts + 4 * rows * depth),
        name="join_heads",
    )(grads, *weights)


def line_factors(line):
    places = [(*device.coords, device.core_on_chip) for device in line]
    moving = [first != second for first, second in zip(places[0], places[1])].index(True)
    inner = len({place[moving] for place in places})
    return len(places) // inner, inner


class Grid:
    def __init__(self, mesh):
        devices = mesh.devices
        self.a, self.b = line_factors(list(devices[:, 0]))
        self.y, self.c = line_factors(list(devices[0, :]))
        self.size = {"a": self.a, "b": self.b, "y": self.y, "c": self.c}
        self.bits = self.a.bit_length() - 1

    def places(self):
        batch, seq = lax.axis_index("batch"), lax.axis_index("seq")
        return jnp.stack([batch // self.b, batch % self.b, seq // self.c, seq % self.c]).astype(jnp.int32)

    def shift(self, value, axis, step):
        name = "batch" if axis in "ab" else "seq"
        outer, inner = (self.a, self.b) if axis in "ab" else (self.y, self.c)
        pairs = []
        for i in range(outer):
            for j in range(inner):
                if axis in "ay":
                    pairs.append((i * inner + j, (i + step) % outer * inner + j))
                else:
                    pairs.append((i * inner + j, i * inner + (j + step) % inner))
        return lax.ppermute(value, name, pairs)

    def swap(self, value, step):
        pairs = [
            (i * self.b + j, (i ^ step) * self.b + j) for i in range(self.a) for j in range(self.b)
        ]
        return lax.ppermute(value, "batch", pairs)


def after(value, *tokens):
    return lax.optimization_barrier((value, *tokens))[0]


def settle(jobs, *tokens, hold=()):
    flights = tuple(tuple(job.flight) for job in jobs)
    parts = tuple(tuple(job.parts) for job in hold)
    landed, tokens, parts = lax.optimization_barrier((flights, tokens, parts))
    for job, held in zip(hold, parts):
        job.parts = list(held)
    for job, flight in zip(jobs, landed):
        job.flight = list(flight)
        job.land()
    return tokens[0] if len(tokens) == 1 else tokens


def bit_reversed(value, bits):
    return sum((value >> i & 1) << (bits - 1 - i) for i in range(bits))


def spread(grid, value, axis):
    return [value] + [grid.shift(value, axis, k) for k in range(1, grid.size[axis])]


def pieces(weights, place, count, width):
    rows = []
    for weight in weights:
        wide = weight.shape[1] // count
        piece = lax.dynamic_slice_in_dim(weight, place * wide, wide, 1)
        rows += [piece[:, i : i + width] for i in range(0, wide, width)]
    return jnp.concatenate(rows, axis=0)


def _assemble_body(place_ref, mine_ref, theirs_ref, *outs, grid, plan, split):
    y, c = place_ref[2], place_ref[3]
    for out, (row, height, blocks, width) in zip(outs, plan):
        for step in range(grid.y):
            side = lax.rem(y - step + grid.y, grid.y) if split else step
            for other, source in enumerate((mine_ref, theirs_ref)):
                column = side * grid.c + lax.rem(c + other, grid.c)
                for block in range(blocks):
                    place = pl.multiple_of((column * blocks + block) * width, width)
                    out[:, pl.ds(place, width)] = source[step, 0, pl.ds(row + block * height, height), :]


def assemble(grid, places, mine, theirs, shapes, width, split, name):
    plan, row = [], 0
    columns = grid.y * grid.c
    batches = grid.a * grid.b
    for height, wide in shapes:
        blocks = wide // (columns * width)
        rows = height // batches
        plan.append((row, rows, blocks, width))
        row += rows * blocks

    def slot(i, p):
        step_a = lax.rem(p[0] - lax.div(i, grid.b) + grid.a, grid.a)
        step_b = lax.rem(p[1] - lax.rem(i, grid.b) + grid.b, grid.b)
        return (0, step_b * grid.a + step_a, 0, 0)

    piece = pl.BlockSpec((grid.y, 1, row, width), slot)
    return pl.pallas_call(
        partial(_assemble_body, grid=grid, plan=plan, split=split),
        grid_spec=pltpu.PrefetchScalarGridSpec(
            num_scalar_prefetch=1,
            grid=(batches,),
            in_specs=[piece, piece],
            out_specs=[pl.BlockSpec((h // batches, w), lambda i, p: (i, 0)) for h, w in shapes],
        ),
        out_shape=[jax.ShapeDtypeStruct(shape, BF16) for shape in shapes],
        compiler_params=pltpu.CompilerParams(vmem_limit_bytes=48 << 20),
        cost_estimate=pl.CostEstimate(flops=0, transcendentals=0, bytes_accessed=4 * sum(h * w for h, w in shapes)),
        name=name,
    )(places, mine, theirs)


class Gather:
    def __init__(self, grid, places, weights, width, split, name):
        self.grid, self.places, self.width, self.split, self.name = grid, places, width, split, name
        self.shapes = [(w.shape[0] * grid.a * grid.b, w.shape[1]) for w in weights]
        seq, columns = lax.axis_index("seq"), grid.y * grid.c
        if split:
            self.value = pieces(weights, seq, columns, width)[None]
        else:
            core = lax.rem(seq, grid.c)
            self.value = jnp.stack(
                [pieces(weights, i * grid.c + core, columns, width) for i in range(grid.y)]
            )

    def send(self, axis):
        self.axis = axis
        self.flight = spread(self.grid, self.value, axis)[1:]

    def land(self):
        parts = [self.value, *self.flight]
        if self.axis == "y":
            self.value = jnp.concatenate(parts, axis=0)
        else:
            self.value = jnp.stack(parts, axis=1)

    def whole(self):
        grid = self.grid
        mine = self.value.reshape(grid.y, grid.b * grid.a, *self.value.shape[-2:])
        theirs = grid.shift(mine, "c", 1)
        return assemble(
            grid, self.places, mine, theirs, self.shapes, self.width, self.split, self.name
        )


def _weight_grad_body(place_ref, *refs, grid, height, have_sum, aliased, split):
    left_ref, right_ref = refs[:2]
    refs = refs[2:]
    sum_ref = None
    if have_sum:
        sum_ref, refs = refs[0], refs[1:]
    refs = refs[aliased:]
    direct = height % 128 == 0
    outs, turned, natural = (refs[:-1], refs[-1], None) if direct else (refs[:-2], refs[-2], refs[-1])
    a, b = place_ref[0], place_ref[1]
    side, block = pl.program_id(0), pl.program_id(1)

    @pl.when((side == 0) & (block == 0))
    def _():
        if not direct:
            natural[...] = left_ref[...].T
        for step_b in range(grid.b):
            for step_a in range(grid.a):
                other = lax.bitwise_xor(a, jnp.int32(bit_reversed(step_a, grid.bits)))
                owner = other * grid.b + lax.rem(b + step_b, grid.b)
                here = pl.ds(pl.multiple_of(owner * height, height), height)
                turned[step_b, step_a] = left_ref[:, here].T if direct else natural[here, :]

    samples = turned.shape[-1]
    half = grid.a * height
    for step_b in range(grid.b):
        part = jnp.dot(
            turned[step_b].reshape(half, samples),
            right_ref[...].reshape(samples, -1),
            preferred_element_type=F32,
        ).reshape(grid.a, height, -1)
        if have_sum:
            part = part + sum_ref[0, step_b].astype(F32)
        part = part.astype(BF16)
        if split == "b":
            outs[step_b][0] = part
        elif split == "y":
            for k, out in enumerate(outs):

                @pl.when(side == k)
                def _(out=out, part=part):
                    out[step_b] = part
        else:
            outs[0][0, step_b] = part


def weight_grad(grid, places, left, right, width, core_step, total_rows, row, buffers, split, received=None, name="weight_grad", local=False, sub=None):
    samples, depth = left.shape
    height = depth // (grid.a * grid.b)
    sides = 1 if local else grid.y
    columns = 1 if local else grid.y * grid.c
    many = right.ndim == 5
    blocks = right.shape[1] if many else right.shape[1] // (columns * width)
    lo, count = (0, blocks) if sub is None else sub
    first = row // height

    def right_index(k, i, p):
        if local:
            return (0, 0)
        side = lax.rem(p[2] + k, grid.y)
        core = lax.rem(p[3] + core_step, grid.c)
        if many:
            return (side * grid.c + core, lo + i, 0, 0, 0)
        return (0, (side * grid.c + core) * blocks + lo + i)

    if split == "b":
        shape = (sides, grid.a, total_rows, width)
        specs = [pl.BlockSpec((1, grid.a, height, width), lambda k, i, p: (k, 0, first + i, 0))] * grid.b
        number = grid.b
    elif split == "y":
        shape = (grid.b, grid.a, total_rows, width)

        def index_of(which):
            def index(k, i, p):
                return (0, 0, first + jnp.where(k < which, 0, jnp.where(k > which, count - 1, i)), 0)

            return index

        specs = [pl.BlockSpec((grid.b, grid.a, height, width), index_of(k)) for k in range(sides)]
        number = sides
    else:
        shape = (sides, grid.b, grid.a, total_rows, width)
        specs = [pl.BlockSpec((1, grid.b, grid.a, height, width), lambda k, i, p: (k, 0, 0, first + i, 0))]
        number = 1
    in_specs = [
        pl.BlockSpec((samples, depth), lambda k, i, p: (0, 0), pipeline_mode=pl.Buffered(1)),
        pl.BlockSpec((1, 1, *right.shape[2:]) if many else (samples, width), right_index),
    ]
    operands = [left, right]
    if received is not None:
        in_specs.append(pl.BlockSpec((1, grid.b, grid.a, height, width), lambda k, i, p: (k, 0, 0, first + i, 0)))
        operands.append(received)
    aliases = {}
    if buffers is not None:
        for i, buffer in enumerate(buffers):
            aliases[1 + len(operands)] = i
            in_specs.append(pl.BlockSpec(memory_space=pl.ANY))
            operands.append(buffer)
    body = partial(
        _weight_grad_body, grid=grid, height=height, have_sum=received is not None,
        aliased=0 if buffers is None else len(buffers), split=split,
    )
    work = sides * count * width
    return pl.pallas_call(
        body,
        grid_spec=pltpu.PrefetchScalarGridSpec(
            num_scalar_prefetch=1,
            grid=(sides, count),
            in_specs=in_specs,
            out_specs=specs,
            scratch_shapes=[pltpu.VMEM((grid.b, grid.a, height, samples), BF16)]
            + ([] if height % 128 == 0 else [pltpu.VMEM((depth, samples), BF16)]),
        ),
        out_shape=[jax.ShapeDtypeStruct(shape, BF16)] * number,
        input_output_aliases=aliases,
        compiler_params=pltpu.CompilerParams(vmem_limit_bytes=48 << 20),
        cost_estimate=pl.CostEstimate(flops=2 * samples * depth * work, transcendentals=0, bytes_accessed=2 * (samples * (depth + work) + depth * work)),
        name=name,
    )(places, *operands)


def added(parts):
    total = parts[0].astype(F32)
    for part in parts[1:]:
        total = total + part.astype(F32)
    return total


class Reduce:
    def __init__(self, grid, places, pairs, width, order, name, sub=None):
        self.grid, self.places, self.pairs, self.width = grid, places, pairs, width
        self.axes, self.name, self.sub = tuple(order), name, sub
        self.extra = None
        self.heights = [left.shape[1] // (grid.a * grid.b) for left, _ in pairs]
        columns = grid.y * grid.c
        self.counts = [
            right.shape[1] if right.ndim == 5 else right.shape[1] // (columns * width) if sub is None else sub[1]
            for _, right in pairs
        ]

    def _products(self, core_step, split, received, tokens):
        buffers, row = None, 0
        total = sum(h * n for h, n in zip(self.heights, self.counts))
        for i, ((left, right), h, n) in enumerate(zip(self.pairs, self.heights, self.counts)):
            if i == 0 and tokens:
                right = after(right, *tokens)
            buffers = weight_grad(
                self.grid, self.places, left, right, self.width, core_step, total, row, buffers, split,
                received, name=f"{self.name}_{i}_{core_step}", sub=self.sub,
            )
            row += h * n
        return buffers

    def far(self, *tokens):
        self.parts = self._products(1, None, None, tokens)

    def ship(self):
        self.received = self.grid.shift(self.parts[0], "c", 1)

    def near(self, *tokens):
        self.parts = self._products(0, self.axes[0], self.received, tokens)
        return self.parts[0]

    def send(self, stage, *tokens):
        grid, axis = self.grid, self.axes[stage]
        self.stage = stage
        if tokens:
            self.parts = list(lax.optimization_barrier((tuple(self.parts), tokens))[0])
        if self.extra is not None and axis == "b":
            self.parts = [jnp.concatenate([p, q], axis=-2) for p, q in zip(self.parts, self.extra)]
        self.flight = [grid.shift(self.parts[k], axis, k) for k in range(1, grid.size[axis])]

    def land(self):
        parts = [self.parts[0], *self.flight]
        if self.stage == 1:
            half = self.grid.a // 2
            self.parts = [added([p[k * half : (k + 1) * half] for p in parts]).astype(BF16) for k in range(2)]
        else:
            following = self.grid.size[self.axes[1]]
            self.parts = [added([p[k] for p in parts]).astype(BF16) for k in range(following)]


class Bundle:
    def __init__(self, *jobs):
        self.jobs, self.stage = jobs, 0
        self.grid = jobs[0].grid
        self.near, self.away = (
            jnp.concatenate([job.parts[k] for job in jobs], axis=1) for k in range(2)
        )

    def send(self):
        self.flight = [self.grid.swap(self.away, 1 << self.stage)]

    def land(self):
        total = [self.near, self.flight[0]]
        self.stage += 1
        if self.stage < self.grid.bits:
            half = self.near.shape[0] // 2
            self.near, self.away = (
                added([part[k * half : (k + 1) * half] for part in total]).astype(BF16)
                for k in range(2)
            )
            return
        row = 0
        for job in self.jobs:
            height = job.parts[0].shape[1]
            job.result = added([part[0, row : row + height] for part in total])
            row += height


def gather_everywhere(shard):
    rows = shard.shape[0] // lax.axis_size("seq")
    part = lax.dynamic_slice_in_dim(shard, lax.axis_index("seq") * rows, rows, 0)
    return lax.all_gather(part, ("batch", "seq"), axis=0, tiled=True)


class Share:
    def __init__(self, grid, value):
        self.grid, self.value = grid, value

    def send(self, axis):
        self.flight = spread(self.grid, self.value, axis)[1:]

    def land(self):
        self.value = added([self.value, *self.flight])


class Collect:
    def __init__(self, grid, places, shard):
        self.grid, self.places, self.shape, self.value = grid, places, shard.shape, shard[None, None]

    def send(self, axis):
        self.axis = axis
        self.flight = spread(self.grid, self.value, axis)[1:]

    def land(self):
        self.value = jnp.concatenate([self.value, *self.flight], axis=1 if self.axis == "a" else 0)

    def whole(self):
        grid, places = self.grid, self.places
        value = self.value.reshape(grid.b * grid.a, *self.shape)
        owner = jnp.arange(grid.a * grid.b, dtype=jnp.int32)
        step_a = (places[0] - owner // grid.b) % grid.a
        step_b = (places[1] - owner % grid.b) % grid.b
        value = jnp.take(value, step_b * grid.a + step_a, axis=0)
        return value.transpose(1, 0, 2).reshape(self.shape[0], -1)


def layer_norm(values, scale_row, shift_row):
    center = values - jnp.mean(values, axis=-1, keepdims=True)
    spread = jnp.mean(center * center, axis=-1, keepdims=True)
    return center * lax.rsqrt(spread + epsilon) * scale_row + shift_row


def glu_gate(gated_rows):
    half_width = gated_rows.shape[-1] // 2
    return gated_rows[..., :half_width] * jax.nn.sigmoid(gated_rows[..., half_width:])


def batch_norm(conv_value, sum_first, sum_second, scale_row, shift_row, count_all):
    center = sum_first / count_all
    spread = sum_second / count_all - center * center
    return (conv_value - center) * lax.rsqrt(spread + epsilon) * scale_row + shift_row


def position_table(length, model_width):
    fine = 64
    coarse = 2 * length // fine
    column = jnp.arange(model_width, dtype=jnp.int32)
    rates = jnp.exp((column // 2).astype(jnp.float32) * (-2.0 * math.log(10000.0) / model_width))
    odd = (column % 2 == 1)[None, :]
    start = (jnp.arange(coarse, dtype=jnp.int32) * fine - (length - 1)).astype(jnp.float32)
    large = start[:, None] * rates[None, :]
    small = jnp.arange(fine, dtype=jnp.int32).astype(jnp.float32)[:, None] * rates[None, :]
    sin_large, cos_large = jnp.sin(large), jnp.cos(large)
    first = jnp.where(odd, cos_large, sin_large)[:, None, :]
    second = jnp.where(odd, -sin_large, cos_large)[:, None, :]
    table = first * jnp.cos(small)[None] + second * jnp.sin(small)[None]
    return table.astype(jnp.bfloat16).reshape(2 * length, model_width)


def depth_conv(padded, kernel_rows, length):
    result = kernel_rows[0] * padded[:, 0:length]
    for offset in range(1, kernel_rows.shape[0]):
        result = result + kernel_rows[offset] * padded[:, offset : offset + length]
    return result


def depth_conv_back(padded_grad, kernel_rows, length):
    last_tap = kernel_rows.shape[0] - 1
    result = kernel_rows[0] * padded_grad[:, last_tap : last_tap + length]
    for offset in range(1, last_tap + 1):
        result = (
            result
            + kernel_rows[offset] * padded_grad[:, last_tap - offset : last_tap - offset + length]
        )
    return result


def matmul_rows(left_side, right_side):
    return jnp.dot(left_side, right_side, preferred_element_type=jnp.float32)


def times_transpose(left_side, right_side):
    return lax.dot_general(
        left_side, right_side, (((1,), (1,)), ((), ())), preferred_element_type=jnp.float32
    )


def transpose_times(left_side, right_side):
    return lax.dot_general(
        left_side, right_side, (((0,), (0,)), ((), ())), preferred_element_type=jnp.float32
    )


def linear_back(grad_rows, weight):
    grad_low = grad_rows.astype(jnp.bfloat16)
    return (times_transpose(grad_low, weight), grad_low)


def ffn_enter(values, scale_row, shift_row, weight_in):
    normed_low = layer_norm(values, scale_row, shift_row).astype(jnp.bfloat16)
    hidden_pre = matmul_rows(normed_low, weight_in)
    hidden_low = jax.nn.silu(hidden_pre).astype(jnp.bfloat16)
    return (normed_low, hidden_pre.astype(jnp.bfloat16), hidden_low)


def ffn_forward(values, scale_row, shift_row, weight_in, weight_out):
    saved = ffn_enter(values, scale_row, shift_row, weight_in)
    return (matmul_rows(saved[2], weight_out), saved)


def ffn_backward_exit(grad_rows, weight_out, saved_parts):
    grad_hidden, grad_out_low = linear_back(grad_rows, weight_out)
    silu_value, silu_back = jax.vjp(jax.nn.silu, saved_parts[1].astype(jnp.float32))
    return (silu_back(grad_hidden)[0].astype(jnp.bfloat16), grad_out_low)


def ffn_backward_entry(grad_pre_low, values, scale_row, shift_row, weight_in):
    norm_value, norm_back = jax.vjp(layer_norm, values, scale_row, shift_row)
    return norm_back(times_transpose(grad_pre_low, weight_in))


def ffn_backward(grad_rows, values, scale_row, shift_row, weight_in, weight_out, saved_parts):
    normed_low, hidden_pre, hidden_low = saved_parts
    grad_hidden, grad_out_low = linear_back(grad_rows, weight_out)
    silu_value, silu_back = jax.vjp(jax.nn.silu, hidden_pre.astype(jnp.float32))
    grad_pre = silu_back(grad_hidden)[0]
    grad_normed, grad_pre_low = linear_back(grad_pre, weight_in)
    norm_value, norm_back = jax.vjp(layer_norm, values, scale_row, shift_row)
    grad_values, grad_scale, grad_shift = norm_back(grad_normed)
    return (grad_values, grad_scale, grad_shift, grad_pre_low, grad_out_low)


def sum_everywhere(value):
    for axis in ("seq", "batch"):
        size, step = lax.axis_size(axis), 1
        while step < size:
            value = value + lax.ppermute(value, axis, [(i, i ^ step) for i in range(size)])
            step *= 2
    return value


def per_device(
    grid,
    acoustic_sequence,
    utterance_durations,
    chosen_entry_number,
    discretizer_score_perturbation,
    softmax_heat,
    normalizer_affine_rows,
    discretizer_score_projection,
    lexicon_vectors,
    opening_dense_entry_projection,
    opening_dense_exit_projection,
    request_projection,
    lookup_projection,
    content_projection_kernel,
    relative_offset_projection,
    mixing_exit_projection,
    unit_kernel_before_gating,
    channelwise_filter_coefficients,
    unit_kernel_after_normalizing,
    closing_dense_entry_projection,
    closing_dense_exit_projection,
    result_adjoint,
    discrete_label_adjoint,
):
    places = grid.places()
    small = Collect(
        grid,
        places,
        jnp.concatenate([normalizer_affine_rows, channelwise_filter_coefficients], axis=0),
    )
    vector_rows = normalizer_affine_rows.shape[0]
    model_width = acoustic_sequence.shape[2]
    piece_width = model_width // (grid.y * grid.c)
    gather = partial(Gather, grid, places)
    first = gather([opening_dense_entry_projection], piece_width, True, "gather_opening_entry")
    second = gather([opening_dense_exit_projection], piece_width, True, "gather_opening_exit")
    third = gather(
        [request_projection, lookup_projection, content_projection_kernel, relative_offset_projection],
        piece_width,
        False,
        "gather_attention",
    )
    first.send("a")
    small.send("a")
    settle([first, small])
    first.send("b")
    small.send("b")
    second.send("a")
    settle([first, small, second])
    conv_shards, entry_shard, exit_shard, quant_shard, lexicon_shard, first.value = lax.optimization_barrier(
        (
            (mixing_exit_projection, unit_kernel_after_normalizing, unit_kernel_before_gating),
            closing_dense_entry_projection,
            closing_dense_exit_projection,
            discretizer_score_projection,
            lexicon_vectors,
            first.value,
        )
    )
    convolution_all = gather_everywhere(jnp.concatenate(conv_shards, axis=1))
    out_all, conv_out_all, conv_in_all = jnp.split(
        convolution_all, [model_width, 2 * model_width], axis=1
    )
    closing_in_all = gather_everywhere(entry_shard)
    closing_out_all = gather_everywhere(exit_shard)
    quantizer_all = gather_everywhere(jnp.concatenate([quant_shard, lexicon_shard], axis=1))
    small_all = small.whole()
    vectors_all, depth_all = small_all[:vector_rows], small_all[vector_rows:]
    first.send("y")
    second.send("b")
    third.send("a")
    settle([first, second, third])
    groups, local_len, model_width = acoustic_sequence.shape
    seq_count = lax.axis_size("seq")
    seq_place = lax.axis_index("seq")
    full_len = local_len * seq_count
    entries = lexicon_vectors.shape[0] * grid.a * grid.b
    total_rows = groups * local_len
    local_width = model_width // seq_count
    kernel_size = depth_all.shape[0]
    rim_width = kernel_size // 2
    height = model_width // (grid.a * grid.b)
    params_f = vectors_all.astype(jnp.float32)
    depth_f = depth_all.astype(jnp.float32)
    positions = seq_place * local_len + jnp.arange(local_len, dtype=jnp.int32)
    valid_mask = (positions[None, :] < utterance_durations[:, None]).astype(jnp.float32)
    valid_rows = valid_mask.reshape(total_rows, 1)
    inputs_low = acoustic_sequence.reshape(total_rows, model_width)
    inputs_f = inputs_low.astype(jnp.float32)
    second.send("y")
    third.send("b")
    (macaron_in_all,) = first.whole()
    macaron_saved = ffn_enter(inputs_f, params_f[0], params_f[5], macaron_in_all)
    macaron_hidden = settle([second, third], macaron_saved[2])
    macaron_saved = (*macaron_saved[:2], macaron_hidden)
    (macaron_out_all,) = second.whole()
    query_all, key_all, value_all, pos_all = third.whole()
    macaron_value = matmul_rows(macaron_hidden, macaron_out_all)
    first_mid = inputs_f + 0.5 * macaron_value
    attn_normed = layer_norm(first_mid, params_f[1], params_f[6]).astype(jnp.bfloat16)
    stacked = project_heads(attn_normed, [query_all, key_all, value_all], groups, seq_count)
    by_heads = lax.all_to_all(stacked, "seq", split_axis=0, concat_axis=0, tiled=True)
    table_low = position_table(full_len, model_width)
    pos_columns = lax.dynamic_slice_in_dim(pos_all, seq_place * local_width, local_width, 1)
    position_low = matmul_rows(table_low, pos_columns).astype(jnp.bfloat16)
    biases = lax.dynamic_slice_in_dim(params_f[12:14], seq_place * local_width, local_width, 1)
    by_heads, position_low = lax.optimization_barrier((by_heads, position_low))
    attended_low, probs = attend_forward(by_heads, position_low, biases, utterance_durations)
    back_time = lax.all_to_all(
        attended_low, "seq", split_axis=0, concat_axis=0, tiled=True
    )
    attended_rows = back_time.transpose(1, 2, 0, 3).reshape(total_rows, model_width)
    second_mid = first_mid + matmul_rows(attended_rows, out_all)
    conv_normed = layer_norm(second_mid, params_f[2], params_f[7]).astype(jnp.bfloat16)
    gated_rows = matmul_rows(conv_normed, conv_in_all)
    glu_low = (
        (valid_rows * glu_gate(gated_rows))
        .astype(jnp.bfloat16)
        .reshape(groups, local_len, model_width)
    )
    padded_glu = extended(glu_low, (("seq", 1),), rim_width)
    conv_value = depth_conv(padded_glu, depth_f, local_len).reshape(total_rows, model_width)
    masked_conv = valid_rows * conv_value
    sums = sum_everywhere(
        jnp.stack(
            [
                jnp.sum(masked_conv, axis=0),
                jnp.sum(masked_conv * conv_value, axis=0),
                jnp.broadcast_to(jnp.sum(valid_mask), (model_width,)),
            ]
        )
    )
    sum_first, sum_second, count_all = sums[0], sums[1], sums[2]
    bound_norm = partial(batch_norm, count_all=count_all)
    normalized = bound_norm(conv_value, sum_first, sum_second, params_f[10], params_f[11])
    act_low = jax.nn.silu(normalized).astype(jnp.bfloat16)
    third_mid = second_mid + matmul_rows(act_low, conv_out_all)
    closing_value, closing_saved = ffn_forward(
        third_mid, params_f[3], params_f[8], closing_in_all, closing_out_all
    )
    quant_all, codebook_all = quantizer_all[:, :entries], quantizer_all[:, entries:]
    quant_logits = matmul_rows(inputs_low, quant_all)
    scaled_logits = (
        quant_logits
        + discretizer_score_perturbation.reshape(total_rows, entries).astype(jnp.float32)
    ) / softmax_heat
    relaxed_assignments = jax.nn.softmax(scaled_logits, axis=-1)
    soft_low = relaxed_assignments.astype(jnp.bfloat16)
    one_hot = (
        chosen_entry_number.reshape(total_rows, 1) == jnp.arange(entries, dtype=jnp.int32)[None, :]
    ).astype(jnp.bfloat16)
    codes_value = valid_rows * (
        matmul_rows(one_hot, codebook_all) + matmul_rows(soft_low, codebook_all)
    )
    grad_codes = (
        valid_rows * discrete_label_adjoint.reshape(total_rows, model_width).astype(jnp.float32)
    ).astype(jnp.bfloat16)
    grad_soft = times_transpose(grad_codes, codebook_all)
    rescaled_derivative = relaxed_assignments * (
        grad_soft - jnp.sum(grad_soft * relaxed_assignments, axis=-1, keepdims=True)
    )
    score_derivative_lowprecision = (rescaled_derivative / softmax_heat).astype(jnp.bfloat16)
    grad_quant_in = times_transpose(score_derivative_lowprecision, quant_all)
    fourth_mid = third_mid + 0.5 * closing_value
    final_value, final_back = jax.vjp(layer_norm, fourth_mid, params_f[4], params_f[9])
    output = (valid_rows * final_value).astype(jnp.bfloat16).reshape(groups, local_len, model_width)
    codes = codes_value.astype(jnp.bfloat16).reshape(groups, local_len, model_width)
    grad_final = valid_rows * result_adjoint.reshape(total_rows, model_width).astype(jnp.float32)
    grad_fourth, scale_four, shift_four = final_back(grad_final)
    grad_closing, scale_three, shift_three, close_pre_low, close_out_low = ffn_backward(
        0.5 * grad_fourth,
        third_mid,
        params_f[3],
        params_f[8],
        closing_in_all,
        closing_out_all,
        closing_saved,
    )
    grad_third = grad_fourth + grad_closing
    close_normed, close_pre, close_hidden = closing_saved
    reduce = partial(Reduce, grid, places)
    closing_job = reduce(
        [(close_hidden, close_out_low), (close_normed, close_pre_low)], piece_width, "by", "closing"
    )
    closing_job.far()
    closing_job.ship()
    grad_act, grad_third_low = linear_back(grad_third, conv_out_all)
    silu_value, silu_back = jax.vjp(jax.nn.silu, normalized)
    grad_normalized = silu_back(grad_act)[0]
    norm_value, norm_back = jax.vjp(
        bound_norm, conv_value, sum_first, sum_second, params_f[10], params_f[11]
    )
    grad_conv_direct, part_first, part_second, grad_bn_scale, grad_bn_shift = norm_back(
        grad_normalized
    )
    totals = sum_everywhere(jnp.stack([part_first, part_second]))
    chosen_soft = one_hot + soft_low
    early_job = reduce(
        [
            (act_low, grad_third_low),
            (inputs_low, score_derivative_lowprecision),
            (chosen_soft, grad_codes),
        ],
        piece_width,
        "yb",
        "early",
    )
    early_job.far()
    early_job.ship()
    closing_job.near()
    early_job.near()
    totals = settle([], totals, hold=[closing_job, early_job])
    closing_job.send(0)
    early_job.send(0)
    total_first, total_second = totals[0], totals[1]
    grad_conv = grad_conv_direct + valid_rows * (total_first + 2.0 * conv_value * total_second)
    grad_conv_low = grad_conv.astype(jnp.bfloat16).reshape(groups, local_len, model_width)
    padded_grad = extended(grad_conv_low, (("seq", 1),), rim_width)
    grad_glu = valid_rows * depth_conv_back(padded_grad, depth_f, local_len).reshape(
        total_rows, model_width
    )
    grad_conv_float = grad_conv_low.astype(jnp.float32)
    grad_depth = jnp.stack(
        [
            jnp.sum(
                padded_glu[:, offset : offset + local_len].astype(jnp.float32) * grad_conv_float,
                axis=(0, 1),
            )
            for offset in range(kernel_size)
        ]
    )
    glu_value, glu_back = jax.vjp(glu_gate, gated_rows)
    grad_gated = glu_back(grad_glu)[0]
    grad_conv_normed, grad_gated_low = linear_back(grad_gated, conv_in_all)
    conv_norm_value, conv_norm_back = jax.vjp(layer_norm, second_mid, params_f[2], params_f[7])
    grad_from_conv, scale_two, shift_two = conv_norm_back(grad_conv_normed)
    grad_second = grad_third + grad_from_conv
    grad_second_low = grad_second.astype(jnp.bfloat16)
    grad_attended = unproject_heads(grad_second_low, out_all, groups, seq_count)
    grad_heads = lax.all_to_all(grad_attended, "seq", split_axis=0, concat_axis=0, tiled=True)

    middle_job = reduce(
        [(conv_normed, grad_gated_low), (attended_rows, grad_second_low)],
        piece_width,
        "by",
        "middle",
    )
    middle_job.far()
    grad_heads = settle([], grad_heads, hold=[middle_job])
    middle_job.ship()
    grad_stack, grad_position_low, grad_biases = attend_backward(
        probs, by_heads, grad_heads, position_low, biases
    )
    grad_stack = settle([closing_job, early_job], grad_stack)
    grad_time = lax.all_to_all(grad_stack, "seq", split_axis=0, concat_axis=0, tiled=True)
    position_parts = weight_grad(
        grid, places, table_low, grad_position_low, piece_width, 0, height, 0, None, "b",
        name="position_grad", local=True,
    )
    middle_job.near()
    grad_time, *position_parts = settle([], grad_time, *position_parts, hold=[middle_job])
    closing_job.send(1)
    early_job.send(1)
    middle_job.send(0)
    grad_attn_normed = join_heads(grad_time, [query_all, key_all, value_all])
    attn_norm_value, attn_norm_back = jax.vjp(layer_norm, first_mid, params_f[1], params_f[6])
    grad_from_attn, scale_one, shift_one = attn_norm_back(grad_attn_normed)
    grad_first = grad_second + grad_from_attn
    attention_job = reduce(
        [(attn_normed, grad_time)], piece_width, "yb", "attention"
    )
    attention_job.extra = [part[0] for part in position_parts]
    attention_job.far()
    attention_job.ship()
    content_full, position_full = lax.dynamic_update_slice_in_dim(
        jnp.zeros((2, model_width), jnp.float32), grad_biases, seq_place * local_width, 1
    )
    mac_normed, mac_pre, mac_hidden = macaron_saved
    mac_out_low = (0.5 * grad_first).astype(jnp.bfloat16)
    macaron_out_job = reduce([(mac_hidden, mac_out_low)], piece_width, "by", "opening_exit")
    macaron_out_job.far()
    macaron_out_job.ship()
    attention_job.near()
    macaron_out_job.near()
    mac_out_low = settle(
        [closing_job, early_job], mac_out_low, hold=[attention_job, macaron_out_job]
    )
    first_tails = Bundle(closing_job, early_job)
    first_tails.send()
    attention_job.send(0)
    mac_pre_low, mac_out_low = ffn_backward_exit(mac_out_low, macaron_out_all, macaron_saved)
    halves = mac_pre_low.shape[1] // model_width // 2
    macaron_in_jobs = [
        reduce([(mac_normed, mac_pre_low)], piece_width, order, name, sub=(i * halves, halves))
        for i, (order, name) in enumerate((("yb", "opening_entry"), ("by", "opening_entry_more")))
    ]
    for job in macaron_in_jobs:
        job.far()
    mac_pre_low = settle([middle_job, first_tails], mac_pre_low, hold=macaron_in_jobs)
    for job in macaron_in_jobs:
        job.ship()
    first_tails.send()
    middle_job.send(1)
    macaron_out_job.send(0)
    grad_macaron, scale_zero, shift_zero = ffn_backward_entry(
        mac_pre_low, inputs_f, params_f[0], params_f[5], macaron_in_all
    )
    grad_layer_in = grad_first + grad_macaron
    frames_grad = (
        (grad_layer_in + grad_quant_in).astype(jnp.bfloat16).reshape(groups, local_len, model_width)
    )
    vectors_grad = jnp.stack(
        [
            scale_zero,
            scale_one,
            scale_two,
            scale_three,
            scale_four,
            shift_zero,
            shift_one,
            shift_two,
            shift_three,
            shift_four,
            grad_bn_scale,
            grad_bn_shift,
            content_full,
            position_full,
        ]
    )
    small = Share(grid, jnp.concatenate([vectors_grad, grad_depth], axis=0))
    small.send("c")
    small.land()
    for job in macaron_in_jobs:
        job.near()
    small.value = settle(
        [first_tails, middle_job, attention_job, macaron_out_job],
        small.value,
        hold=macaron_in_jobs,
    )
    for job in macaron_in_jobs:
        job.send(0)
    attention_job.send(1)
    macaron_out_job.send(1)
    middle_tails = Bundle(middle_job)
    middle_tails.send()
    small.send("y")
    settle([small, middle_tails, attention_job, macaron_out_job, *macaron_in_jobs])
    for job in macaron_in_jobs:
        job.send(1)
    middle_tails.send()
    late_tails = Bundle(attention_job, macaron_out_job)
    late_tails.send()
    small.send("b")
    settle([small, middle_tails, late_tails, *macaron_in_jobs])
    late_tails.send()
    last_tails = Bundle(*macaron_in_jobs)
    last_tails.send()
    small.send("a")
    settle([small, last_tails, late_tails])
    last_tails.send()
    settle([last_tails])
    small_width = model_width // (grid.a * grid.b)
    small_sums = lax.dynamic_slice_in_dim(
        small.value, lax.axis_index("batch") * small_width, small_width, 1
    )
    vectors_sum, depth_sum = small_sums[:vector_rows], small_sums[vector_rows:]

    def rows_of(job, count):
        return (job.result[i * height : (i + 1) * height] for i in range(count))

    exit_rows = close_hidden.shape[1] // (grid.a * grid.b)
    closing_out_sum, closing_in_sum = closing_job.result[:exit_rows], closing_job.result[exit_rows:]
    conv_out_sum, quant_sum, codebook_sum = rows_of(early_job, 3)
    conv_in_sum, out_sum = middle_job.result[: 2 * height], middle_job.result[2 * height :]
    query_sum, key_sum, value_sum, pos_sum = rows_of(attention_job, 4)
    macaron_out_sum = macaron_out_job.result
    macaron_in_sum = jnp.concatenate([job.result for job in macaron_in_jobs])

    def side_by_side(blocks):
        return jnp.concatenate(
            [blocks[i : i + height] for i in range(0, blocks.shape[0], height)], axis=1
        )

    closing_in_sum, conv_in_sum, macaron_in_sum = (
        side_by_side(closing_in_sum),
        side_by_side(conv_in_sum),
        side_by_side(macaron_in_sum),
    )
    return (
        output,
        codes,
        frames_grad,
        vectors_sum,
        quant_sum,
        codebook_sum,
        macaron_in_sum,
        macaron_out_sum,
        query_sum,
        key_sum,
        value_sum,
        pos_sum,
        out_sum,
        conv_in_sum,
        depth_sum,
        conv_out_sum,
        closing_in_sum,
        closing_out_sum,
    )


def solution(mesh):
    placed = (
        P("batch", "seq", None),
        P("batch"),
        P("batch", "seq"),
        P("batch", "seq", None),
        P(),
        P(None, "batch"),
        P("batch", None),
        P("batch", None),
        P("batch", None),
        P("batch", None),
        P("batch", None),
        P("batch", None),
        P("batch", None),
        P("batch", None),
        P("batch", None),
        P("batch", None),
        P(None, "batch"),
        P("batch", None),
        P("batch", None),
        P("batch", None),
        P("batch", "seq", None),
        P("batch", "seq", None),
    )
    return jax.shard_map(
        partial(per_device, Grid(mesh)),
        mesh=mesh,
        in_specs=placed,
        out_specs=(
            P("batch", "seq", None),
            P("batch", "seq", None),
            P("batch", "seq", None),
            P(None, "batch"),
            P("batch", "seq"),
            P("batch", "seq"),
            P("batch", "seq"),
            P("batch", "seq"),
            P("batch", "seq"),
            P("batch", "seq"),
            P("batch", "seq"),
            P("batch", "seq"),
            P("batch", "seq"),
            P("batch", "seq"),
            P(None, "batch"),
            P("batch", "seq"),
            P("batch", "seq"),
            P("batch", "seq"),
        ),
        check_vma=False,
    )
```

```python
from functools import partial
import math

import jax
import jax.numpy as jnp
from jax import lax
from jax.experimental import pallas as pl
from jax.experimental.pallas import tpu as pltpu
from jax.sharding import PartitionSpec as P

HEAD_WIDTH = 128


epsilon = 1e-05

F32, BF16 = jnp.float32, jnp.bfloat16
SHARE = 4


def cost(flops, transcendentals, bytes_accessed):
    return pl.CostEstimate(
        flops=flops // SHARE,
        transcendentals=transcendentals // SHARE,
        bytes_accessed=bytes_accessed // SHARE,
    )


def dot(a, b, ca, cb):
    return lax.dot_general(a, b, (((ca,), (cb,)), ((), ())), preferred_element_type=F32)

def _fwd_body(len_ref, q_ref, k_ref, v_ref, pos_ref, bias_ref, o_ref, p_ref, *, rows, full, scale):
    block = pl.program_id(2)
    length = len_ref[pl.program_id(0)]
    query = q_ref[0, 0, 0].astype(F32)
    content_query = (query + bias_ref[0:1, :]).astype(BF16)
    position_query = (query + bias_ref[1:2, :]).astype(BF16)
    content = dot(content_query, k_ref[:, 0, 0].reshape(full, -1), 1, 1)
    span = full + rows
    start = pl.multiple_of(full - rows - block * rows, rows)
    relative = dot(position_query, pos_ref[pl.ds(start, span), :], 1, 1)
    relative = pltpu.roll(relative, span - (rows - 1), 1, stride=1, stride_axis=0)
    raw = content + relative[:, :full]
    seen = lax.broadcasted_iota(jnp.int32, raw.shape, 1) < length
    scores = jnp.where(seen, raw * scale, -1e30)
    top = jnp.max(scores, axis=-1, keepdims=True)
    weights = jnp.exp(scores - top)
    total = jnp.sum(weights, axis=-1, keepdims=True)
    low = (weights * (1.0 / total)).astype(BF16)
    p_ref[0, 0] = low
    o_ref[0, 0] = dot(low, v_ref[:, 0, 0].reshape(full, -1), 1, 0).astype(BF16)

def attend_forward(by_heads, position, bias, lengths):
    parts, _, groups, rows, width = by_heads.shape
    depth, full = HEAD_WIDTH, parts * rows
    heads = width // depth
    body = partial(_fwd_body, rows=rows, full=full, scale=1.0 / math.sqrt(depth))
    flops = groups * heads * full * (2 * full * depth * 3 + 2 * rows * depth)
    return pl.pallas_call(
        body,
        grid_spec=pltpu.PrefetchScalarGridSpec(
            num_scalar_prefetch=1,
            grid=(groups, heads, parts),
            in_specs=[
                pl.BlockSpec((1, 1, 1, rows, depth), lambda u, h, i, n: (i, 0, u, 0, h)),
                pl.BlockSpec((parts, 1, 1, rows, depth), lambda u, h, i, n: (0, 1, u, 0, h)),
                pl.BlockSpec((parts, 1, 1, rows, depth), lambda u, h, i, n: (0, 2, u, 0, h)),
                pl.BlockSpec((2 * full, depth), lambda u, h, i, n: (0, h)),
                pl.BlockSpec((2, depth), lambda u, h, i, n: (0, h)),
            ],
            out_specs=[
                pl.BlockSpec((1, 1, rows, depth), lambda u, h, i, n: (i, u, 0, h)),
                pl.BlockSpec((1, 1, rows, full), lambda u, h, i, n: (u, h, i, 0)),
            ],
        ),
        out_shape=[
            jax.ShapeDtypeStruct((parts, groups, rows, width), BF16),
            jax.ShapeDtypeStruct((groups, heads, full, full), BF16),
        ],
        compiler_params=pltpu.CompilerParams(vmem_limit_bytes=48 << 20),
        cost_estimate=cost(flops=flops, transcendentals=groups * heads * full * full, bytes_accessed=groups * heads * full * full * 2 + 5 * groups * full * width * 2),
        name="attend_forward",
    )(lengths, by_heads, by_heads, by_heads, position, bias)

def _bwd_body(p_ref, q_ref, k_ref, v_ref, g_ref, pos_ref, bias_ref, d_ref, dpos_ref, dbias_ref,
              key_acc, value_acc, pos_acc, bias_acc, *, rows, full, scale):
    group, block = pl.program_id(1), pl.program_id(2)
    last_block = block == pl.num_programs(2) - 1

    @pl.when((group == 0) & (block == 0))
    def _():
        pos_acc[...] = jnp.zeros_like(pos_acc)
        bias_acc[...] = jnp.zeros_like(bias_acc)

    @pl.when(block == 0)
    def _():
        key_acc[...] = jnp.zeros_like(key_acc)
        value_acc[...] = jnp.zeros_like(value_acc)

    query = q_ref[0, 0, 0].astype(F32)
    content_query = (query + bias_ref[0:1, :]).astype(BF16)
    position_query = (query + bias_ref[1:2, :]).astype(BF16)
    keys, values, grad = k_ref[:, 0, 0].reshape(full, -1), v_ref[:, 0, 0].reshape(full, -1), g_ref[0, 0]
    low = p_ref[0, 0]
    weights = low.astype(F32)
    grad_weights = dot(grad, values, 1, 1)
    value_acc[...] += dot(grad, low, 0, 0)
    inner = jnp.sum(grad_weights * weights, axis=-1, keepdims=True)
    grad_raw = (weights * (grad_weights - inner) * scale).astype(BF16)
    key_acc[...] += dot(content_query, grad_raw, 0, 0)
    grad_content = dot(grad_raw, keys, 1, 0)
    row = lax.broadcasted_iota(jnp.int32, (rows, rows), 0)
    column = lax.broadcasted_iota(jnp.int32, (rows, rows), 1)
    flip = jnp.where(row + column == rows - 1, 1.0, 0.0).astype(BF16)
    span = full + rows
    start = pl.multiple_of(full - rows - block * rows, rows)
    turned = jnp.concatenate([dot(flip, grad_raw, 1, 0).astype(BF16), jnp.zeros((rows, rows), BF16)], axis=1)
    turned = pltpu.roll(turned, 0, 1, stride=1, stride_axis=0)
    turned_query = dot(flip, position_query, 1, 0).astype(BF16)
    pos_acc[:, pl.ds(start, span)] += dot(turned_query, turned, 0, 0)
    grad_turned = dot(turned, pos_ref[pl.ds(start, span), :], 1, 0)
    high = grad_turned.astype(BF16)
    rest = (grad_turned - high.astype(F32)).astype(BF16)
    grad_position = dot(flip, high, 1, 0) + dot(flip, rest, 1, 0)
    d_ref[block, 0, 0] = (grad_content + grad_position).astype(BF16)
    bias_acc[0:1, :] += jnp.sum(grad_content, axis=0, keepdims=True)
    bias_acc[1:2, :] += jnp.sum(grad_position, axis=0, keepdims=True)

    @pl.when(last_block)
    def _():
        d_ref[:, 1, 0] = key_acc[...].T.astype(BF16).reshape(full // rows, rows, -1)
        d_ref[:, 2, 0] = value_acc[...].T.astype(BF16).reshape(full // rows, rows, -1)

    @pl.when(last_block & (group == pl.num_programs(1) - 1))
    def _():
        dpos_ref[...] = pos_acc[...].T.astype(BF16)
        dbias_ref[...] = bias_acc[...]

def attend_backward(probs, by_heads, grad_heads, position, bias):
    parts, _, groups, rows, width = by_heads.shape
    depth, full = HEAD_WIDTH, parts * rows
    heads = width // depth
    body = partial(_bwd_body, rows=rows, full=full, scale=1.0 / math.sqrt(depth))
    flops = groups * heads * full * (2 * full * depth * 7 + 6 * rows * depth)
    return pl.pallas_call(
        body,
        grid_spec=pltpu.PrefetchScalarGridSpec(
            num_scalar_prefetch=0,
            grid=(heads, groups, parts),
            in_specs=[
                pl.BlockSpec((1, 1, rows, full), lambda h, u, i: (u, h, i, 0)),
                pl.BlockSpec((1, 1, 1, rows, depth), lambda h, u, i: (i, 0, u, 0, h)),
                pl.BlockSpec((parts, 1, 1, rows, depth), lambda h, u, i: (0, 1, u, 0, h)),
                pl.BlockSpec((parts, 1, 1, rows, depth), lambda h, u, i: (0, 2, u, 0, h)),
                pl.BlockSpec((1, 1, rows, depth), lambda h, u, i: (i, u, 0, h)),
                pl.BlockSpec((2 * full, depth), lambda h, u, i: (0, h)),
                pl.BlockSpec((2, depth), lambda h, u, i: (0, h)),
            ],
            out_specs=[
                pl.BlockSpec((parts, 3, 1, rows, depth), lambda h, u, i: (0, 0, u, 0, h)),
                pl.BlockSpec((2 * full, depth), lambda h, u, i: (0, h)),
                pl.BlockSpec((2, depth), lambda h, u, i: (0, h)),
            ],
            scratch_shapes=[
                pltpu.VMEM((depth, full), F32),
                pltpu.VMEM((depth, full), F32),
                pltpu.VMEM((depth, 2 * full), F32),
                pltpu.VMEM((2, depth), F32),
            ],
        ),
        out_shape=[
            jax.ShapeDtypeStruct((parts, 3, groups, rows, width), BF16),
            jax.ShapeDtypeStruct((2 * full, width), BF16),
            jax.ShapeDtypeStruct((2, width), F32),
        ],
        compiler_params=pltpu.CompilerParams(vmem_limit_bytes=48 << 20),
        cost_estimate=cost(flops=flops, transcendentals=0, bytes_accessed=groups * heads * full * full * 2 + 8 * groups * full * width * 2),
        name="attend_backward",
    )(probs, by_heads, by_heads, by_heads, grad_heads, position, bias)


def extended(value, sides, width):
    for axis, dim in sides:
        size, length = (lax.axis_size(axis), value.shape[dim])
        up = [(i, (i + 1) % size) for i in range(size - 1)]
        down = [(j, i) for i, j in up]
        last = lax.slice_in_dim(value, length - width, length, axis=dim)
        initial = lax.slice_in_dim(value, 0, width, axis=dim)
        before = lax.ppermute(last, axis, up)
        after = lax.ppermute(initial, axis, down)
        value = jnp.concatenate([before, value, after], axis=dim)
    return value


def _project_body(left_ref, *refs):
    out = refs[-1]
    for i, weight in enumerate(refs[:-1]):
        out[0, i] = dot(left_ref[...], weight[...], 1, 0).astype(BF16).reshape(out.shape[2:])


def project_heads(left, weights, groups, parts):
    rows, depth = left.shape
    width = weights[0].shape[1] // parts
    shape = (parts, len(weights), groups, rows // groups, width)
    return pl.pallas_call(
        _project_body,
        grid=(parts,),
        in_specs=[pl.BlockSpec((rows, depth), lambda s: (0, 0))]
        + [pl.BlockSpec((depth, width), lambda s: (0, s))] * len(weights),
        out_specs=pl.BlockSpec((1, *shape[1:]), lambda s: (s, 0, 0, 0, 0)),
        out_shape=jax.ShapeDtypeStruct(shape, BF16),
        compiler_params=pltpu.CompilerParams(vmem_limit_bytes=48 << 20),
        cost_estimate=cost(flops=2 * rows * depth * width * parts * len(weights), transcendentals=0, bytes_accessed=2 * len(weights) * (rows + depth) * width * parts + 2 * rows * depth),
        name="project_heads",
    )(left, *weights)


def _unproject_body(left_ref, weight_ref, out_ref):
    out_ref[0] = dot(left_ref[...], weight_ref[...], 1, 1).astype(BF16).reshape(out_ref.shape[1:])


def unproject_heads(left, weight, groups, parts):
    rows, depth = left.shape
    width = weight.shape[0] // parts
    shape = (parts, groups, rows // groups, width)
    return pl.pallas_call(
        _unproject_body,
        grid=(parts,),
        in_specs=[
            pl.BlockSpec((rows, depth), lambda s: (0, 0)),
            pl.BlockSpec((width, depth), lambda s: (s, 0)),
        ],
        out_specs=pl.BlockSpec((1, *shape[1:]), lambda s: (s, 0, 0, 0)),
        out_shape=jax.ShapeDtypeStruct(shape, BF16),
        compiler_params=pltpu.CompilerParams(vmem_limit_bytes=48 << 20),
        cost_estimate=cost(flops=2 * rows * depth * width * parts, transcendentals=0, bytes_accessed=2 * (rows + depth) * width * parts + 2 * rows * depth),
        name="unproject_heads",
    )(left, weight)


def _join_body(grad_ref, *refs):
    out = refs[-1]

    @pl.when(pl.program_id(0) == 0)
    def _():
        out[...] = jnp.zeros_like(out)

    total = out[...]
    for i, weight in enumerate(refs[:-1]):
        total = total + dot(grad_ref[0, i].reshape(out.shape[0], -1), weight[...], 1, 1)
    out[...] = total


def join_heads(grads, weights):
    parts, count, groups, frames, width = grads.shape
    rows, depth = groups * frames, weights[0].shape[0]
    return pl.pallas_call(
        _join_body,
        grid=(parts,),
        in_specs=[pl.BlockSpec((1, count, groups, frames, width), lambda s: (s, 0, 0, 0, 0))]
        + [pl.BlockSpec((depth, width), lambda s: (0, s))] * count,
        out_specs=pl.BlockSpec((rows, depth), lambda s: (0, 0)),
        out_shape=jax.ShapeDtypeStruct((rows, depth), F32),
        compiler_params=pltpu.CompilerParams(vmem_limit_bytes=48 << 20),
        cost_estimate=cost(flops=2 * rows * depth * width * parts * count, transcendentals=0, bytes_accessed=2 * count * (rows + depth) * width * parts + 4 * rows * depth),
        name="join_heads",
    )(grads, *weights)


def line_factors(line):
    places = [(*device.coords, device.core_on_chip) for device in line]
    moving = [first != second for first, second in zip(places[0], places[1])].index(True)
    inner = len({place[moving] for place in places})
    return len(places) // inner, inner


class Grid:
    def __init__(self, mesh):
        devices = mesh.devices
        self.a, self.b = line_factors(list(devices[:, 0]))
        self.y, self.c = line_factors(list(devices[0, :]))
        self.size = {"a": self.a, "b": self.b, "y": self.y, "c": self.c}
        self.bits = self.a.bit_length() - 1

    def places(self):
        batch, seq = lax.axis_index("batch"), lax.axis_index("seq")
        return jnp.stack([batch // self.b, batch % self.b, seq // self.c, seq % self.c]).astype(jnp.int32)

    def shift(self, value, axis, step):
        name = "batch" if axis in "ab" else "seq"
        outer, inner = (self.a, self.b) if axis in "ab" else (self.y, self.c)
        pairs = []
        for i in range(outer):
            for j in range(inner):
                if axis in "ay":
                    pairs.append((i * inner + j, (i + step) % outer * inner + j))
                else:
                    pairs.append((i * inner + j, i * inner + (j + step) % inner))
        return lax.ppermute(value, name, pairs)

    def swap(self, value, step):
        pairs = [
            (i * self.b + j, (i ^ step) * self.b + j) for i in range(self.a) for j in range(self.b)
        ]
        return lax.ppermute(value, "batch", pairs)


def after(value, *tokens):
    return lax.optimization_barrier((value, *tokens))[0]


def settle(jobs, *tokens, hold=()):
    flights = tuple(tuple(job.flight) for job in jobs)
    parts = tuple(tuple(job.parts) for job in hold)
    landed, tokens, parts = lax.optimization_barrier((flights, tokens, parts))
    for job, held in zip(hold, parts):
        job.parts = list(held)
    for job, flight in zip(jobs, landed):
        job.flight = list(flight)
        job.land()
    moving = [job for job in jobs if isinstance(job, (Reduce, Bundle)) and job.result is None]
    if tokens and moving:
        parts = tuple(tuple(job.parts) for job in moving)
        tokens, parts = lax.optimization_barrier((tokens, parts))
        for job, held in zip(moving, parts):
            job.parts = list(held)
    return tokens[0] if len(tokens) == 1 else tokens


def bit_reversed(value, bits):
    return sum((value >> i & 1) << (bits - 1 - i) for i in range(bits))


def spread(grid, value, axis):
    return [value] + [grid.shift(value, axis, k) for k in range(1, grid.size[axis])]


def pieces(weights, place, count, width):
    rows = []
    for weight in weights:
        wide = weight.shape[1] // count
        piece = lax.dynamic_slice_in_dim(weight, place * wide, wide, 1)
        rows += [piece[:, i : i + width] for i in range(0, wide, width)]
    return jnp.concatenate(rows, axis=0)


def _assemble_body(place_ref, mine_ref, theirs_ref, *outs, grid, plan, split):
    y, c = place_ref[2], place_ref[3]
    for out, (row, height, blocks, width) in zip(outs, plan):
        for step in range(grid.y):
            side = lax.rem(y - step + grid.y, grid.y) if split else step
            for other, source in enumerate((mine_ref, theirs_ref)):
                column = side * grid.c + lax.rem(c + other, grid.c)
                for block in range(blocks):
                    place = pl.multiple_of((column * blocks + block) * width, width)
                    out[:, pl.ds(place, width)] = source[step, 0, pl.ds(row + block * height, height), :]


def assemble(grid, places, mine, theirs, shapes, width, split, name):
    plan, row = [], 0
    columns = grid.y * grid.c
    batches = grid.a * grid.b
    for height, wide in shapes:
        blocks = wide // (columns * width)
        rows = height // batches
        plan.append((row, rows, blocks, width))
        row += rows * blocks

    def slot(i, p):
        step_a = lax.rem(p[0] - lax.div(i, grid.b) + grid.a, grid.a)
        step_b = lax.rem(p[1] - lax.rem(i, grid.b) + grid.b, grid.b)
        return (0, step_b * grid.a + step_a, 0, 0)

    piece = pl.BlockSpec((grid.y, 1, row, width), slot)
    return pl.pallas_call(
        partial(_assemble_body, grid=grid, plan=plan, split=split),
        grid_spec=pltpu.PrefetchScalarGridSpec(
            num_scalar_prefetch=1,
            grid=(batches,),
            in_specs=[piece, piece],
            out_specs=[pl.BlockSpec((h // batches, w), lambda i, p: (i, 0)) for h, w in shapes],
        ),
        out_shape=[jax.ShapeDtypeStruct(shape, BF16) for shape in shapes],
        compiler_params=pltpu.CompilerParams(vmem_limit_bytes=48 << 20),
        cost_estimate=cost(flops=0, transcendentals=0, bytes_accessed=4 * sum(h * w for h, w in shapes)),
        name=name,
    )(places, mine, theirs)


class Gather:
    def __init__(self, grid, places, weights, width, split, name):
        self.grid, self.places, self.width, self.split, self.name = grid, places, width, split, name
        self.shapes = [(w.shape[0] * grid.a * grid.b, w.shape[1]) for w in weights]
        seq, columns = lax.axis_index("seq"), grid.y * grid.c
        if split:
            self.value = pieces(weights, seq, columns, width)[None]
        else:
            core = lax.rem(seq, grid.c)
            self.value = jnp.stack(
                [pieces(weights, i * grid.c + core, columns, width) for i in range(grid.y)]
            )

    def send(self, axis):
        self.axis = axis
        self.flight = spread(self.grid, self.value, axis)[1:]

    def land(self):
        parts = [self.value, *self.flight]
        if self.axis == "y":
            self.value = jnp.concatenate(parts, axis=0)
        else:
            self.value = jnp.stack(parts, axis=1)

    def whole(self):
        grid = self.grid
        mine = self.value.reshape(grid.y, grid.b * grid.a, *self.value.shape[-2:])
        theirs = grid.shift(mine, "c", 1)
        return assemble(
            grid, self.places, mine, theirs, self.shapes, self.width, self.split, self.name
        )


def _weight_grad_body(place_ref, *refs, grid, height, have_sum, aliased, split):
    left_ref, right_ref = refs[:2]
    refs = refs[2:]
    sum_ref = None
    if have_sum:
        sum_ref, refs = refs[0], refs[1:]
    refs = refs[aliased:]
    direct = height % 128 == 0
    outs, turned, natural = (refs[:-1], refs[-1], None) if direct else (refs[:-2], refs[-2], refs[-1])
    a, b = place_ref[0], place_ref[1]
    side, block = pl.program_id(0), pl.program_id(1)

    @pl.when((side == 0) & (block == 0))
    def _():
        if not direct:
            natural[...] = left_ref[...].T
        for step_b in range(grid.b):
            for step_a in range(grid.a):
                other = lax.bitwise_xor(a, jnp.int32(bit_reversed(step_a, grid.bits)))
                owner = other * grid.b + lax.rem(b + step_b, grid.b)
                here = pl.ds(pl.multiple_of(owner * height, height), height)
                turned[step_b, step_a] = left_ref[:, here].T if direct else natural[here, :]

    samples = turned.shape[-1]
    half = grid.a * height
    for step_b in range(grid.b):
        part = jnp.dot(
            turned[step_b].reshape(half, samples),
            right_ref[...].reshape(samples, -1),
            preferred_element_type=F32,
        ).reshape(grid.a, height, -1)
        if have_sum:
            part = part + sum_ref[0, step_b].astype(F32)
        part = part.astype(BF16)
        if split == "b":
            outs[step_b][0] = part
        elif split == "y":
            for k, out in enumerate(outs):

                @pl.when(side == k)
                def _(out=out, part=part):
                    out[step_b] = part
        else:
            outs[0][0, step_b] = part


def weight_grad(grid, places, left, right, width, core_step, total_rows, row, buffers, split, received=None, name="weight_grad", local=False, sub=None):
    samples, depth = left.shape
    height = depth // (grid.a * grid.b)
    sides = 1 if local else grid.y
    columns = 1 if local else grid.y * grid.c
    many = right.ndim == 5
    blocks = right.shape[1] if many else right.shape[1] // (columns * width)
    lo, count = (0, blocks) if sub is None else sub
    first = row // height

    def right_index(k, i, p):
        if local:
            return (0, 0)
        side = lax.rem(p[2] + k, grid.y)
        core = lax.rem(p[3] + core_step, grid.c)
        if many:
            return (side * grid.c + core, lo + i, 0, 0, 0)
        return (0, (side * grid.c + core) * blocks + lo + i)

    if split == "b":
        shape = (sides, grid.a, total_rows, width)
        specs = [pl.BlockSpec((1, grid.a, height, width), lambda k, i, p: (k, 0, first + i, 0))] * grid.b
        number = grid.b
    elif split == "y":
        shape = (grid.b, grid.a, total_rows, width)

        def index_of(which):
            def index(k, i, p):
                return (0, 0, first + jnp.where(k < which, 0, jnp.where(k > which, count - 1, i)), 0)

            return index

        specs = [pl.BlockSpec((grid.b, grid.a, height, width), index_of(k)) for k in range(sides)]
        number = sides
    else:
        shape = (sides, grid.b, grid.a, total_rows, width)
        specs = [pl.BlockSpec((1, grid.b, grid.a, height, width), lambda k, i, p: (k, 0, 0, first + i, 0))]
        number = 1
    in_specs = [
        pl.BlockSpec((samples, depth), lambda k, i, p: (0, 0), pipeline_mode=pl.Buffered(1)),
        pl.BlockSpec((1, 1, *right.shape[2:]) if many else (samples, width), right_index),
    ]
    operands = [left, right]
    if received is not None:
        in_specs.append(pl.BlockSpec((1, grid.b, grid.a, height, width), lambda k, i, p: (k, 0, 0, first + i, 0)))
        operands.append(received)
    aliases = {}
    if buffers is not None:
        for i, buffer in enumerate(buffers):
            aliases[1 + len(operands)] = i
            in_specs.append(pl.BlockSpec(memory_space=pl.ANY))
            operands.append(buffer)
    body = partial(
        _weight_grad_body, grid=grid, height=height, have_sum=received is not None,
        aliased=0 if buffers is None else len(buffers), split=split,
    )
    work = sides * count * width
    return pl.pallas_call(
        body,
        grid_spec=pltpu.PrefetchScalarGridSpec(
            num_scalar_prefetch=1,
            grid=(sides, count),
            in_specs=in_specs,
            out_specs=specs,
            scratch_shapes=[pltpu.VMEM((grid.b, grid.a, height, samples), BF16)]
            + ([] if height % 128 == 0 else [pltpu.VMEM((depth, samples), BF16)]),
        ),
        out_shape=[jax.ShapeDtypeStruct(shape, BF16)] * number,
        input_output_aliases=aliases,
        compiler_params=pltpu.CompilerParams(vmem_limit_bytes=48 << 20),
        cost_estimate=cost(flops=2 * samples * depth * work, transcendentals=0, bytes_accessed=2 * (samples * (depth + work) + depth * work)),
        name=name,
    )(places, *operands)


def added(parts):
    total = parts[0].astype(F32)
    for part in parts[1:]:
        total = total + part.astype(F32)
    return total


class Reduce:
    def __init__(self, grid, places, pairs, width, order, name, sub=None):
        self.grid, self.places, self.pairs, self.width = grid, places, pairs, width
        self.axes, self.name, self.sub = tuple(order), name, sub
        self.extra, self.result = None, None
        self.heights = [left.shape[1] // (grid.a * grid.b) for left, _ in pairs]
        columns = grid.y * grid.c
        self.counts = [
            right.shape[1] if right.ndim == 5 else right.shape[1] // (columns * width) if sub is None else sub[1]
            for _, right in pairs
        ]

    def _products(self, core_step, split, received, tokens):
        buffers, row = None, 0
        total = sum(h * n for h, n in zip(self.heights, self.counts))
        for i, ((left, right), h, n) in enumerate(zip(self.pairs, self.heights, self.counts)):
            if i == 0 and tokens:
                right = after(right, *tokens)
            buffers = weight_grad(
                self.grid, self.places, left, right, self.width, core_step, total, row, buffers, split,
                received, name=f"{self.name}_{i}_{core_step}", sub=self.sub,
            )
            row += h * n
        return buffers

    def far(self, *tokens):
        self.parts = self._products(1, None, None, tokens)

    def ship(self):
        self.received = self.grid.shift(self.parts[0], "c", 1)

    def near(self, *tokens):
        self.parts = self._products(0, self.axes[0], self.received, tokens)
        return self.parts[0]

    def send(self, stage, *tokens):
        grid, axis = self.grid, self.axes[stage]
        self.stage = stage
        if tokens:
            self.parts = list(lax.optimization_barrier((tuple(self.parts), tokens))[0])
        if self.extra is not None and axis == "b":
            self.parts = [jnp.concatenate([p, q], axis=-2) for p, q in zip(self.parts, self.extra)]
        self.flight = [grid.shift(self.parts[k], axis, k) for k in range(1, grid.size[axis])]

    def land(self):
        parts = [self.parts[0], *self.flight]
        if self.stage == 1:
            half = self.grid.a // 2
            self.parts = [added([p[k * half : (k + 1) * half] for p in parts]).astype(BF16) for k in range(2)]
        else:
            following = self.grid.size[self.axes[1]]
            self.parts = [added([p[k] for p in parts]).astype(BF16) for k in range(following)]


class Bundle:
    def __init__(self, *jobs):
        self.jobs, self.stage, self.result = jobs, 0, None
        self.grid = jobs[0].grid
        self.parts = [jnp.concatenate([job.parts[k] for job in jobs], axis=1) for k in range(2)]

    def send(self):
        self.flight = [self.grid.swap(self.parts[1], 1 << self.stage)]

    def land(self):
        total = [self.parts[0], self.flight[0]]
        self.stage += 1
        if self.stage < self.grid.bits:
            half = self.parts[0].shape[0] // 2
            self.parts = [
                added([part[k * half : (k + 1) * half] for part in total]).astype(BF16)
                for k in range(2)
            ]
            return
        row = 0
        for job in self.jobs:
            height = job.parts[0].shape[1]
            job.result = added([part[0, row : row + height] for part in total])
            row += height
        self.result = True


def gather_everywhere(shard):
    rows = shard.shape[0] // lax.axis_size("seq")
    part = lax.dynamic_slice_in_dim(shard, lax.axis_index("seq") * rows, rows, 0)
    return lax.all_gather(part, ("batch", "seq"), axis=0, tiled=True)


class Share:
    def __init__(self, grid, value):
        self.grid, self.value = grid, value

    def send(self, axis):
        self.flight = spread(self.grid, self.value, axis)[1:]

    def land(self):
        self.value = added([self.value, *self.flight])


class Collect:
    def __init__(self, grid, places, shard):
        self.grid, self.places, self.shape, self.value = grid, places, shard.shape, shard[None, None]

    def send(self, axis):
        self.axis = axis
        self.flight = spread(self.grid, self.value, axis)[1:]

    def land(self):
        self.value = jnp.concatenate([self.value, *self.flight], axis=1 if self.axis == "a" else 0)

    def whole(self):
        grid, places = self.grid, self.places
        value = self.value.reshape(grid.b * grid.a, *self.shape)
        owner = jnp.arange(grid.a * grid.b, dtype=jnp.int32)
        step_a = (places[0] - owner // grid.b) % grid.a
        step_b = (places[1] - owner % grid.b) % grid.b
        value = jnp.take(value, step_b * grid.a + step_a, axis=0)
        return value.transpose(1, 0, 2).reshape(self.shape[0], -1)


def layer_norm(values, scale_row, shift_row):
    center = values - jnp.mean(values, axis=-1, keepdims=True)
    spread = jnp.mean(center * center, axis=-1, keepdims=True)
    return center * lax.rsqrt(spread + epsilon) * scale_row + shift_row


def glu_gate(gated_rows):
    half_width = gated_rows.shape[-1] // 2
    return gated_rows[..., :half_width] * jax.nn.sigmoid(gated_rows[..., half_width:])


def batch_norm(conv_value, sum_first, sum_second, scale_row, shift_row, count_all):
    center = sum_first / count_all
    spread = sum_second / count_all - center * center
    return (conv_value - center) * lax.rsqrt(spread + epsilon) * scale_row + shift_row


def position_table(length, model_width):
    fine = 64
    coarse = 2 * length // fine
    column = jnp.arange(model_width, dtype=jnp.int32)
    rates = jnp.exp((column // 2).astype(jnp.float32) * (-2.0 * math.log(10000.0) / model_width))
    odd = (column % 2 == 1)[None, :]
    start = (jnp.arange(coarse, dtype=jnp.int32) * fine - (length - 1)).astype(jnp.float32)
    large = start[:, None] * rates[None, :]
    small = jnp.arange(fine, dtype=jnp.int32).astype(jnp.float32)[:, None] * rates[None, :]
    sin_large, cos_large = jnp.sin(large), jnp.cos(large)
    first = jnp.where(odd, cos_large, sin_large)[:, None, :]
    second = jnp.where(odd, -sin_large, cos_large)[:, None, :]
    table = first * jnp.cos(small)[None] + second * jnp.sin(small)[None]
    return table.astype(jnp.bfloat16).reshape(2 * length, model_width)


def depth_conv(padded, kernel_rows, length):
    result = kernel_rows[0] * padded[:, 0:length]
    for offset in range(1, kernel_rows.shape[0]):
        result = result + kernel_rows[offset] * padded[:, offset : offset + length]
    return result


def depth_conv_back(padded_grad, kernel_rows, length):
    last_tap = kernel_rows.shape[0] - 1
    result = kernel_rows[0] * padded_grad[:, last_tap : last_tap + length]
    for offset in range(1, last_tap + 1):
        result = (
            result
            + kernel_rows[offset] * padded_grad[:, last_tap - offset : last_tap - offset + length]
        )
    return result


def matmul_rows(left_side, right_side):
    return jnp.dot(left_side, right_side, preferred_element_type=jnp.float32)


def times_transpose(left_side, right_side):
    return lax.dot_general(
        left_side, right_side, (((1,), (1,)), ((), ())), preferred_element_type=jnp.float32
    )


def transpose_times(left_side, right_side):
    return lax.dot_general(
        left_side, right_side, (((0,), (0,)), ((), ())), preferred_element_type=jnp.float32
    )


def linear_back(grad_rows, weight):
    grad_low = grad_rows.astype(jnp.bfloat16)
    return (times_transpose(grad_low, weight), grad_low)


def ffn_enter(values, scale_row, shift_row, weight_in):
    normed_low = layer_norm(values, scale_row, shift_row).astype(jnp.bfloat16)
    hidden_pre = matmul_rows(normed_low, weight_in)
    hidden_low = jax.nn.silu(hidden_pre).astype(jnp.bfloat16)
    return (normed_low, hidden_pre.astype(jnp.bfloat16), hidden_low)


def ffn_forward(values, scale_row, shift_row, weight_in, weight_out):
    saved = ffn_enter(values, scale_row, shift_row, weight_in)
    return (matmul_rows(saved[2], weight_out), saved)


def ffn_backward_exit(grad_rows, weight_out, saved_parts):
    grad_hidden, grad_out_low = linear_back(grad_rows, weight_out)
    silu_value, silu_back = jax.vjp(jax.nn.silu, saved_parts[1].astype(jnp.float32))
    return (silu_back(grad_hidden)[0].astype(jnp.bfloat16), grad_out_low)


def ffn_backward_entry(grad_pre_low, values, scale_row, shift_row, weight_in):
    norm_value, norm_back = jax.vjp(layer_norm, values, scale_row, shift_row)
    return norm_back(times_transpose(grad_pre_low, weight_in))


def ffn_backward(grad_rows, values, scale_row, shift_row, weight_in, weight_out, saved_parts):
    normed_low, hidden_pre, hidden_low = saved_parts
    grad_hidden, grad_out_low = linear_back(grad_rows, weight_out)
    silu_value, silu_back = jax.vjp(jax.nn.silu, hidden_pre.astype(jnp.float32))
    grad_pre = silu_back(grad_hidden)[0]
    grad_normed, grad_pre_low = linear_back(grad_pre, weight_in)
    norm_value, norm_back = jax.vjp(layer_norm, values, scale_row, shift_row)
    grad_values, grad_scale, grad_shift = norm_back(grad_normed)
    return (grad_values, grad_scale, grad_shift, grad_pre_low, grad_out_low)


def sum_everywhere(value):
    for axis in ("seq", "batch"):
        size, step = lax.axis_size(axis), 1
        while step < size:
            value = value + lax.ppermute(value, axis, [(i, i ^ step) for i in range(size)])
            step *= 2
    return value


def per_device(
    grid,
    acoustic_sequence,
    utterance_durations,
    chosen_entry_number,
    discretizer_score_perturbation,
    softmax_heat,
    normalizer_affine_rows,
    discretizer_score_projection,
    lexicon_vectors,
    opening_dense_entry_projection,
    opening_dense_exit_projection,
    request_projection,
    lookup_projection,
    content_projection_kernel,
    relative_offset_projection,
    mixing_exit_projection,
    unit_kernel_before_gating,
    channelwise_filter_coefficients,
    unit_kernel_after_normalizing,
    closing_dense_entry_projection,
    closing_dense_exit_projection,
    result_adjoint,
    discrete_label_adjoint,
):
    places = grid.places()
    small = Collect(
        grid,
        places,
        jnp.concatenate([normalizer_affine_rows, channelwise_filter_coefficients], axis=0),
    )
    vector_rows = normalizer_affine_rows.shape[0]
    model_width = acoustic_sequence.shape[2]
    piece_width = model_width // (grid.y * grid.c)
    gather = partial(Gather, grid, places)
    second = gather([opening_dense_exit_projection], piece_width, True, "gather_opening_exit")
    sixth = gather([closing_dense_exit_projection], piece_width, False, "gather_closing_exit")
    third = gather(
        [request_projection, lookup_projection, content_projection_kernel, relative_offset_projection],
        piece_width,
        False,
        "gather_attention",
    )
    macaron_in_all = gather_everywhere(opening_dense_entry_projection)
    small.send("a")
    second.send("a")
    settle([small, second])
    small.send("b")
    second.send("b")
    third.send("a")
    settle([small, second, third])
    small_all = small.whole()
    vectors_all, depth_all = small_all[:vector_rows], small_all[vector_rows:]
    middle_shards = (
        mixing_exit_projection,
        unit_kernel_after_normalizing,
        unit_kernel_before_gating,
        discretizer_score_projection,
        lexicon_vectors,
    )
    middle_shards, entry_shard, second.value = lax.optimization_barrier(
        (middle_shards, closing_dense_entry_projection, second.value)
    )
    middle_all = gather_everywhere(jnp.concatenate(middle_shards, axis=1))
    out_all, conv_out_all, conv_in_all, quant_all, codebook_all = jnp.split(
        middle_all, [model_width * i for i in (1, 2, 4, 5)], axis=1
    )
    closing_in_all = gather_everywhere(entry_shard)
    groups, local_len, model_width = acoustic_sequence.shape
    seq_count = lax.axis_size("seq")
    seq_place = lax.axis_index("seq")
    full_len = local_len * seq_count
    entries = lexicon_vectors.shape[0] * grid.a * grid.b
    total_rows = groups * local_len
    local_width = model_width // seq_count
    kernel_size = depth_all.shape[0]
    rim_width = kernel_size // 2
    height = model_width // (grid.a * grid.b)
    params_f = vectors_all.astype(jnp.float32)
    depth_f = depth_all.astype(jnp.float32)
    positions = seq_place * local_len + jnp.arange(local_len, dtype=jnp.int32)
    valid_mask = (positions[None, :] < utterance_durations[:, None]).astype(jnp.float32)
    valid_rows = valid_mask.reshape(total_rows, 1)
    inputs_low = acoustic_sequence.reshape(total_rows, model_width)
    inputs_f = inputs_low.astype(jnp.float32)
    second.send("y")
    third.send("b")
    macaron_saved = ffn_enter(inputs_f, params_f[0], params_f[5], macaron_in_all)
    sixth.send("a")
    macaron_hidden = settle([second, third, sixth], macaron_saved[2])
    sixth.send("b")
    macaron_saved = (*macaron_saved[:2], macaron_hidden)
    (macaron_out_all,) = second.whole()
    query_all, key_all, value_all, pos_all = third.whole()
    macaron_value = matmul_rows(macaron_hidden, macaron_out_all)
    first_mid = inputs_f + 0.5 * macaron_value
    attn_normed = layer_norm(first_mid, params_f[1], params_f[6]).astype(jnp.bfloat16)
    stacked = project_heads(attn_normed, [query_all, key_all, value_all], groups, seq_count)
    by_heads = lax.all_to_all(stacked, "seq", split_axis=0, concat_axis=0, tiled=True)
    table_low = position_table(full_len, model_width)
    pos_columns = lax.dynamic_slice_in_dim(pos_all, seq_place * local_width, local_width, 1)
    position_low = matmul_rows(table_low, pos_columns).astype(jnp.bfloat16)
    biases = lax.dynamic_slice_in_dim(params_f[12:14], seq_place * local_width, local_width, 1)
    by_heads, position_low = settle([], by_heads, position_low)
    attended_low, probs = attend_forward(by_heads, position_low, biases, utterance_durations)
    attended_low = settle([sixth], attended_low)
    back_time = lax.all_to_all(
        attended_low, "seq", split_axis=0, concat_axis=0, tiled=True
    )
    attended_rows = back_time.transpose(1, 2, 0, 3).reshape(total_rows, model_width)
    second_mid = first_mid + matmul_rows(attended_rows, out_all)
    conv_normed = layer_norm(second_mid, params_f[2], params_f[7]).astype(jnp.bfloat16)
    gated_rows = matmul_rows(conv_normed, conv_in_all)
    glu_low = (
        (valid_rows * glu_gate(gated_rows))
        .astype(jnp.bfloat16)
        .reshape(groups, local_len, model_width)
    )
    padded_glu = extended(glu_low, (("seq", 1),), rim_width)
    conv_value = depth_conv(padded_glu, depth_f, local_len).reshape(total_rows, model_width)
    masked_conv = valid_rows * conv_value
    sums = sum_everywhere(
        jnp.stack(
            [
                jnp.sum(masked_conv, axis=0),
                jnp.sum(masked_conv * conv_value, axis=0),
                jnp.broadcast_to(jnp.sum(valid_mask), (model_width,)),
            ]
        )
    )
    sum_first, sum_second, count_all = sums[0], sums[1], sums[2]
    bound_norm = partial(batch_norm, count_all=count_all)
    normalized = bound_norm(conv_value, sum_first, sum_second, params_f[10], params_f[11])
    act_low = jax.nn.silu(normalized).astype(jnp.bfloat16)
    (closing_out_all,) = sixth.whole()
    third_mid = second_mid + matmul_rows(act_low, conv_out_all)
    closing_value, closing_saved = ffn_forward(
        third_mid, params_f[3], params_f[8], closing_in_all, closing_out_all
    )
    quant_logits = matmul_rows(inputs_low, quant_all)
    scaled_logits = (
        quant_logits
        + discretizer_score_perturbation.reshape(total_rows, entries).astype(jnp.float32)
    ) / softmax_heat
    relaxed_assignments = jax.nn.softmax(scaled_logits, axis=-1)
    soft_low = relaxed_assignments.astype(jnp.bfloat16)
    one_hot = (
        chosen_entry_number.reshape(total_rows, 1) == jnp.arange(entries, dtype=jnp.int32)[None, :]
    ).astype(jnp.bfloat16)
    codes_value = valid_rows * (
        matmul_rows(one_hot, codebook_all) + matmul_rows(soft_low, codebook_all)
    )
    grad_codes = (
        valid_rows * discrete_label_adjoint.reshape(total_rows, model_width).astype(jnp.float32)
    ).astype(jnp.bfloat16)
    grad_soft = times_transpose(grad_codes, codebook_all)
    rescaled_derivative = relaxed_assignments * (
        grad_soft - jnp.sum(grad_soft * relaxed_assignments, axis=-1, keepdims=True)
    )
    score_derivative_lowprecision = (rescaled_derivative / softmax_heat).astype(jnp.bfloat16)
    grad_quant_in = times_transpose(score_derivative_lowprecision, quant_all)
    fourth_mid = third_mid + 0.5 * closing_value
    final_value, final_back = jax.vjp(layer_norm, fourth_mid, params_f[4], params_f[9])
    output = (valid_rows * final_value).astype(jnp.bfloat16).reshape(groups, local_len, model_width)
    codes = codes_value.astype(jnp.bfloat16).reshape(groups, local_len, model_width)
    grad_final = valid_rows * result_adjoint.reshape(total_rows, model_width).astype(jnp.float32)
    grad_fourth, scale_four, shift_four = final_back(grad_final)
    grad_closing, scale_three, shift_three, close_pre_low, close_out_low = ffn_backward(
        0.5 * grad_fourth,
        third_mid,
        params_f[3],
        params_f[8],
        closing_in_all,
        closing_out_all,
        closing_saved,
    )
    grad_third = grad_fourth + grad_closing
    close_normed, close_pre, close_hidden = closing_saved
    reduce = partial(Reduce, grid, places)
    closing_job = reduce(
        [(close_hidden, close_out_low), (close_normed, close_pre_low)], piece_width, "by", "closing"
    )
    closing_job.far()
    closing_job.ship()
    grad_act, grad_third_low = linear_back(grad_third, conv_out_all)
    silu_value, silu_back = jax.vjp(jax.nn.silu, normalized)
    grad_normalized = silu_back(grad_act)[0]
    norm_value, norm_back = jax.vjp(
        bound_norm, conv_value, sum_first, sum_second, params_f[10], params_f[11]
    )
    grad_conv_direct, part_first, part_second, grad_bn_scale, grad_bn_shift = norm_back(
        grad_normalized
    )
    totals = sum_everywhere(jnp.stack([part_first, part_second]))
    chosen_soft = one_hot + soft_low
    early_job = reduce(
        [
            (act_low, grad_third_low),
            (inputs_low, score_derivative_lowprecision),
            (chosen_soft, grad_codes),
        ],
        piece_width,
        "yb",
        "early",
    )
    early_job.far()
    early_job.ship()
    closing_job.near()
    early_job.near()
    totals = settle([], totals, hold=[closing_job, early_job])
    closing_job.send(0)
    early_job.send(0)
    total_first, total_second = totals[0], totals[1]
    grad_conv = grad_conv_direct + valid_rows * (total_first + 2.0 * conv_value * total_second)
    grad_conv_low = grad_conv.astype(jnp.bfloat16).reshape(groups, local_len, model_width)
    padded_grad = extended(grad_conv_low, (("seq", 1),), rim_width)
    grad_glu = valid_rows * depth_conv_back(padded_grad, depth_f, local_len).reshape(
        total_rows, model_width
    )
    grad_conv_float = grad_conv_low.astype(jnp.float32)
    grad_depth = jnp.stack(
        [
            jnp.sum(
                padded_glu[:, offset : offset + local_len].astype(jnp.float32) * grad_conv_float,
                axis=(0, 1),
            )
            for offset in range(kernel_size)
        ]
    )
    glu_value, glu_back = jax.vjp(glu_gate, gated_rows)
    grad_gated = glu_back(grad_glu)[0]
    grad_conv_normed, grad_gated_low = linear_back(grad_gated, conv_in_all)
    conv_norm_value, conv_norm_back = jax.vjp(layer_norm, second_mid, params_f[2], params_f[7])
    grad_from_conv, scale_two, shift_two = conv_norm_back(grad_conv_normed)
    grad_second = grad_third + grad_from_conv
    grad_second_low = grad_second.astype(jnp.bfloat16)
    grad_attended = unproject_heads(grad_second_low, out_all, groups, seq_count)
    grad_heads = lax.all_to_all(grad_attended, "seq", split_axis=0, concat_axis=0, tiled=True)

    middle_job = reduce(
        [(conv_normed, grad_gated_low), (attended_rows, grad_second_low)],
        piece_width,
        "by",
        "middle",
    )
    middle_job.far()
    grad_heads = settle([], grad_heads, hold=[middle_job])
    middle_job.ship()
    grad_stack, grad_position_low, grad_biases = attend_backward(
        probs, by_heads, grad_heads, position_low, biases
    )
    grad_stack = settle([early_job], grad_stack)
    grad_time = lax.all_to_all(grad_stack, "seq", split_axis=0, concat_axis=0, tiled=True)
    position_parts = weight_grad(
        grid, places, table_low, grad_position_low, piece_width, 0, height, 0, None, "b",
        name="position_grad", local=True,
    )
    middle_job.near()
    grad_time, *position_parts = settle(
        [closing_job], grad_time, *position_parts, hold=[middle_job]
    )
    closing_job.send(1)
    early_job.send(1)
    middle_job.send(0)
    grad_attn_normed = join_heads(grad_time, [query_all, key_all, value_all])
    attn_norm_value, attn_norm_back = jax.vjp(layer_norm, first_mid, params_f[1], params_f[6])
    grad_from_attn, scale_one, shift_one = attn_norm_back(grad_attn_normed)
    grad_first = grad_second + grad_from_attn
    attention_job = reduce(
        [(attn_normed, grad_time)], piece_width, "yb", "attention"
    )
    attention_job.extra = [part[0] for part in position_parts]
    attention_job.far()
    attention_job.ship()
    content_full, position_full = lax.dynamic_update_slice_in_dim(
        jnp.zeros((2, model_width), jnp.float32), grad_biases, seq_place * local_width, 1
    )
    mac_normed, mac_pre, mac_hidden = macaron_saved
    mac_out_low = (0.5 * grad_first).astype(jnp.bfloat16)
    macaron_out_job = reduce([(mac_hidden, mac_out_low)], piece_width, "by", "opening_exit")
    macaron_out_job.far()
    macaron_out_job.ship()
    attention_job.near()
    macaron_out_job.near()
    mac_out_low = settle([], mac_out_low, hold=[attention_job, macaron_out_job])
    attention_job.send(0)
    macaron_out_job.send(0)
    mac_pre_low, mac_out_low = ffn_backward_exit(mac_out_low, macaron_out_all, macaron_saved)
    halves = mac_pre_low.shape[1] // model_width // 2
    macaron_in_jobs = [
        reduce([(mac_normed, mac_pre_low)], piece_width, order, name, sub=(i * halves, halves))
        for i, (order, name) in enumerate((("yb", "opening_entry"), ("by", "opening_entry_more")))
    ]
    for job in macaron_in_jobs:
        job.far()
    mac_pre_low = settle(
        [closing_job, early_job, middle_job], mac_pre_low, hold=macaron_in_jobs
    )
    for job in macaron_in_jobs:
        job.ship()
    first_tails = Bundle(closing_job, early_job)
    first_tails.send()
    middle_job.send(1)
    grad_macaron, scale_zero, shift_zero = ffn_backward_entry(
        mac_pre_low, inputs_f, params_f[0], params_f[5], macaron_in_all
    )
    grad_layer_in = grad_first + grad_macaron
    frames_grad = (
        (grad_layer_in + grad_quant_in).astype(jnp.bfloat16).reshape(groups, local_len, model_width)
    )
    vectors_grad = jnp.stack(
        [
            scale_zero,
            scale_one,
            scale_two,
            scale_three,
            scale_four,
            shift_zero,
            shift_one,
            shift_two,
            shift_three,
            shift_four,
            grad_bn_scale,
            grad_bn_shift,
            content_full,
            position_full,
        ]
    )
    small = Share(grid, jnp.concatenate([vectors_grad, grad_depth], axis=0))
    small.send("c")
    small.land()
    for job in macaron_in_jobs:
        job.near()
    small.value = settle(
        [first_tails, middle_job, attention_job, macaron_out_job],
        small.value,
        hold=macaron_in_jobs,
    )
    for job in macaron_in_jobs:
        job.send(0)
    attention_job.send(1)
    macaron_out_job.send(1)
    first_tails.send()
    middle_tails = Bundle(middle_job)
    middle_tails.send()
    small.send("y")
    settle([small, first_tails, middle_tails, attention_job, macaron_out_job, *macaron_in_jobs])
    for job in macaron_in_jobs:
        job.send(1)
    late_tails = Bundle(attention_job, macaron_out_job)
    late_tails.send()
    middle_tails.send()
    small.send("b")
    settle([small, middle_tails, late_tails, *macaron_in_jobs])
    late_tails.send()
    last_tails = Bundle(*macaron_in_jobs)
    last_tails.send()
    small.send("a")
    settle([small, last_tails, late_tails])
    last_tails.send()
    settle([last_tails])
    small_width = model_width // (grid.a * grid.b)
    small_sums = lax.dynamic_slice_in_dim(
        small.value, lax.axis_index("batch") * small_width, small_width, 1
    )
    vectors_sum, depth_sum = small_sums[:vector_rows], small_sums[vector_rows:]

    def rows_of(job, count):
        return (job.result[i * height : (i + 1) * height] for i in range(count))

    exit_rows = close_hidden.shape[1] // (grid.a * grid.b)
    closing_out_sum, closing_in_sum = closing_job.result[:exit_rows], closing_job.result[exit_rows:]
    conv_out_sum, quant_sum, codebook_sum = rows_of(early_job, 3)
    conv_in_sum, out_sum = middle_job.result[: 2 * height], middle_job.result[2 * height :]
    query_sum, key_sum, value_sum, pos_sum = rows_of(attention_job, 4)
    macaron_out_sum = macaron_out_job.result
    macaron_in_sum = jnp.concatenate([job.result for job in macaron_in_jobs])

    def side_by_side(blocks):
        return jnp.concatenate(
            [blocks[i : i + height] for i in range(0, blocks.shape[0], height)], axis=1
        )

    closing_in_sum, conv_in_sum, macaron_in_sum = (
        side_by_side(closing_in_sum),
        side_by_side(conv_in_sum),
        side_by_side(macaron_in_sum),
    )
    return (
        output,
        codes,
        frames_grad,
        vectors_sum,
        quant_sum,
        codebook_sum,
        macaron_in_sum,
        macaron_out_sum,
        query_sum,
        key_sum,
        value_sum,
        pos_sum,
        out_sum,
        conv_in_sum,
        depth_sum,
        conv_out_sum,
        closing_in_sum,
        closing_out_sum,
    )


def solution(mesh):
    placed = (
        P("batch", "seq", None),
        P("batch"),
        P("batch", "seq"),
        P("batch", "seq", None),
        P(),
        P(None, "batch"),
        P("batch", None),
        P("batch", None),
        P("batch", None),
        P("batch", None),
        P("batch", None),
        P("batch", None),
        P("batch", None),
        P("batch", None),
        P("batch", None),
        P("batch", None),
        P(None, "batch"),
        P("batch", None),
        P("batch", None),
        P("batch", None),
        P("batch", "seq", None),
        P("batch", "seq", None),
    )
    return jax.shard_map(
        partial(per_device, Grid(mesh)),
        mesh=mesh,
        in_specs=placed,
        out_specs=(
            P("batch", "seq", None),
            P("batch", "seq", None),
            P("batch", "seq", None),
            P(None, "batch"),
            P("batch", "seq"),
            P("batch", "seq"),
            P("batch", "seq"),
            P("batch", "seq"),
            P("batch", "seq"),
            P("batch", "seq"),
            P("batch", "seq"),
            P("batch", "seq"),
            P("batch", "seq"),
            P("batch", "seq"),
            P(None, "batch"),
            P("batch", "seq"),
            P("batch", "seq"),
            P("batch", "seq"),
        ),
        check_vma=False,
    )
```

```python
from functools import partial
import math

import jax
import jax.numpy as jnp
from jax import lax
from jax.experimental import pallas as pl
from jax.experimental.pallas import tpu as pltpu
from jax.sharding import PartitionSpec as P

HEAD_WIDTH = 128


epsilon = 1e-05

F32, BF16 = jnp.float32, jnp.bfloat16
SHARE = 4


def cost(flops, transcendentals, bytes_accessed):
    return pl.CostEstimate(
        flops=flops // SHARE,
        transcendentals=transcendentals // SHARE,
        bytes_accessed=bytes_accessed // SHARE,
    )


def dot(a, b, ca, cb):
    return lax.dot_general(a, b, (((ca,), (cb,)), ((), ())), preferred_element_type=F32)

def _fwd_body(len_ref, q_ref, k_ref, v_ref, pos_ref, bias_ref, o_ref, p_ref, *, rows, full, scale):
    block = pl.program_id(2)
    length = len_ref[pl.program_id(0)]
    query = q_ref[0, 0, 0].astype(F32)
    content_query = (query + bias_ref[0:1, :]).astype(BF16)
    position_query = (query + bias_ref[1:2, :]).astype(BF16)
    content = dot(content_query, k_ref[:, 0, 0].reshape(full, -1), 1, 1)
    span = full + rows
    start = pl.multiple_of(full - rows - block * rows, rows)
    relative = dot(position_query, pos_ref[pl.ds(start, span), :], 1, 1)
    relative = pltpu.roll(relative, span - (rows - 1), 1, stride=1, stride_axis=0)
    raw = content + relative[:, :full]
    seen = lax.broadcasted_iota(jnp.int32, raw.shape, 1) < length
    scores = jnp.where(seen, raw * scale, -1e30)
    top = jnp.max(scores, axis=-1, keepdims=True)
    weights = jnp.exp(scores - top)
    total = jnp.sum(weights, axis=-1, keepdims=True)
    low = (weights * (1.0 / total)).astype(BF16)
    p_ref[0, 0] = low
    o_ref[0, 0] = dot(low, v_ref[:, 0, 0].reshape(full, -1), 1, 0).astype(BF16)

def attend_forward(by_heads, position, bias, lengths):
    parts, _, groups, rows, width = by_heads.shape
    depth, full = HEAD_WIDTH, parts * rows
    heads = width // depth
    body = partial(_fwd_body, rows=rows, full=full, scale=1.0 / math.sqrt(depth))
    flops = groups * heads * full * (2 * full * depth * 3 + 2 * rows * depth)
    return pl.pallas_call(
        body,
        grid_spec=pltpu.PrefetchScalarGridSpec(
            num_scalar_prefetch=1,
            grid=(groups, heads, parts),
            in_specs=[
                pl.BlockSpec((1, 1, 1, rows, depth), lambda u, h, i, n: (i, 0, u, 0, h)),
                pl.BlockSpec((parts, 1, 1, rows, depth), lambda u, h, i, n: (0, 1, u, 0, h)),
                pl.BlockSpec((parts, 1, 1, rows, depth), lambda u, h, i, n: (0, 2, u, 0, h)),
                pl.BlockSpec((2 * full, depth), lambda u, h, i, n: (0, h)),
                pl.BlockSpec((2, depth), lambda u, h, i, n: (0, h)),
            ],
            out_specs=[
                pl.BlockSpec((1, 1, rows, depth), lambda u, h, i, n: (i, u, 0, h)),
                pl.BlockSpec((1, 1, rows, full), lambda u, h, i, n: (u, h, i, 0)),
            ],
        ),
        out_shape=[
            jax.ShapeDtypeStruct((parts, groups, rows, width), BF16),
            jax.ShapeDtypeStruct((groups, heads, full, full), BF16),
        ],
        compiler_params=pltpu.CompilerParams(vmem_limit_bytes=48 << 20),
        cost_estimate=cost(flops=flops, transcendentals=groups * heads * full * full, bytes_accessed=groups * heads * full * full * 2 + 5 * groups * full * width * 2),
        name="attend_forward",
    )(lengths, by_heads, by_heads, by_heads, position, bias)

def _bwd_body(p_ref, q_ref, k_ref, v_ref, g_ref, pos_ref, bias_ref, d_ref, dpos_ref, dbias_ref,
              key_acc, value_acc, pos_acc, bias_acc, *, rows, full, scale):
    group, block = pl.program_id(1), pl.program_id(2)
    last_block = block == pl.num_programs(2) - 1

    @pl.when((group == 0) & (block == 0))
    def _():
        pos_acc[...] = jnp.zeros_like(pos_acc)
        bias_acc[...] = jnp.zeros_like(bias_acc)

    @pl.when(block == 0)
    def _():
        key_acc[...] = jnp.zeros_like(key_acc)
        value_acc[...] = jnp.zeros_like(value_acc)

    query = q_ref[0, 0, 0].astype(F32)
    content_query = (query + bias_ref[0:1, :]).astype(BF16)
    position_query = (query + bias_ref[1:2, :]).astype(BF16)
    keys, values, grad = k_ref[:, 0, 0].reshape(full, -1), v_ref[:, 0, 0].reshape(full, -1), g_ref[0, 0]
    low = p_ref[0, 0]
    weights = low.astype(F32)
    grad_weights = dot(grad, values, 1, 1)
    value_acc[...] += dot(grad, low, 0, 0)
    inner = jnp.sum(grad_weights * weights, axis=-1, keepdims=True)
    grad_raw = (weights * (grad_weights - inner) * scale).astype(BF16)
    key_acc[...] += dot(content_query, grad_raw, 0, 0)
    grad_content = dot(grad_raw, keys, 1, 0)
    row = lax.broadcasted_iota(jnp.int32, (rows, rows), 0)
    column = lax.broadcasted_iota(jnp.int32, (rows, rows), 1)
    flip = jnp.where(row + column == rows - 1, 1.0, 0.0).astype(BF16)
    span = full + rows
    start = pl.multiple_of(full - rows - block * rows, rows)
    turned = jnp.concatenate([dot(flip, grad_raw, 1, 0).astype(BF16), jnp.zeros((rows, rows), BF16)], axis=1)
    turned = pltpu.roll(turned, 0, 1, stride=1, stride_axis=0)
    turned_query = dot(flip, position_query, 1, 0).astype(BF16)
    pos_acc[:, pl.ds(start, span)] += dot(turned_query, turned, 0, 0)
    grad_turned = dot(turned, pos_ref[pl.ds(start, span), :], 1, 0)
    high = grad_turned.astype(BF16)
    rest = (grad_turned - high.astype(F32)).astype(BF16)
    grad_position = dot(flip, high, 1, 0) + dot(flip, rest, 1, 0)
    d_ref[block, 0, 0] = (grad_content + grad_position).astype(BF16)
    bias_acc[0:1, :] += jnp.sum(grad_content, axis=0, keepdims=True)
    bias_acc[1:2, :] += jnp.sum(grad_position, axis=0, keepdims=True)

    @pl.when(last_block)
    def _():
        d_ref[:, 1, 0] = key_acc[...].T.astype(BF16).reshape(full // rows, rows, -1)
        d_ref[:, 2, 0] = value_acc[...].T.astype(BF16).reshape(full // rows, rows, -1)

    @pl.when(last_block & (group == pl.num_programs(1) - 1))
    def _():
        dpos_ref[...] = pos_acc[...].T.astype(BF16)
        dbias_ref[...] = bias_acc[...]

def attend_backward(probs, by_heads, grad_heads, position, bias):
    parts, _, groups, rows, width = by_heads.shape
    depth, full = HEAD_WIDTH, parts * rows
    heads = width // depth
    body = partial(_bwd_body, rows=rows, full=full, scale=1.0 / math.sqrt(depth))
    flops = groups * heads * full * (2 * full * depth * 7 + 6 * rows * depth)
    return pl.pallas_call(
        body,
        grid_spec=pltpu.PrefetchScalarGridSpec(
            num_scalar_prefetch=0,
            grid=(heads, groups, parts),
            in_specs=[
                pl.BlockSpec((1, 1, rows, full), lambda h, u, i: (u, h, i, 0)),
                pl.BlockSpec((1, 1, 1, rows, depth), lambda h, u, i: (i, 0, u, 0, h)),
                pl.BlockSpec((parts, 1, 1, rows, depth), lambda h, u, i: (0, 1, u, 0, h)),
                pl.BlockSpec((parts, 1, 1, rows, depth), lambda h, u, i: (0, 2, u, 0, h)),
                pl.BlockSpec((1, 1, rows, depth), lambda h, u, i: (i, u, 0, h)),
                pl.BlockSpec((2 * full, depth), lambda h, u, i: (0, h)),
                pl.BlockSpec((2, depth), lambda h, u, i: (0, h)),
            ],
            out_specs=[
                pl.BlockSpec((parts, 3, 1, rows, depth), lambda h, u, i: (0, 0, u, 0, h)),
                pl.BlockSpec((2 * full, depth), lambda h, u, i: (0, h)),
                pl.BlockSpec((2, depth), lambda h, u, i: (0, h)),
            ],
            scratch_shapes=[
                pltpu.VMEM((depth, full), F32),
                pltpu.VMEM((depth, full), F32),
                pltpu.VMEM((depth, 2 * full), F32),
                pltpu.VMEM((2, depth), F32),
            ],
        ),
        out_shape=[
            jax.ShapeDtypeStruct((parts, 3, groups, rows, width), BF16),
            jax.ShapeDtypeStruct((2 * full, width), BF16),
            jax.ShapeDtypeStruct((2, width), F32),
        ],
        compiler_params=pltpu.CompilerParams(vmem_limit_bytes=48 << 20),
        cost_estimate=cost(flops=flops, transcendentals=0, bytes_accessed=groups * heads * full * full * 2 + 8 * groups * full * width * 2),
        name="attend_backward",
    )(probs, by_heads, by_heads, by_heads, grad_heads, position, bias)


def extended(value, sides, width):
    for axis, dim in sides:
        size, length = (lax.axis_size(axis), value.shape[dim])
        up = [(i, (i + 1) % size) for i in range(size - 1)]
        down = [(j, i) for i, j in up]
        last = lax.slice_in_dim(value, length - width, length, axis=dim)
        initial = lax.slice_in_dim(value, 0, width, axis=dim)
        before = lax.ppermute(last, axis, up)
        after = lax.ppermute(initial, axis, down)
        value = jnp.concatenate([before, value, after], axis=dim)
    return value


def _project_body(left_ref, *refs):
    out = refs[-1]
    for i, weight in enumerate(refs[:-1]):
        out[0, i] = dot(left_ref[...], weight[...], 1, 0).astype(BF16).reshape(out.shape[2:])


def project_heads(left, weights, groups, parts):
    rows, depth = left.shape
    width = weights[0].shape[1] // parts
    shape = (parts, len(weights), groups, rows // groups, width)
    return pl.pallas_call(
        _project_body,
        grid=(parts,),
        in_specs=[pl.BlockSpec((rows, depth), lambda s: (0, 0))]
        + [pl.BlockSpec((depth, width), lambda s: (0, s))] * len(weights),
        out_specs=pl.BlockSpec((1, *shape[1:]), lambda s: (s, 0, 0, 0, 0)),
        out_shape=jax.ShapeDtypeStruct(shape, BF16),
        compiler_params=pltpu.CompilerParams(vmem_limit_bytes=48 << 20),
        cost_estimate=cost(flops=2 * rows * depth * width * parts * len(weights), transcendentals=0, bytes_accessed=2 * len(weights) * (rows + depth) * width * parts + 2 * rows * depth),
        name="project_heads",
    )(left, *weights)


def _unproject_body(left_ref, weight_ref, out_ref):
    out_ref[0] = dot(left_ref[...], weight_ref[...], 1, 1).astype(BF16).reshape(out_ref.shape[1:])


def unproject_heads(left, weight, groups, parts):
    rows, depth = left.shape
    width = weight.shape[0] // parts
    shape = (parts, groups, rows // groups, width)
    return pl.pallas_call(
        _unproject_body,
        grid=(parts,),
        in_specs=[
            pl.BlockSpec((rows, depth), lambda s: (0, 0)),
            pl.BlockSpec((width, depth), lambda s: (s, 0)),
        ],
        out_specs=pl.BlockSpec((1, *shape[1:]), lambda s: (s, 0, 0, 0)),
        out_shape=jax.ShapeDtypeStruct(shape, BF16),
        compiler_params=pltpu.CompilerParams(vmem_limit_bytes=48 << 20),
        cost_estimate=cost(flops=2 * rows * depth * width * parts, transcendentals=0, bytes_accessed=2 * (rows + depth) * width * parts + 2 * rows * depth),
        name="unproject_heads",
    )(left, weight)


def _join_body(grad_ref, *refs):
    out = refs[-1]

    @pl.when(pl.program_id(0) == 0)
    def _():
        out[...] = jnp.zeros_like(out)

    total = out[...]
    for i, weight in enumerate(refs[:-1]):
        total = total + dot(grad_ref[0, i].reshape(out.shape[0], -1), weight[...], 1, 1)
    out[...] = total


def join_heads(grads, weights):
    parts, count, groups, frames, width = grads.shape
    rows, depth = groups * frames, weights[0].shape[0]
    return pl.pallas_call(
        _join_body,
        grid=(parts,),
        in_specs=[pl.BlockSpec((1, count, groups, frames, width), lambda s: (s, 0, 0, 0, 0))]
        + [pl.BlockSpec((depth, width), lambda s: (0, s))] * count,
        out_specs=pl.BlockSpec((rows, depth), lambda s: (0, 0)),
        out_shape=jax.ShapeDtypeStruct((rows, depth), F32),
        compiler_params=pltpu.CompilerParams(vmem_limit_bytes=48 << 20),
        cost_estimate=cost(flops=2 * rows * depth * width * parts * count, transcendentals=0, bytes_accessed=2 * count * (rows + depth) * width * parts + 4 * rows * depth),
        name="join_heads",
    )(grads, *weights)


def line_factors(line):
    places = [(*device.coords, device.core_on_chip) for device in line]
    moving = [first != second for first, second in zip(places[0], places[1])].index(True)
    inner = len({place[moving] for place in places})
    return len(places) // inner, inner


class Grid:
    def __init__(self, mesh):
        devices = mesh.devices
        self.a, self.b = line_factors(list(devices[:, 0]))
        self.y, self.c = line_factors(list(devices[0, :]))
        self.size = {"a": self.a, "b": self.b, "y": self.y, "c": self.c}
        self.bits = self.a.bit_length() - 1

    def places(self):
        batch, seq = lax.axis_index("batch"), lax.axis_index("seq")
        return jnp.stack([batch // self.b, batch % self.b, seq // self.c, seq % self.c]).astype(jnp.int32)

    def shift(self, value, axis, step):
        name = "batch" if axis in "ab" else "seq"
        outer, inner = (self.a, self.b) if axis in "ab" else (self.y, self.c)
        pairs = []
        for i in range(outer):
            for j in range(inner):
                if axis in "ay":
                    pairs.append((i * inner + j, (i + step) % outer * inner + j))
                else:
                    pairs.append((i * inner + j, i * inner + (j + step) % inner))
        return lax.ppermute(value, name, pairs)

    def swap(self, value, step):
        pairs = [
            (i * self.b + j, (i ^ step) * self.b + j) for i in range(self.a) for j in range(self.b)
        ]
        return lax.ppermute(value, "batch", pairs)


def after(value, *tokens):
    return lax.optimization_barrier((value, *tokens))[0]


def settle(jobs, *tokens, hold=()):
    flights = tuple(tuple(job.flight) for job in jobs)
    parts = tuple(tuple(job.parts) for job in hold)
    landed, tokens, parts = lax.optimization_barrier((flights, tokens, parts))
    for job, held in zip(hold, parts):
        job.parts = list(held)
    for job, flight in zip(jobs, landed):
        job.flight = list(flight)
        job.land()
    moving = [job for job in jobs if isinstance(job, (Reduce, Bundle)) and job.result is None]
    if tokens and moving:
        parts = tuple(tuple(job.parts) for job in moving)
        tokens, parts = lax.optimization_barrier((tokens, parts))
        for job, held in zip(moving, parts):
            job.parts = list(held)
    return tokens[0] if len(tokens) == 1 else tokens


def bit_reversed(value, bits):
    return sum((value >> i & 1) << (bits - 1 - i) for i in range(bits))


def spread(grid, value, axis):
    return [value] + [grid.shift(value, axis, k) for k in range(1, grid.size[axis])]


def pieces(weights, place, count, width):
    rows = []
    for weight in weights:
        wide = weight.shape[1] // count
        piece = lax.dynamic_slice_in_dim(weight, place * wide, wide, 1)
        rows += [piece[:, i : i + width] for i in range(0, wide, width)]
    return jnp.concatenate(rows, axis=0)


def _assemble_body(place_ref, mine_ref, theirs_ref, *outs, grid, plan, split):
    y, c = place_ref[2], place_ref[3]
    for out, (row, height, blocks, width) in zip(outs, plan):
        for step in range(grid.y):
            side = lax.rem(y - step + grid.y, grid.y) if split else step
            for other, source in enumerate((mine_ref, theirs_ref)):
                column = side * grid.c + lax.rem(c + other, grid.c)
                for block in range(blocks):
                    place = pl.multiple_of((column * blocks + block) * width, width)
                    out[:, pl.ds(place, width)] = source[step, 0, pl.ds(row + block * height, height), :]


def assemble(grid, places, mine, theirs, shapes, width, split, name):
    plan, row = [], 0
    columns = grid.y * grid.c
    batches = grid.a * grid.b
    for height, wide in shapes:
        blocks = wide // (columns * width)
        rows = height // batches
        plan.append((row, rows, blocks, width))
        row += rows * blocks

    def slot(i, p):
        step_a = lax.rem(p[0] - lax.div(i, grid.b) + grid.a, grid.a)
        step_b = lax.rem(p[1] - lax.rem(i, grid.b) + grid.b, grid.b)
        return (0, step_b * grid.a + step_a, 0, 0)

    piece = pl.BlockSpec((grid.y, 1, row, width), slot)
    return pl.pallas_call(
        partial(_assemble_body, grid=grid, plan=plan, split=split),
        grid_spec=pltpu.PrefetchScalarGridSpec(
            num_scalar_prefetch=1,
            grid=(batches,),
            in_specs=[piece, piece],
            out_specs=[pl.BlockSpec((h // batches, w), lambda i, p: (i, 0)) for h, w in shapes],
        ),
        out_shape=[jax.ShapeDtypeStruct(shape, BF16) for shape in shapes],
        compiler_params=pltpu.CompilerParams(vmem_limit_bytes=48 << 20),
        cost_estimate=cost(flops=0, transcendentals=0, bytes_accessed=4 * sum(h * w for h, w in shapes)),
        name=name,
    )(places, mine, theirs)


class Gather:
    def __init__(self, grid, places, weights, width, split, name):
        self.grid, self.places, self.width, self.split, self.name = grid, places, width, split, name
        self.shapes = [(w.shape[0] * grid.a * grid.b, w.shape[1]) for w in weights]
        seq, columns = lax.axis_index("seq"), grid.y * grid.c
        if split:
            self.value = pieces(weights, seq, columns, width)[None]
        else:
            core = lax.rem(seq, grid.c)
            self.value = jnp.stack(
                [pieces(weights, i * grid.c + core, columns, width) for i in range(grid.y)]
            )

    def send(self, axis):
        self.axis = axis
        self.flight = spread(self.grid, self.value, axis)[1:]

    def land(self):
        parts = [self.value, *self.flight]
        if self.axis == "y":
            self.value = jnp.concatenate(parts, axis=0)
        else:
            self.value = jnp.stack(parts, axis=1)

    def whole(self):
        grid = self.grid
        mine = self.value.reshape(grid.y, grid.b * grid.a, *self.value.shape[-2:])
        theirs = grid.shift(mine, "c", 1)
        return assemble(
            grid, self.places, mine, theirs, self.shapes, self.width, self.split, self.name
        )


def _weight_grad_body(place_ref, *refs, grid, height, have_sum, aliased, split):
    left_ref, right_ref = refs[:2]
    refs = refs[2:]
    sum_ref = None
    if have_sum:
        sum_ref, refs = refs[0], refs[1:]
    refs = refs[aliased:]
    direct = height % 128 == 0
    outs, turned, natural = (refs[:-1], refs[-1], None) if direct else (refs[:-2], refs[-2], refs[-1])
    a, b = place_ref[0], place_ref[1]
    side, block = pl.program_id(0), pl.program_id(1)

    @pl.when((side == 0) & (block == 0))
    def _():
        if not direct:
            natural[...] = left_ref[...].T
        for step_b in range(grid.b):
            for step_a in range(grid.a):
                other = lax.bitwise_xor(a, jnp.int32(bit_reversed(step_a, grid.bits)))
                owner = other * grid.b + lax.rem(b + step_b, grid.b)
                here = pl.ds(pl.multiple_of(owner * height, height), height)
                turned[step_b, step_a] = left_ref[:, here].T if direct else natural[here, :]

    samples = turned.shape[-1]
    half = grid.a * height
    for step_b in range(grid.b):
        part = jnp.dot(
            turned[step_b].reshape(half, samples),
            right_ref[...].reshape(samples, -1),
            preferred_element_type=F32,
        ).reshape(grid.a, height, -1)
        if have_sum:
            part = part + sum_ref[0, step_b].astype(F32)
        part = part.astype(BF16)
        if split == "b":
            outs[step_b][0] = part
        elif split == "y":
            for k, out in enumerate(outs):

                @pl.when(side == k)
                def _(out=out, part=part):
                    out[step_b] = part
        else:
            outs[0][0, step_b] = part


def weight_grad(grid, places, left, right, width, core_step, total_rows, row, buffers, split, received=None, name="weight_grad", local=False, sub=None):
    samples, depth = left.shape
    height = depth // (grid.a * grid.b)
    sides = 1 if local else grid.y
    columns = 1 if local else grid.y * grid.c
    many = right.ndim == 5
    blocks = right.shape[1] if many else right.shape[1] // (columns * width)
    lo, count = (0, blocks) if sub is None else sub
    first = row // height

    def right_index(k, i, p):
        if local:
            return (0, 0)
        side = lax.rem(p[2] + k, grid.y)
        core = lax.rem(p[3] + core_step, grid.c)
        if many:
            return (side * grid.c + core, lo + i, 0, 0, 0)
        return (0, (side * grid.c + core) * blocks + lo + i)

    if split == "b":
        shape = (sides, grid.a, total_rows, width)
        specs = [pl.BlockSpec((1, grid.a, height, width), lambda k, i, p: (k, 0, first + i, 0))] * grid.b
        number = grid.b
    elif split == "y":
        shape = (grid.b, grid.a, total_rows, width)

        def index_of(which):
            def index(k, i, p):
                return (0, 0, first + jnp.where(k < which, 0, jnp.where(k > which, count - 1, i)), 0)

            return index

        specs = [pl.BlockSpec((grid.b, grid.a, height, width), index_of(k)) for k in range(sides)]
        number = sides
    else:
        shape = (sides, grid.b, grid.a, total_rows, width)
        specs = [pl.BlockSpec((1, grid.b, grid.a, height, width), lambda k, i, p: (k, 0, 0, first + i, 0))]
        number = 1
    in_specs = [
        pl.BlockSpec((samples, depth), lambda k, i, p: (0, 0), pipeline_mode=pl.Buffered(1)),
        pl.BlockSpec((1, 1, *right.shape[2:]) if many else (samples, width), right_index),
    ]
    operands = [left, right]
    if received is not None:
        in_specs.append(pl.BlockSpec((1, grid.b, grid.a, height, width), lambda k, i, p: (k, 0, 0, first + i, 0)))
        operands.append(received)
    aliases = {}
    if buffers is not None:
        for i, buffer in enumerate(buffers):
            aliases[1 + len(operands)] = i
            in_specs.append(pl.BlockSpec(memory_space=pl.ANY))
            operands.append(buffer)
    body = partial(
        _weight_grad_body, grid=grid, height=height, have_sum=received is not None,
        aliased=0 if buffers is None else len(buffers), split=split,
    )
    work = sides * count * width
    return pl.pallas_call(
        body,
        grid_spec=pltpu.PrefetchScalarGridSpec(
            num_scalar_prefetch=1,
            grid=(sides, count),
            in_specs=in_specs,
            out_specs=specs,
            scratch_shapes=[pltpu.VMEM((grid.b, grid.a, height, samples), BF16)]
            + ([] if height % 128 == 0 else [pltpu.VMEM((depth, samples), BF16)]),
        ),
        out_shape=[jax.ShapeDtypeStruct(shape, BF16)] * number,
        input_output_aliases=aliases,
        compiler_params=pltpu.CompilerParams(vmem_limit_bytes=48 << 20),
        cost_estimate=cost(flops=2 * samples * depth * work, transcendentals=0, bytes_accessed=2 * (samples * (depth + work) + depth * work)),
        name=name,
    )(places, *operands)


def added(parts):
    total = parts[0].astype(F32)
    for part in parts[1:]:
        total = total + part.astype(F32)
    return total


class Reduce:
    def __init__(self, grid, places, pairs, width, order, name, sub=None):
        self.grid, self.places, self.pairs, self.width = grid, places, pairs, width
        self.axes, self.name, self.sub = tuple(order), name, sub
        self.extra, self.result = None, None
        self.heights = [left.shape[1] // (grid.a * grid.b) for left, _ in pairs]
        columns = grid.y * grid.c
        self.counts = [
            right.shape[1] if right.ndim == 5 else right.shape[1] // (columns * width) if sub is None else sub[1]
            for _, right in pairs
        ]

    def _products(self, core_step, split, received, tokens):
        buffers, row = None, 0
        total = sum(h * n for h, n in zip(self.heights, self.counts))
        for i, ((left, right), h, n) in enumerate(zip(self.pairs, self.heights, self.counts)):
            if i == 0 and tokens:
                right = after(right, *tokens)
            buffers = weight_grad(
                self.grid, self.places, left, right, self.width, core_step, total, row, buffers, split,
                received, name=f"{self.name}_{i}_{core_step}", sub=self.sub,
            )
            row += h * n
        return buffers

    def far(self, *tokens):
        self.parts = self._products(1, None, None, tokens)

    def ship(self):
        self.received = self.grid.shift(self.parts[0], "c", 1)

    def near(self, *tokens):
        self.parts = self._products(0, self.axes[0], self.received, tokens)
        return self.parts[0]

    def send(self, stage, *tokens):
        grid, axis = self.grid, self.axes[stage]
        self.stage = stage
        if tokens:
            self.parts = list(lax.optimization_barrier((tuple(self.parts), tokens))[0])
        if self.extra is not None and axis == "b":
            self.parts = [jnp.concatenate([p, q], axis=-2) for p, q in zip(self.parts, self.extra)]
        self.flight = [grid.shift(self.parts[k], axis, k) for k in range(1, grid.size[axis])]

    def land(self):
        parts = [self.parts[0], *self.flight]
        if self.stage == 1:
            half = self.grid.a // 2
            self.parts = [added([p[k * half : (k + 1) * half] for p in parts]).astype(BF16) for k in range(2)]
        else:
            following = self.grid.size[self.axes[1]]
            self.parts = [added([p[k] for p in parts]).astype(BF16) for k in range(following)]


class Bundle:
    def __init__(self, *jobs):
        self.jobs, self.stage, self.result = jobs, 0, None
        self.grid = jobs[0].grid
        self.parts = [jnp.concatenate([job.parts[k] for job in jobs], axis=1) for k in range(2)]

    def send(self):
        self.flight = [self.grid.swap(self.parts[1], 1 << self.stage)]

    def land(self):
        total = [self.parts[0], self.flight[0]]
        self.stage += 1
        if self.stage < self.grid.bits:
            half = self.parts[0].shape[0] // 2
            self.parts = [
                added([part[k * half : (k + 1) * half] for part in total]).astype(BF16)
                for k in range(2)
            ]
            return
        row = 0
        for job in self.jobs:
            height = job.parts[0].shape[1]
            job.result = added([part[0, row : row + height] for part in total])
            row += height
        self.result = True


def gather_everywhere(shard):
    rows = shard.shape[0] // lax.axis_size("seq")
    part = lax.dynamic_slice_in_dim(shard, lax.axis_index("seq") * rows, rows, 0)
    return lax.all_gather(part, ("batch", "seq"), axis=0, tiled=True)


class Share:
    def __init__(self, grid, value):
        self.grid, self.value = grid, value

    def send(self, axis):
        self.flight = spread(self.grid, self.value, axis)[1:]

    def land(self):
        self.value = added([self.value, *self.flight])


class Collect:
    def __init__(self, grid, places, shard):
        self.grid, self.places, self.shape, self.value = grid, places, shard.shape, shard[None, None]

    def send(self, axis):
        self.axis = axis
        self.flight = spread(self.grid, self.value, axis)[1:]

    def land(self):
        self.value = jnp.concatenate([self.value, *self.flight], axis=1 if self.axis == "a" else 0)

    def whole(self):
        grid, places = self.grid, self.places
        value = self.value.reshape(grid.b * grid.a, *self.shape)
        owner = jnp.arange(grid.a * grid.b, dtype=jnp.int32)
        step_a = (places[0] - owner // grid.b) % grid.a
        step_b = (places[1] - owner % grid.b) % grid.b
        value = jnp.take(value, step_b * grid.a + step_a, axis=0)
        return value.transpose(1, 0, 2).reshape(self.shape[0], -1)


def layer_norm(values, scale_row, shift_row):
    center = values - jnp.mean(values, axis=-1, keepdims=True)
    spread = jnp.mean(center * center, axis=-1, keepdims=True)
    return center * lax.rsqrt(spread + epsilon) * scale_row + shift_row


def glu_gate(gated_rows):
    half_width = gated_rows.shape[-1] // 2
    return gated_rows[..., :half_width] * jax.nn.sigmoid(gated_rows[..., half_width:])


def batch_norm(conv_value, sum_first, sum_second, scale_row, shift_row, count_all):
    center = sum_first / count_all
    spread = sum_second / count_all - center * center
    return (conv_value - center) * lax.rsqrt(spread + epsilon) * scale_row + shift_row


def position_table(length, model_width):
    fine = 64
    coarse = 2 * length // fine
    column = jnp.arange(model_width, dtype=jnp.int32)
    rates = jnp.exp((column // 2).astype(jnp.float32) * (-2.0 * math.log(10000.0) / model_width))
    odd = (column % 2 == 1)[None, :]
    start = (jnp.arange(coarse, dtype=jnp.int32) * fine - (length - 1)).astype(jnp.float32)
    large = start[:, None] * rates[None, :]
    small = jnp.arange(fine, dtype=jnp.int32).astype(jnp.float32)[:, None] * rates[None, :]
    sin_large, cos_large = jnp.sin(large), jnp.cos(large)
    first = jnp.where(odd, cos_large, sin_large)[:, None, :]
    second = jnp.where(odd, -sin_large, cos_large)[:, None, :]
    table = first * jnp.cos(small)[None] + second * jnp.sin(small)[None]
    return table.astype(jnp.bfloat16).reshape(2 * length, model_width)


def depth_conv(padded, kernel_rows, length):
    result = kernel_rows[0] * padded[:, 0:length]
    for offset in range(1, kernel_rows.shape[0]):
        result = result + kernel_rows[offset] * padded[:, offset : offset + length]
    return result


def depth_conv_back(padded_grad, kernel_rows, length):
    last_tap = kernel_rows.shape[0] - 1
    result = kernel_rows[0] * padded_grad[:, last_tap : last_tap + length]
    for offset in range(1, last_tap + 1):
        result = (
            result
            + kernel_rows[offset] * padded_grad[:, last_tap - offset : last_tap - offset + length]
        )
    return result


def matmul_rows(left_side, right_side):
    return jnp.dot(left_side, right_side, preferred_element_type=jnp.float32)


def times_transpose(left_side, right_side):
    return lax.dot_general(
        left_side, right_side, (((1,), (1,)), ((), ())), preferred_element_type=jnp.float32
    )


def transpose_times(left_side, right_side):
    return lax.dot_general(
        left_side, right_side, (((0,), (0,)), ((), ())), preferred_element_type=jnp.float32
    )


def linear_back(grad_rows, weight):
    grad_low = grad_rows.astype(jnp.bfloat16)
    return (times_transpose(grad_low, weight), grad_low)


def ffn_enter(values, scale_row, shift_row, weight_in):
    normed_low = layer_norm(values, scale_row, shift_row).astype(jnp.bfloat16)
    hidden_pre = matmul_rows(normed_low, weight_in)
    hidden_low = jax.nn.silu(hidden_pre).astype(jnp.bfloat16)
    return (normed_low, hidden_pre.astype(jnp.bfloat16), hidden_low)


def ffn_forward(values, scale_row, shift_row, weight_in, weight_out):
    saved = ffn_enter(values, scale_row, shift_row, weight_in)
    return (matmul_rows(saved[2], weight_out), saved)


def ffn_backward_exit(grad_rows, weight_out, saved_parts):
    grad_hidden, grad_out_low = linear_back(grad_rows, weight_out)
    silu_value, silu_back = jax.vjp(jax.nn.silu, saved_parts[1].astype(jnp.float32))
    return (silu_back(grad_hidden)[0].astype(jnp.bfloat16), grad_out_low)


def ffn_backward_entry(grad_pre_low, values, scale_row, shift_row, weight_in):
    norm_value, norm_back = jax.vjp(layer_norm, values, scale_row, shift_row)
    return norm_back(times_transpose(grad_pre_low, weight_in))


def ffn_backward(grad_rows, values, scale_row, shift_row, weight_in, weight_out, saved_parts):
    normed_low, hidden_pre, hidden_low = saved_parts
    grad_hidden, grad_out_low = linear_back(grad_rows, weight_out)
    silu_value, silu_back = jax.vjp(jax.nn.silu, hidden_pre.astype(jnp.float32))
    grad_pre = silu_back(grad_hidden)[0]
    grad_normed, grad_pre_low = linear_back(grad_pre, weight_in)
    norm_value, norm_back = jax.vjp(layer_norm, values, scale_row, shift_row)
    grad_values, grad_scale, grad_shift = norm_back(grad_normed)
    return (grad_values, grad_scale, grad_shift, grad_pre_low, grad_out_low)


def sum_everywhere(value):
    for axis in ("seq", "batch"):
        size, step = lax.axis_size(axis), 1
        while step < size:
            value = value + lax.ppermute(value, axis, [(i, i ^ step) for i in range(size)])
            step *= 2
    return value


def per_device(
    grid,
    acoustic_sequence,
    utterance_durations,
    chosen_entry_number,
    discretizer_score_perturbation,
    softmax_heat,
    normalizer_affine_rows,
    discretizer_score_projection,
    lexicon_vectors,
    opening_dense_entry_projection,
    opening_dense_exit_projection,
    request_projection,
    lookup_projection,
    content_projection_kernel,
    relative_offset_projection,
    mixing_exit_projection,
    unit_kernel_before_gating,
    channelwise_filter_coefficients,
    unit_kernel_after_normalizing,
    closing_dense_entry_projection,
    closing_dense_exit_projection,
    result_adjoint,
    discrete_label_adjoint,
):
    places = grid.places()
    small = Collect(
        grid,
        places,
        jnp.concatenate([normalizer_affine_rows, channelwise_filter_coefficients], axis=0),
    )
    vector_rows = normalizer_affine_rows.shape[0]
    model_width = acoustic_sequence.shape[2]
    piece_width = model_width // (grid.y * grid.c)
    gather = partial(Gather, grid, places)
    second = gather([opening_dense_exit_projection], piece_width, True, "gather_opening_exit")
    sixth = gather([closing_dense_exit_projection], piece_width, False, "gather_closing_exit")
    third = gather(
        [request_projection, lookup_projection, content_projection_kernel, relative_offset_projection],
        piece_width,
        False,
        "gather_attention",
    )
    macaron_in_all = gather_everywhere(opening_dense_entry_projection)
    small.send("a")
    second.send("a")
    settle([small, second])
    small.send("b")
    second.send("b")
    third.send("a")
    settle([small, second, third])
    small_all = small.whole()
    vectors_all, depth_all = small_all[:vector_rows], small_all[vector_rows:]
    middle_shards = (
        mixing_exit_projection,
        unit_kernel_after_normalizing,
        unit_kernel_before_gating,
        discretizer_score_projection,
        lexicon_vectors,
    )
    middle_shards, entry_shard, second.value = lax.optimization_barrier(
        (middle_shards, closing_dense_entry_projection, second.value)
    )
    middle_all = gather_everywhere(jnp.concatenate(middle_shards, axis=1))
    out_all, conv_out_all, conv_in_all, quant_all, codebook_all = jnp.split(
        middle_all, [model_width * i for i in (1, 2, 4, 5)], axis=1
    )
    closing_in_all = gather_everywhere(entry_shard)
    groups, local_len, model_width = acoustic_sequence.shape
    seq_count = lax.axis_size("seq")
    seq_place = lax.axis_index("seq")
    full_len = local_len * seq_count
    entries = lexicon_vectors.shape[0] * grid.a * grid.b
    total_rows = groups * local_len
    local_width = model_width // seq_count
    kernel_size = depth_all.shape[0]
    rim_width = kernel_size // 2
    height = model_width // (grid.a * grid.b)
    params_f = vectors_all.astype(jnp.float32)
    depth_f = depth_all.astype(jnp.float32)
    positions = seq_place * local_len + jnp.arange(local_len, dtype=jnp.int32)
    valid_mask = (positions[None, :] < utterance_durations[:, None]).astype(jnp.float32)
    valid_rows = valid_mask.reshape(total_rows, 1)
    inputs_low = acoustic_sequence.reshape(total_rows, model_width)
    inputs_f = inputs_low.astype(jnp.float32)
    second.send("y")
    third.send("b")
    macaron_saved = ffn_enter(inputs_f, params_f[0], params_f[5], macaron_in_all)
    sixth.send("a")
    macaron_hidden = settle([second, third, sixth], macaron_saved[2])
    sixth.send("b")
    macaron_saved = (*macaron_saved[:2], macaron_hidden)
    (macaron_out_all,) = second.whole()
    query_all, key_all, value_all, pos_all = third.whole()
    macaron_value = matmul_rows(macaron_hidden, macaron_out_all)
    first_mid = inputs_f + 0.5 * macaron_value
    attn_normed = layer_norm(first_mid, params_f[1], params_f[6]).astype(jnp.bfloat16)
    stacked = project_heads(attn_normed, [query_all, key_all, value_all], groups, seq_count)
    by_heads = lax.all_to_all(stacked, "seq", split_axis=0, concat_axis=0, tiled=True)
    table_low = position_table(full_len, model_width)
    pos_columns = lax.dynamic_slice_in_dim(pos_all, seq_place * local_width, local_width, 1)
    position_low = matmul_rows(table_low, pos_columns).astype(jnp.bfloat16)
    biases = lax.dynamic_slice_in_dim(params_f[12:14], seq_place * local_width, local_width, 1)
    by_heads, position_low = settle([], by_heads, position_low)
    attended_low, probs = attend_forward(by_heads, position_low, biases, utterance_durations)
    attended_low = settle([sixth], attended_low)
    back_time = lax.all_to_all(
        attended_low, "seq", split_axis=0, concat_axis=0, tiled=True
    )
    attended_rows = back_time.transpose(1, 2, 0, 3).reshape(total_rows, model_width)
    second_mid = first_mid + matmul_rows(attended_rows, out_all)
    conv_normed = layer_norm(second_mid, params_f[2], params_f[7]).astype(jnp.bfloat16)
    gated_rows = matmul_rows(conv_normed, conv_in_all)
    glu_low = (
        (valid_rows * glu_gate(gated_rows))
        .astype(jnp.bfloat16)
        .reshape(groups, local_len, model_width)
    )
    padded_glu = extended(glu_low, (("seq", 1),), rim_width)
    conv_value = depth_conv(padded_glu, depth_f, local_len).reshape(total_rows, model_width)
    masked_conv = valid_rows * conv_value
    sums = sum_everywhere(
        jnp.stack(
            [
                jnp.sum(masked_conv, axis=0),
                jnp.sum(masked_conv * conv_value, axis=0),
                jnp.broadcast_to(jnp.sum(valid_mask), (model_width,)),
            ]
        )
    )
    sum_first, sum_second, count_all = sums[0], sums[1], sums[2]
    bound_norm = partial(batch_norm, count_all=count_all)
    normalized = bound_norm(conv_value, sum_first, sum_second, params_f[10], params_f[11])
    act_low = jax.nn.silu(normalized).astype(jnp.bfloat16)
    (closing_out_all,) = sixth.whole()
    third_mid = second_mid + matmul_rows(act_low, conv_out_all)
    closing_value, closing_saved = ffn_forward(
        third_mid, params_f[3], params_f[8], closing_in_all, closing_out_all
    )
    quant_logits = matmul_rows(inputs_low, quant_all)
    scaled_logits = (
        quant_logits
        + discretizer_score_perturbation.reshape(total_rows, entries).astype(jnp.float32)
    ) / softmax_heat
    relaxed_assignments = jax.nn.softmax(scaled_logits, axis=-1)
    soft_low = relaxed_assignments.astype(jnp.bfloat16)
    one_hot = (
        chosen_entry_number.reshape(total_rows, 1) == jnp.arange(entries, dtype=jnp.int32)[None, :]
    ).astype(jnp.bfloat16)
    codes_value = valid_rows * (
        matmul_rows(one_hot, codebook_all) + matmul_rows(soft_low, codebook_all)
    )
    grad_codes = (
        valid_rows * discrete_label_adjoint.reshape(total_rows, model_width).astype(jnp.float32)
    ).astype(jnp.bfloat16)
    grad_soft = times_transpose(grad_codes, codebook_all)
    rescaled_derivative = relaxed_assignments * (
        grad_soft - jnp.sum(grad_soft * relaxed_assignments, axis=-1, keepdims=True)
    )
    score_derivative_lowprecision = (rescaled_derivative / softmax_heat).astype(jnp.bfloat16)
    grad_quant_in = times_transpose(score_derivative_lowprecision, quant_all)
    fourth_mid = third_mid + 0.5 * closing_value
    final_value, final_back = jax.vjp(layer_norm, fourth_mid, params_f[4], params_f[9])
    output = (valid_rows * final_value).astype(jnp.bfloat16).reshape(groups, local_len, model_width)
    codes = codes_value.astype(jnp.bfloat16).reshape(groups, local_len, model_width)
    grad_final = valid_rows * result_adjoint.reshape(total_rows, model_width).astype(jnp.float32)
    grad_fourth, scale_four, shift_four = final_back(grad_final)
    grad_closing, scale_three, shift_three, close_pre_low, close_out_low = ffn_backward(
        0.5 * grad_fourth,
        third_mid,
        params_f[3],
        params_f[8],
        closing_in_all,
        closing_out_all,
        closing_saved,
    )
    grad_third = grad_fourth + grad_closing
    close_normed, close_pre, close_hidden = closing_saved
    reduce = partial(Reduce, grid, places)
    closing_job = reduce(
        [(close_hidden, close_out_low), (close_normed, close_pre_low)], piece_width, "by", "closing"
    )
    closing_job.far()
    closing_job.ship()
    grad_act, grad_third_low = linear_back(grad_third, conv_out_all)
    silu_value, silu_back = jax.vjp(jax.nn.silu, normalized)
    grad_normalized = silu_back(grad_act)[0]
    norm_value, norm_back = jax.vjp(
        bound_norm, conv_value, sum_first, sum_second, params_f[10], params_f[11]
    )
    grad_conv_direct, part_first, part_second, grad_bn_scale, grad_bn_shift = norm_back(
        grad_normalized
    )
    totals = sum_everywhere(jnp.stack([part_first, part_second]))
    chosen_soft = one_hot + soft_low
    early_job = reduce(
        [
            (act_low, grad_third_low),
            (inputs_low, score_derivative_lowprecision),
            (chosen_soft, grad_codes),
        ],
        piece_width,
        "yb",
        "early",
    )
    early_job.far()
    early_job.ship()
    closing_job.near()
    totals = settle([], totals, hold=[closing_job])
    closing_job.send(0)
    total_first, total_second = totals[0], totals[1]
    grad_conv = grad_conv_direct + valid_rows * (total_first + 2.0 * conv_value * total_second)
    grad_conv_low = grad_conv.astype(jnp.bfloat16).reshape(groups, local_len, model_width)
    padded_grad = extended(grad_conv_low, (("seq", 1),), rim_width)
    grad_glu = valid_rows * depth_conv_back(padded_grad, depth_f, local_len).reshape(
        total_rows, model_width
    )
    grad_conv_float = grad_conv_low.astype(jnp.float32)
    grad_depth = jnp.stack(
        [
            jnp.sum(
                padded_glu[:, offset : offset + local_len].astype(jnp.float32) * grad_conv_float,
                axis=(0, 1),
            )
            for offset in range(kernel_size)
        ]
    )
    glu_value, glu_back = jax.vjp(glu_gate, gated_rows)
    grad_gated = glu_back(grad_glu)[0]
    grad_conv_normed, grad_gated_low = linear_back(grad_gated, conv_in_all)
    conv_norm_value, conv_norm_back = jax.vjp(layer_norm, second_mid, params_f[2], params_f[7])
    grad_from_conv, scale_two, shift_two = conv_norm_back(grad_conv_normed)
    grad_second = grad_third + grad_from_conv
    grad_second_low = grad_second.astype(jnp.bfloat16)
    grad_attended = unproject_heads(grad_second_low, out_all, groups, seq_count)
    grad_heads = lax.all_to_all(grad_attended, "seq", split_axis=0, concat_axis=0, tiled=True)

    middle_job = reduce(
        [(conv_normed, grad_gated_low), (attended_rows, grad_second_low)],
        piece_width,
        "by",
        "middle",
    )
    middle_job.far()
    early_job.near()
    grad_heads = settle([], grad_heads, hold=[early_job, middle_job])
    early_job.send(0)
    middle_job.ship()
    grad_stack, grad_position_low, grad_biases = attend_backward(
        probs, by_heads, grad_heads, position_low, biases
    )
    grad_stack = settle([early_job], grad_stack)
    grad_time = lax.all_to_all(grad_stack, "seq", split_axis=0, concat_axis=0, tiled=True)
    position_parts = weight_grad(
        grid, places, table_low, grad_position_low, piece_width, 0, height, 0, None, "b",
        name="position_grad", local=True,
    )
    middle_job.near()
    grad_time, *position_parts = settle(
        [closing_job], grad_time, *position_parts, hold=[middle_job]
    )
    closing_job.send(1)
    early_job.send(1)
    middle_job.send(0)
    grad_attn_normed = join_heads(grad_time, [query_all, key_all, value_all])
    attn_norm_value, attn_norm_back = jax.vjp(layer_norm, first_mid, params_f[1], params_f[6])
    grad_from_attn, scale_one, shift_one = attn_norm_back(grad_attn_normed)
    grad_first = grad_second + grad_from_attn
    attention_job = reduce(
        [(attn_normed, grad_time)], piece_width, "yb", "attention"
    )
    attention_job.extra = [part[0] for part in position_parts]
    attention_job.far()
    attention_job.ship()
    content_full, position_full = lax.dynamic_update_slice_in_dim(
        jnp.zeros((2, model_width), jnp.float32), grad_biases, seq_place * local_width, 1
    )
    mac_normed, mac_pre, mac_hidden = macaron_saved
    mac_out_low = (0.5 * grad_first).astype(jnp.bfloat16)
    macaron_out_job = reduce([(mac_hidden, mac_out_low)], piece_width, "by", "opening_exit")
    macaron_out_job.far()
    macaron_out_job.ship()
    attention_job.near()
    macaron_out_job.near()
    mac_out_low = settle([], mac_out_low, hold=[attention_job, macaron_out_job])
    attention_job.send(0)
    macaron_out_job.send(0)
    mac_pre_low, mac_out_low = ffn_backward_exit(mac_out_low, macaron_out_all, macaron_saved)
    halves = mac_pre_low.shape[1] // model_width // 2
    macaron_in_jobs = [
        reduce([(mac_normed, mac_pre_low)], piece_width, order, name, sub=(i * halves, halves))
        for i, (order, name) in enumerate((("yb", "opening_entry"), ("by", "opening_entry_more")))
    ]
    for job in macaron_in_jobs:
        job.far()
    mac_pre_low = settle(
        [closing_job, early_job, middle_job], mac_pre_low, hold=macaron_in_jobs
    )
    for job in macaron_in_jobs:
        job.ship()
    first_tails = Bundle(closing_job, early_job)
    first_tails.send()
    middle_job.send(1)
    grad_macaron, scale_zero, shift_zero = ffn_backward_entry(
        mac_pre_low, inputs_f, params_f[0], params_f[5], macaron_in_all
    )
    grad_layer_in = grad_first + grad_macaron
    frames_grad = (
        (grad_layer_in + grad_quant_in).astype(jnp.bfloat16).reshape(groups, local_len, model_width)
    )
    vectors_grad = jnp.stack(
        [
            scale_zero,
            scale_one,
            scale_two,
            scale_three,
            scale_four,
            shift_zero,
            shift_one,
            shift_two,
            shift_three,
            shift_four,
            grad_bn_scale,
            grad_bn_shift,
            content_full,
            position_full,
        ]
    )
    small = Share(grid, jnp.concatenate([vectors_grad, grad_depth], axis=0))
    small.send("c")
    small.land()
    for job in macaron_in_jobs:
        job.near()
    small.value = settle(
        [first_tails, middle_job, attention_job, macaron_out_job],
        small.value,
        hold=macaron_in_jobs,
    )
    for job in macaron_in_jobs:
        job.send(0)
    attention_job.send(1)
    macaron_out_job.send(1)
    first_tails.send()
    middle_tails = Bundle(middle_job)
    middle_tails.send()
    small.send("y")
    settle([small, first_tails, middle_tails, attention_job, macaron_out_job, *macaron_in_jobs])
    for job in macaron_in_jobs:
        job.send(1)
    late_tails = Bundle(attention_job, macaron_out_job)
    late_tails.send()
    middle_tails.send()
    small.send("b")
    settle([small, middle_tails, late_tails, *macaron_in_jobs])
    late_tails.send()
    last_tails = Bundle(*macaron_in_jobs)
    last_tails.send()
    small.send("a")
    settle([small, last_tails, late_tails])
    last_tails.send()
    settle([last_tails])
    small_width = model_width // (grid.a * grid.b)
    small_sums = lax.dynamic_slice_in_dim(
        small.value, lax.axis_index("batch") * small_width, small_width, 1
    )
    vectors_sum, depth_sum = small_sums[:vector_rows], small_sums[vector_rows:]

    def rows_of(job, count):
        return (job.result[i * height : (i + 1) * height] for i in range(count))

    exit_rows = close_hidden.shape[1] // (grid.a * grid.b)
    closing_out_sum, closing_in_sum = closing_job.result[:exit_rows], closing_job.result[exit_rows:]
    conv_out_sum, quant_sum, codebook_sum = rows_of(early_job, 3)
    conv_in_sum, out_sum = middle_job.result[: 2 * height], middle_job.result[2 * height :]
    query_sum, key_sum, value_sum, pos_sum = rows_of(attention_job, 4)
    macaron_out_sum = macaron_out_job.result
    macaron_in_sum = jnp.concatenate([job.result for job in macaron_in_jobs])

    def side_by_side(blocks):
        return jnp.concatenate(
            [blocks[i : i + height] for i in range(0, blocks.shape[0], height)], axis=1
        )

    closing_in_sum, conv_in_sum, macaron_in_sum = (
        side_by_side(closing_in_sum),
        side_by_side(conv_in_sum),
        side_by_side(macaron_in_sum),
    )
    return (
        output,
        codes,
        frames_grad,
        vectors_sum,
        quant_sum,
        codebook_sum,
        macaron_in_sum,
        macaron_out_sum,
        query_sum,
        key_sum,
        value_sum,
        pos_sum,
        out_sum,
        conv_in_sum,
        depth_sum,
        conv_out_sum,
        closing_in_sum,
        closing_out_sum,
    )


def solution(mesh):
    placed = (
        P("batch", "seq", None),
        P("batch"),
        P("batch", "seq"),
        P("batch", "seq", None),
        P(),
        P(None, "batch"),
        P("batch", None),
        P("batch", None),
        P("batch", None),
        P("batch", None),
        P("batch", None),
        P("batch", None),
        P("batch", None),
        P("batch", None),
        P("batch", None),
        P("batch", None),
        P(None, "batch"),
        P("batch", None),
        P("batch", None),
        P("batch", None),
        P("batch", "seq", None),
        P("batch", "seq", None),
    )
    return jax.shard_map(
        partial(per_device, Grid(mesh)),
        mesh=mesh,
        in_specs=placed,
        out_specs=(
            P("batch", "seq", None),
            P("batch", "seq", None),
            P("batch", "seq", None),
            P(None, "batch"),
            P("batch", "seq"),
            P("batch", "seq"),
            P("batch", "seq"),
            P("batch", "seq"),
            P("batch", "seq"),
            P("batch", "seq"),
            P("batch", "seq"),
            P("batch", "seq"),
            P("batch", "seq"),
            P("batch", "seq"),
            P(None, "batch"),
            P("batch", "seq"),
            P("batch", "seq"),
            P("batch", "seq"),
        ),
        check_vma=False,
    )
```
